32 devices in a mesh: items: 8 (over y, x, core), heads: 4 (over z).
Axes of the slice: x: 2, y: 2, z: 4, core: 2. Of those that a mesh axis runs over, the one named last changes fastest.
Arguments:
- latents: bfloat16 [16384, 1024], P(('items', 'heads')), may hold values from -6 to 6
- pixels: bfloat16 [261, 131072], P(None, 'items'), may hold values from -6 to 6
- pixel_item: int32 [8, 16384], P('items'), may hold values from 0 to 3, never falling along the last dimension, each value on 1 to 6144 neighbouring positions
- cotangent: bfloat16 [16384, 1024], P(('items', 'heads')), may hold values from -6 to 6
- cross_query: float32 [1024, 1024], P(('items', 'heads')), may hold values from -0.1875 to 0.1875
- cross_key: float32 [261, 1024], P(None, ('items', 'heads')), may hold values from -0.375 to 0.375
- cross_value: float32 [261, 1024], P(None, ('items', 'heads')), may hold values from -0.375 to 0.375
- cross_out: float32 [1024, 1024], P(('items', 'heads')), may hold values from -4 to 4
- cross_up: float32 [1024, 1024], P('items', 'heads'), may hold values from -0.1875 to 0.1875
- cross_down: float32 [1024, 1024], P('heads', 'items'), may hold values from -0.1875 to 0.1875
- self_query: float32 [1024, 1024], P('items', 'heads'), may hold values from -0.1875 to 0.1875
- self_key: float32 [1024, 1024], P('items', 'heads'), may hold values from -0.1875 to 0.1875
- self_value: float32 [1024, 1024], P('items', 'heads'), may hold values from -0.1875 to 0.1875
- self_out: float32 [1024, 1024], P('heads', 'items'), may hold values from -3 to 3
- self_up: float32 [1024, 1024], P('items', 'heads'), may hold values from -0.1875 to 0.1875
- self_down: float32 [1024, 1024], P('heads', 'items'), may hold values from -0.1875 to 0.1875
- gain_cross: float32 [1024], P(('items', 'heads')), may hold values from 0.1 to 1.9
- gain_cross_mlp: float32 [1024], P(('items', 'heads')), may hold values from 0.1 to 1.9
- gain_self: float32 [1024], P(('items', 'heads')), may hold values from 0.1 to 1.9
- gain_self_mlp: float32 [1024], P(('items', 'heads')), may hold values from 0.1 to 1.9
Outputs:
- layer_out: bfloat16 [16384, 1024], P(('items', 'heads'))
- latents_grad: float32 [16384, 1024], P(('items', 'heads'))
- grad_cross_query: float32 [1024, 1024], P(('items', 'heads'))
- grad_cross_key: float32 [261, 1024], P(None, ('items', 'heads'))
- grad_cross_value: float32 [261, 1024], P(None, ('items', 'heads'))
- grad_cross_out: float32 [1024, 1024], P(('items', 'heads'))
- grad_cross_up: float32 [1024, 1024], P('items', 'heads')
- grad_cross_down: float32 [1024, 1024], P('heads', 'items')
- grad_self_query: float32 [1024, 1024], P('items', 'heads')
- grad_self_key: float32 [1024, 1024], P('items', 'heads')
- grad_self_value: float32 [1024, 1024], P('items', 'heads')
- grad_self_out: float32 [1024, 1024], P('heads', 'items')
- grad_self_up: float32 [1024, 1024], P('items', 'heads')
- grad_self_down: float32 [1024, 1024], P('heads', 'items')
- grad_gain_cross: float32 [1024], P(('items', 'heads'))
- grad_gain_cross_mlp: float32 [1024], P(('items', 'heads'))
- grad_gain_self: float32 [1024], P(('items', 'heads'))
- grad_gain_self_mlp: float32 [1024], P(('items', 'heads'))
The draws below stay inside these ranges and needn't reach their ends.
Inputs may be any that keep to these rules, and one draw needn't show every extreme that they name: `pixel_item`: within each group the item numbers never fall along the pixel rows; every one of the 4 items has 1 to 6144 pixel rows, and some item has exactly 6144.
All inputs are finite; a program needn't handle non-finite values.
Results may differ from the reference program's by a relative error of at most 0.03.
Values may be sent and summed in bfloat16 or wider, within the bound.
A program may use at most 384 MiB of HBM per device.

```python
import math
import jax
import jax.numpy as jnp
import numpy as np
from jax import lax

D = 1024
C_IN = 261
F = 1024
HEADS = 8
HEAD = 128
NLAT = 512
ITEMS_DEV = 4
GROUPS = 8
GROUP_ROWS = 2048
LATENTS = 16384
PIX_GRP = 16384
PIXELS = 131072
PIX_MOST = 6144


def levels(key, shape, pieces, smallest, top_value):
    gain, own = 1.0, jax.random.fold_in(key, 6)
    for dim, parts in pieces:
        heights = jnp.exp(jax.random.uniform(jax.random.fold_in(own, dim), (parts,), jnp.float32, smallest / len(pieces), top_value / len(pieces)))
        gain = gain * jnp.repeat(heights, shape[dim] // parts).reshape([-1 if axis == dim else 1 for axis in range(len(shape))])
    return gain


def split_up(count, total, limit, slope):
    weights = [(1 << 20) // math.isqrt(standing ** slope) + 1 for standing in range(2, count + 1)]
    rest, holding = total - limit - (count - 1), [1] * (count - 1)
    while rest > 0:
        movable = [i for i in range(count - 1) if holding[i] < limit]
        pool, left = sum([weights[i] for i in movable]), rest
        for i in movable:
            addition = min(limit - holding[i], max(1, left * weights[i] // pool), rest)
            holding[i] = holding[i] + addition
            rest = rest - addition
    return np.array([limit] + holding)


def ragged_sizes(stream_key, count, total, most, lean):
    if count == 2:
        one = jax.random.randint(stream_key, (), max(1, total - most), min(most, total - 1) + 1)
        return jnp.stack([one, total - one])
    lengths = jnp.asarray(split_up(count, total, most, lean), jnp.int32)
    twos = (count - 1) // 2
    giver, taker = lengths[1:1 + 2 * twos:2], lengths[2:2 + 2 * twos:2]
    margin = jnp.minimum(giver - 1, most - taker)
    shifted = jax.random.randint(jax.random.fold_in(stream_key, 1), (twos,), 0, 1 << 20) % (margin + 1)
    lengths = lengths.at[1:1 + 2 * twos:2].set(giver - shifted).at[2:2 + 2 * twos:2].set(taker + shifted)
    return lengths[jax.random.permutation(jax.random.fold_in(stream_key, 2), count)]


def scatter_about(stream_key, shape, scale, limit, cuts=(), kind=jnp.bfloat16):
    drawn = scale * jax.random.normal(stream_key, shape, jnp.float32)
    if cuts:
        drawn = drawn * levels(stream_key, shape, cuts, -0.22, 0.18)
    return jnp.clip(drawn, -limit, limit).astype(kind)


def setup_inputs(seed: int = 0) -> dict:
    seeds = jax.random.split(jax.random.key(seed), 21)
    return {
        "latents": scatter_about(seeds[0], (LATENTS, D), 1.0, 6.0, ((0, 32),)),
        "pixels": scatter_about(seeds[1], (C_IN, PIXELS), 1.0, 6.0, ((1, 8),)),
        "pixel_item": jax.vmap(lambda own: jnp.searchsorted(jnp.cumsum(ragged_sizes(own, ITEMS_DEV, PIX_GRP, PIX_MOST, 2)), jnp.arange(PIX_GRP), side="right"))(jax.random.split(seeds[2], GROUPS)).reshape((GROUPS, PIX_GRP)).astype(jnp.int32),
        "cotangent": scatter_about(seeds[3], (LATENTS, D), 1.0, 6.0, ((0, 32),)),
        "cross_query": scatter_about(seeds[4], (D, D), D ** -0.5, 0.1875, ((0, 32),), jnp.float32),
        "cross_key": scatter_about(seeds[5], (C_IN, D), C_IN ** -0.5, 0.375, ((1, 32),), jnp.float32),
        "cross_value": scatter_about(seeds[6], (C_IN, D), C_IN ** -0.5, 0.375, ((1, 32),), jnp.float32),
        "cross_out": scatter_about(seeds[7], (D, D), 2 ** -0.5, 4.0, ((0, 32),), jnp.float32),
        "cross_up": scatter_about(seeds[8], (D, F), D ** -0.5, 0.1875, ((0, 8), (1, 4)), jnp.float32),
        "cross_down": scatter_about(seeds[9], (F, D), F ** -0.5, 0.1875, ((0, 4), (1, 8)), jnp.float32),
        "self_query": scatter_about(seeds[10], (D, D), D ** -0.5, 0.1875, ((0, 8), (1, 4)), jnp.float32),
        "self_key": scatter_about(seeds[11], (D, D), D ** -0.5, 0.1875, ((0, 8), (1, 4)), jnp.float32),
        "self_value": scatter_about(seeds[12], (D, D), D ** -0.5, 0.1875, ((0, 8), (1, 4)), jnp.float32),
        "self_out": scatter_about(seeds[13], (D, D), 4 ** -0.5, 3.0, ((0, 4), (1, 8)), jnp.float32),
        "self_up": scatter_about(seeds[14], (D, F), D ** -0.5, 0.1875, ((0, 8), (1, 4)), jnp.float32),
        "self_down": scatter_about(seeds[15], (F, D), F ** -0.5, 0.1875, ((0, 4), (1, 8)), jnp.float32),
        "gain_cross": jnp.clip(1.0 + 0.18 * jax.random.normal(seeds[16], (D,), jnp.float32), 0.1, 1.9),
        "gain_cross_mlp": jnp.clip(1.0 + 0.18 * jax.random.normal(seeds[17], (D,), jnp.float32), 0.1, 1.9),
        "gain_self": jnp.clip(1.0 + 0.18 * jax.random.normal(seeds[18], (D,), jnp.float32), 0.1, 1.9),
        "gain_self_mlp": jnp.clip(1.0 + 0.18 * jax.random.normal(seeds[19], (D,), jnp.float32), 0.1, 1.9),
    }


EPSILON = 1e-05
MASKED = -1e+30
HIGHEST = lax.Precision.HIGHEST

@jax.custom_vjp
def low(v):
    return lax.optimization_barrier(v.astype(jnp.bfloat16)).astype(jnp.float32)

@jax.custom_vjp
def low_back(v):
    return v

def low_keep(v):
    return (low(v), None)

def low_pass(kept, grad):
    return (grad,)

def back_keep(v):
    return (v, None)

def back_low(kept, grad):
    return (low(grad),)
low.defvjp(low_keep, low_pass)
low_back.defvjp(back_keep, back_low)

def product_high(left_side, right_side):
    return jnp.dot(left_side, right_side, precision=HIGHEST)

def norm_rows(values, gain_vec):
    centre = values - lax.optimization_barrier(jnp.mean(values, axis=-1, keepdims=True))
    spread = lax.optimization_barrier(jnp.mean(centre * centre, axis=-1, keepdims=True))
    return centre * lax.rsqrt(spread + EPSILON) * gain_vec

def norm_pixels(values):
    centre = values - lax.optimization_barrier(jnp.mean(values, axis=0, keepdims=True))
    spread = lax.optimization_barrier(jnp.mean(centre * centre, axis=0, keepdims=True))
    return centre * lax.rsqrt(spread + EPSILON)

def feed_forward(residual, gain_vec, up_weight, down_weight):
    normed = low(norm_rows(residual, gain_vec))
    before = low_back(product_high(normed, up_weight))
    hidden = low(jax.nn.gelu(before))
    return residual + low_back(product_high(hidden, down_weight))

def self_attention(residual, gain_vec, query_weight, key_weight, value_weight, out_weight):
    normed = low(norm_rows(residual, gain_vec))
    group_rows = normed.shape[0]
    shape_four = (group_rows // NLAT, NLAT, HEADS, HEAD)
    query_rows = low(low_back(product_high(normed, query_weight))).reshape(shape_four)
    key_rows = low(low_back(product_high(normed, key_weight))).reshape(shape_four)
    value_rows = low(low_back(product_high(normed, value_weight))).reshape(shape_four)
    scores = jnp.einsum('iqhd,ikhd->ihqk', query_rows, key_rows, precision=HIGHEST) * (1.0 / math.sqrt(HEAD))
    scores = low_back(scores)
    weights = low(jax.nn.softmax(scores, axis=-1))
    mixed_rows = jnp.einsum('ihqk,ikhd->iqhd', weights, value_rows, precision=HIGHEST).reshape(group_rows, HEADS * HEAD)
    mixed_rows = low(low_back(mixed_rows))
    return residual + low_back(product_high(mixed_rows, out_weight))

def group_layer(param_set, latent_rows, pixel_rows, item_ids):
    cross_query, cross_key, cross_value, cross_out, cross_up, cross_down, self_query, self_key, self_value, self_out, self_up, self_down, gain_cross, gain_cross_mlp, gain_self, gain_self_mlp = param_set
    group_rows = latent_rows.shape[0]
    row_item = jnp.arange(group_rows, dtype=jnp.int32) // NLAT
    pixel_norm = low(norm_pixels(pixel_rows))
    key_rows = low(product_high(pixel_norm.T, cross_key))
    value_rows = low(product_high(pixel_norm.T, cross_value))
    normed = low(norm_rows(latent_rows, gain_cross))
    query_rows = low(low_back(product_high(normed, cross_query)))
    scores = low_back(product_high(query_rows, key_rows.T) * (1.0 / math.sqrt(D)))
    scores = jnp.where(row_item[:, None] == item_ids[None, :], scores, MASKED)
    weights = low(jax.nn.softmax(scores, axis=-1))
    mixed_rows = low(low_back(product_high(weights, value_rows)))
    residual = latent_rows + low_back(product_high(mixed_rows, cross_out))
    residual = feed_forward(residual, gain_cross_mlp, cross_up, cross_down)
    residual = self_attention(residual, gain_self, self_query, self_key, self_value, self_out)
    return feed_forward(residual, gain_self_mlp, self_up, self_down)

def reference(latents, pixels, pixel_item, cotangent, cross_query, cross_key, cross_value, cross_out, cross_up, cross_down, self_query, self_key, self_value, self_out, self_up, self_down, gain_cross, gain_cross_mlp, gain_self, gain_self_mlp):
    param_set = (cross_query, cross_key, cross_value, cross_out, cross_up, cross_down, self_query, self_key, self_value, self_out, self_up, self_down, gain_cross, gain_cross_mlp, gain_self, gain_self_mlp)
    pixel_groups = pixels.astype(jnp.float32).reshape(C_IN, GROUPS, PIX_GRP).transpose(1, 0, 2)
    checked = jax.checkpoint(group_layer)

    def forward(latent_all, masters):
        rounded_set = tuple((low(master) for master in masters))
        latent_groups = latent_all.reshape(GROUPS, GROUP_ROWS, D)

        def one_group(carried, group_data):
            return (carried, checked(rounded_set, group_data[0], group_data[1], group_data[2]))
        unused, outputs = lax.scan(one_group, jnp.zeros((), jnp.float32), (latent_groups, pixel_groups, pixel_item))
        return outputs.reshape(LATENTS, D)
    outputs, pullback = jax.vjp(forward, latents.astype(jnp.float32), param_set)
    latents_grad, grads = pullback(cotangent.astype(jnp.float32))
    return (outputs.astype(jnp.bfloat16), latents_grad, grads[0], grads[1], grads[2], grads[3], grads[4], grads[5], grads[6], grads[7], grads[8], grads[9], grads[10], grads[11], grads[12], grads[13], grads[14], grads[15])
```

```python
import math

import jax
import jax.numpy as jnp
from jax import lax
from jax.sharding import PartitionSpec as P

HEAD = 128
NLAT = 512
PIX_MOST = 6144
LANE = 128

EPSILON = 1e-05
MASKED = -1e30
ALL = ("items", "heads")


def rounded(values):
    return values.astype(jnp.bfloat16)


def widened(values):
    return values.astype(jnp.float32)


def product(left_side, right_side):
    return jnp.dot(left_side, right_side, preferred_element_type=jnp.float32)


def product_tn(left_side, right_side):
    return lax.dot_general(
        left_side, right_side, (((0,), (0,)), ((), ())), preferred_element_type=jnp.float32
    )


def product_nt(left_side, right_side):
    return lax.dot_general(
        left_side, right_side, (((1,), (1,)), ((), ())), preferred_element_type=jnp.float32
    )


def split_parts(values):
    high = rounded(values)
    return high, rounded(values - widened(high))


def split_product(left_f32, right_bf16, form=product):
    high, low = split_parts(left_f32)
    return form(high, right_bf16) + form(low, right_bf16)


def norm_rows(values, gain_vec):
    centre = values - jnp.mean(values, axis=-1, keepdims=True)
    spread = jnp.mean(centre * centre, axis=-1, keepdims=True)
    return centre * lax.rsqrt(spread + EPSILON) * gain_vec


def norm_pixels(values):
    centre = values - jnp.mean(values, axis=0, keepdims=True)
    spread = jnp.mean(centre * centre, axis=0, keepdims=True)
    return centre * lax.rsqrt(spread + EPSILON)


def norm_backward(residual, gain_vec, grad_normed):
    unused, norm_back = jax.vjp(norm_rows, residual, gain_vec)
    return norm_back(grad_normed)


def assemble(blocks, kind, items, heads):
    count, first, second = blocks.shape
    if kind == "rows":
        return blocks.reshape(count * first, second)
    if kind == "cols":
        return blocks.transpose(1, 0, 2).reshape(first, count * second)
    if kind == "ih":
        parts = blocks.reshape(items, heads, first, second).transpose(0, 2, 1, 3)
        return parts.reshape(items * first, heads * second)
    parts = blocks.reshape(items, heads, first, second).transpose(1, 2, 0, 3)
    return parts.reshape(heads * first, items * second)


def disassemble(whole, kind, items, heads):
    count = items * heads
    rows, cols = whole.shape
    if kind == "rows":
        return whole.reshape(count, rows // count, cols)
    if kind == "cols":
        return whole.reshape(rows, count, cols // count).transpose(1, 0, 2)
    if kind == "ih":
        parts = whole.reshape(items, rows // items, heads, cols // heads).transpose(0, 2, 1, 3)
        return parts.reshape(count, rows // items, cols // heads)
    parts = whole.reshape(heads, rows // heads, items, cols // items).transpose(2, 0, 1, 3)
    return parts.reshape(count, rows // heads, cols // items)


WEIGHT_KINDS = (
    "rows",
    "cols",
    "cols",
    "rows",
    "ih",
    "hi",
    "ih",
    "ih",
    "ih",
    "hi",
    "ih",
    "hi",
)


WIDTH = 1024
ROW_TILE = 16


def to_rows(flat):
    count, size = flat.shape
    rows = -(-size // (WIDTH * ROW_TILE)) * ROW_TILE
    flat = jnp.pad(flat, ((0, 0), (0, rows * WIDTH - size)))
    return flat.reshape(count, rows, WIDTH)


def pack(pieces):
    blocks, places, row = [], [], 0
    for piece in pieces:
        block = to_rows(piece)
        places.append((row, piece.shape[1]))
        blocks.append(block)
        row += block.shape[1]
    extra = packed_rows(row) - row
    if extra:
        blocks.append(jnp.zeros((pieces[0].shape[0], extra, WIDTH), pieces[0].dtype))
    return jnp.concatenate(blocks, axis=1), places


def packed_rows(rows):
    return -(-rows // 128) * 128


def unpack(packed, place):
    row, size = place
    rows = -(-size // WIDTH)
    return packed[:, row : row + rows, :].reshape(packed.shape[0], rows * WIDTH)[:, :size]


def gather_weights(weights, gains, items, heads):
    count = items * heads
    pieces = [rounded(w).reshape(1, -1) for w in weights]
    pieces.append(rounded(jnp.concatenate(gains)).reshape(1, -1))
    packed, places = pack(pieces)
    local_rows = packed.shape[1]
    gathered = lax.all_gather(packed[0], ALL, axis=0, tiled=True).reshape(count, local_rows, WIDTH)
    whole_weights = []
    for w, kind, place in zip(weights, WEIGHT_KINDS, places):
        blocks = unpack(gathered, place).reshape((count,) + w.shape)
        whole_weights.append(assemble(blocks, kind, items, heads))
    gain_blocks = unpack(gathered, places[-1]).reshape(count, len(gains), -1)
    whole_gains = [widened(gain_blocks[:, k, :].reshape(-1)) for k in range(len(gains))]
    return whole_weights, whole_gains


def reduce_grads(weight_grads, gain_grads, items, heads):
    count = items * heads
    pieces = []
    for g, kind in zip(weight_grads, WEIGHT_KINDS):
        pieces.append(rounded(disassemble(g, kind, items, heads)).reshape(count, -1))
    gain_stack = jnp.stack([g.reshape(count, -1) for g in gain_grads], axis=1)
    pieces.append(rounded(gain_stack).reshape(count, -1))
    packed, places = pack(pieces)
    local_rows = packed.shape[1]
    mine = lax.psum_scatter(
        packed.reshape(count * local_rows, WIDTH), ALL, scatter_dimension=0, tiled=True
    ).reshape(1, local_rows, WIDTH)
    out = [widened(unpack(mine, place)[0]) for place in places[:-1]]
    gain_part = widened(unpack(mine, places[-1])[0]).reshape(len(gain_grads), -1)
    out += [gain_part[k] for k in range(len(gain_grads))]
    return out


def mlp_block(residual, gain_vec, up_w, down_w):
    normed = rounded(norm_rows(residual, gain_vec))
    before = product(normed, up_w)
    hidden = rounded(jax.nn.gelu(before))
    return residual + product(hidden, down_w), (normed, before, hidden)


def mlp_block_back(residual, gain_vec, up_w, down_w, saved, grad_out):
    normed, before, hidden = saved
    grad_round = rounded(grad_out)
    grad_down = product_tn(hidden, grad_round)
    grad_hidden = product_nt(grad_round, down_w)
    unused, gelu_back = jax.vjp(jax.nn.gelu, before)
    grad_before = rounded(gelu_back(grad_hidden)[0])
    grad_up = product_tn(normed, grad_before)
    grad_normed = product_nt(grad_before, up_w)
    grad_residual, grad_gain = norm_backward(residual, gain_vec, grad_normed)
    return grad_out + grad_residual, grad_up, grad_down, grad_gain


def exchange_rows(rows, split):
    if split == 1:
        return [rows]
    heads = lax.axis_size("heads")
    out = [rows]
    for shift in range(1, split):
        pairs = []
        for h in range(heads):
            base, pos = (h // split) * split, h % split
            pairs.append((h, base + (pos - shift) % split))
        out.append(lax.ppermute(rows, "heads", pairs))
    return out


def return_rows(parts, split):
    total = parts[0]
    heads = lax.axis_size("heads")
    for shift in range(1, split):
        pairs = []
        for h in range(heads):
            base, pos = (h // split) * split, h % split
            pairs.append((h, base + (pos + shift) % split))
        total = total + lax.ppermute(parts[shift], "heads", pairs)
    return total


def attention_block(residual, gain_vec, weight_set, split):
    query_w, key_w, value_w, out_w = weight_set
    rows = residual.shape[0]
    heads_n = query_w.shape[1] // HEAD
    normed = rounded(norm_rows(residual, gain_vec))
    query_rows = rounded(product(normed, query_w))
    key_rows = rounded(product(normed, key_w))
    value_rows = rounded(product(normed, value_w))
    key_all = jnp.concatenate(exchange_rows(key_rows, split), axis=0)
    value_all = jnp.concatenate(exchange_rows(value_rows, split), axis=0)
    keys = key_all.shape[0]
    q4 = query_rows.reshape(rows, heads_n, HEAD)
    k4 = key_all.reshape(keys, heads_n, HEAD)
    v4 = value_all.reshape(keys, heads_n, HEAD)
    scores = jnp.einsum("qhd,khd->hqk", q4, k4, preferred_element_type=jnp.float32) * (
        1.0 / math.sqrt(HEAD)
    )
    row_top = jnp.max(scores, axis=-1, keepdims=True)
    raw_weights = jnp.exp(scores - row_top)
    row_total = jnp.sum(raw_weights, axis=-1, keepdims=True)
    weights = raw_weights / row_total
    mixed = jnp.einsum("hqk,khd->qhd", rounded(weights), v4, preferred_element_type=jnp.float32)
    mixed = rounded(mixed.reshape(rows, heads_n * HEAD))
    saved = (normed, q4, k4, v4, weights, mixed)
    return residual + product(mixed, out_w), saved


def attention_block_back(residual, gain_vec, weight_set, split, saved, grad_out):
    query_w, key_w, value_w, out_w = weight_set
    normed, q4, k4, v4, weights, mixed = saved
    rows = residual.shape[0]
    keys = k4.shape[0]
    scale = 1.0 / math.sqrt(HEAD)
    grad_round = rounded(grad_out)
    grad_out_w = product_tn(mixed, grad_round)
    grad_mixed = rounded(product_nt(grad_round, out_w)).reshape(q4.shape)
    grad_value = jnp.einsum(
        "hqk,qhd->khd", rounded(weights), grad_mixed, preferred_element_type=jnp.float32
    ).reshape(keys, -1)
    grad_weights = jnp.einsum("qhd,khd->hqk", grad_mixed, v4, preferred_element_type=jnp.float32)
    grad_scores = weights * (grad_weights - jnp.sum(grad_weights * weights, axis=-1, keepdims=True))
    grad_scores = rounded(grad_scores)
    grad_query = jnp.einsum("hqk,khd->qhd", grad_scores, k4, preferred_element_type=jnp.float32)
    grad_query = rounded((grad_query * scale).reshape(rows, -1))
    grad_key = jnp.einsum("hqk,qhd->khd", grad_scores, q4, preferred_element_type=jnp.float32)
    grad_key = (grad_key * scale).reshape(keys, -1)
    if split > 1:
        grad_key = return_rows(jnp.split(grad_key, split, axis=0), split)
        grad_value = return_rows(jnp.split(grad_value, split, axis=0), split)
    grad_key = rounded(grad_key)
    grad_value = rounded(grad_value)
    grad_query_w = product_tn(normed, grad_query)
    grad_key_w = product_tn(normed, grad_key)
    grad_value_w = product_tn(normed, grad_value)
    grad_normed = (
        product_nt(grad_query, query_w)
        + product_nt(grad_key, key_w)
        + product_nt(grad_value, value_w)
    )
    grad_residual, grad_gain = norm_backward(residual, gain_vec, grad_normed)
    return (grad_out + grad_residual, grad_query_w, grad_key_w, grad_value_w, grad_out_w, grad_gain)


def pixel_window(pixels, item_ids, item):
    count = pixels.shape[1]
    width = min(count, -(-PIX_MOST // LANE) * LANE + LANE)
    start = jnp.sum((item_ids < item).astype(jnp.int32))
    first = jnp.clip((start // LANE) * LANE, 0, count - width)
    window = lax.dynamic_slice_in_dim(pixels, first, width, axis=1)
    ids = lax.dynamic_slice_in_dim(item_ids, first, width, axis=0)
    return window, ids == item


def cross_block(residual, gain_vec, query_w, key_w, value_w, out_w, pixel_norm, allowed):
    scale = 1.0 / math.sqrt(query_w.shape[1])
    normed = rounded(norm_rows(residual, gain_vec))
    query_rows = rounded(product(normed, query_w))
    query_keyed = rounded(product_nt(query_rows, key_w) * scale)
    scores = jnp.where(allowed[None, :], product(query_keyed, pixel_norm), MASKED)
    row_top = jnp.max(scores, axis=-1, keepdims=True)
    raw_weights = jnp.exp(scores - row_top)
    row_total = jnp.sum(raw_weights, axis=-1, keepdims=True)
    weights = raw_weights / row_total
    weights_low = rounded(weights)
    pixel_mix = product_nt(weights_low, pixel_norm)
    mixed = rounded(split_product(pixel_mix, value_w))
    saved = (normed, query_rows, weights, pixel_mix, mixed)
    return residual + product(mixed, out_w), saved


def cross_block_back(
    residual, gain_vec, query_w, key_w, value_w, out_w, pixel_norm, saved, grad_out
):
    normed, query_rows, weights, pixel_mix, mixed = saved
    scale = 1.0 / math.sqrt(query_w.shape[1])
    grad_round = rounded(grad_out)
    grad_out_w = product_tn(mixed, grad_round)
    grad_mixed = rounded(product_nt(grad_round, out_w))
    grad_keyed = rounded(product_nt(grad_mixed, value_w))
    grad_weights = product(grad_keyed, pixel_norm)
    grad_scores = weights * (grad_weights - jnp.sum(grad_weights * weights, axis=-1, keepdims=True))
    grad_scores = rounded(grad_scores)
    score_mix = product_nt(grad_scores, pixel_norm)
    grad_query = rounded(split_product(score_mix, key_w) * scale)
    grad_query_w = product_tn(normed, grad_query)
    grad_key_w = split_product(score_mix, query_rows, product_tn) * scale
    grad_value_w = split_product(pixel_mix, grad_mixed, product_tn)
    grad_normed = product_nt(grad_query, query_w)
    grad_residual, grad_gain = norm_backward(residual, gain_vec, grad_normed)
    return (grad_out + grad_residual, grad_query_w, grad_key_w, grad_value_w, grad_out_w, grad_gain)


def local(latents, pixels, pixel_item, cotangent, *params):
    weights, gains = params[:12], params[12:]
    items = lax.axis_size("items")
    heads = lax.axis_size("heads")
    rows = latents.shape[0]
    split = max(1, NLAT // rows)
    (
        query_cross,
        key_cross,
        value_cross,
        out_cross,
        up_cross,
        down_cross,
        query_self,
        key_self,
        value_self,
        out_self,
        up_self,
        down_self,
    ), gain_list = gather_weights(weights, gains, items, heads)
    attention_set = (query_self, key_self, value_self, out_self)

    item = (lax.axis_index("heads") * rows) // NLAT
    window, allowed = pixel_window(pixels, pixel_item[0], item)
    pixel_norm = rounded(norm_pixels(widened(window)))

    start_rows = widened(latents)
    after_cross, saved_cross = cross_block(
        start_rows, gain_list[0], query_cross, key_cross, value_cross, out_cross, pixel_norm, allowed
    )
    after_mlp_one, saved_mlp_one = mlp_block(after_cross, gain_list[1], up_cross, down_cross)
    after_self, saved_self = attention_block(after_mlp_one, gain_list[2], attention_set, split)
    final_rows, saved_mlp_two = mlp_block(after_self, gain_list[3], up_self, down_self)

    grad_final = widened(cotangent)
    grad_after_self, grad_self_up, grad_self_down, grad_gain_four = mlp_block_back(
        after_self, gain_list[3], up_self, down_self, saved_mlp_two, grad_final
    )
    (
        grad_after_mlp,
        grad_self_query,
        grad_self_key,
        grad_self_value,
        grad_self_out,
        grad_gain_three,
    ) = attention_block_back(
        after_mlp_one, gain_list[2], attention_set, split, saved_self, grad_after_self
    )
    grad_after_cross, grad_cross_up, grad_cross_down, grad_gain_two = mlp_block_back(
        after_cross, gain_list[1], up_cross, down_cross, saved_mlp_one, grad_after_mlp
    )
    (
        latents_grad,
        grad_cross_query,
        grad_cross_key,
        grad_cross_value,
        grad_cross_out,
        grad_gain_one,
    ) = cross_block_back(
        start_rows,
        gain_list[0],
        query_cross,
        key_cross,
        value_cross,
        out_cross,
        pixel_norm,
        saved_cross,
        grad_after_cross,
    )
    weight_grads = (
        grad_cross_query,
        grad_cross_key,
        grad_cross_value,
        grad_cross_out,
        grad_cross_up,
        grad_cross_down,
        grad_self_query,
        grad_self_key,
        grad_self_value,
        grad_self_out,
        grad_self_up,
        grad_self_down,
    )
    gain_grads = (grad_gain_one, grad_gain_two, grad_gain_three, grad_gain_four)
    reduced = reduce_grads(weight_grads, gain_grads, items, heads)
    shaped = [r.reshape(w.shape) for r, w in zip(reduced[:12], weights)]
    shaped += [r.reshape(g.shape) for r, g in zip(reduced[12:], gains)]
    return (rounded(final_rows), latents_grad, *shaped)


def solution(mesh):
    weight_specs = (
        P(ALL, None),
        P(None, ALL),
        P(None, ALL),
        P(ALL, None),
        P("items", "heads"),
        P("heads", "items"),
        P("items", "heads"),
        P("items", "heads"),
        P("items", "heads"),
        P("heads", "items"),
        P("items", "heads"),
        P("heads", "items"),
    )
    gain_specs = (P(ALL),) * 4
    placed = (P(ALL, None), P(None, "items"), P("items", None), P(ALL, None)) + weight_specs + gain_specs
    return jax.shard_map(
        local,
        mesh=mesh,
        in_specs=placed,
        out_specs=(P(ALL, None), P(ALL, None)) + weight_specs + gain_specs,
        check_vma=False,
    )
```

```python
import math

import jax
import jax.numpy as jnp
from jax import lax
from jax.sharding import PartitionSpec as P

HEAD = 128
NLAT = 512
PIX_MOST = 6144
LANE = 128

EPSILON = 1e-05
MASKED = -1e30
ALL = ("items", "heads")


def rounded(values):
    return values.astype(jnp.bfloat16)


def widened(values):
    return values.astype(jnp.float32)


def product(left_side, right_side):
    return jnp.dot(left_side, right_side, preferred_element_type=jnp.float32)


def product_tn(left_side, right_side):
    return lax.dot_general(
        left_side, right_side, (((0,), (0,)), ((), ())), preferred_element_type=jnp.float32
    )


def product_nt(left_side, right_side):
    return lax.dot_general(
        left_side, right_side, (((1,), (1,)), ((), ())), preferred_element_type=jnp.float32
    )


def split_parts(values):
    high = rounded(values)
    return high, rounded(values - widened(high))


def split_product(left_f32, right_bf16, form=product):
    high, low = split_parts(left_f32)
    return form(high, right_bf16) + form(low, right_bf16)


def split_product_right(left_bf16, right_f32):
    high, low = split_parts(right_f32)
    return product_tn(left_bf16, high) + product_tn(left_bf16, low)


def norm_rows(values, gain_vec):
    centre = values - jnp.mean(values, axis=-1, keepdims=True)
    spread = jnp.mean(centre * centre, axis=-1, keepdims=True)
    return centre * lax.rsqrt(spread + EPSILON) * gain_vec


def norm_pixels(values):
    centre = values - jnp.mean(values, axis=0, keepdims=True)
    spread = jnp.mean(centre * centre, axis=0, keepdims=True)
    return centre * lax.rsqrt(spread + EPSILON)


def norm_backward(residual, gain_vec, grad_normed):
    unused, norm_back = jax.vjp(norm_rows, residual, gain_vec)
    return norm_back(grad_normed)


def assemble(blocks, kind, items, heads):
    count, first, second = blocks.shape
    if kind in ("rows", "cols"):
        return blocks.reshape(count * first, second)
    if kind == "ih":
        parts = blocks.reshape(items, heads, first, second).transpose(0, 2, 1, 3)
        return parts.reshape(items * first, heads * second)
    parts = blocks.reshape(items, heads, first, second).transpose(1, 2, 0, 3)
    return parts.reshape(heads * first, items * second)


def disassemble(whole, kind, items, heads):
    count = items * heads
    rows, cols = whole.shape
    if kind in ("rows", "cols"):
        return whole.reshape(count, rows // count, cols)
    if kind == "ih":
        parts = whole.reshape(items, rows // items, heads, cols // heads).transpose(0, 2, 1, 3)
        return parts.reshape(count, rows // items, cols // heads)
    parts = whole.reshape(heads, rows // heads, items, cols // items).transpose(2, 0, 1, 3)
    return parts.reshape(count, rows // heads, cols // items)


WEIGHT_KINDS = (
    "rows",
    "cols",
    "cols",
    "rows",
    "ih",
    "hi",
    "ih",
    "ih",
    "ih",
    "hi",
    "ih",
    "hi",
)


PANEL = 128
ROW_TILE = 16
ROW_GROUP = 48


def panels(block):
    count, first, second = block.shape
    width = -(-second // PANEL) * PANEL
    if width != second:
        block = jnp.pad(block, ((0, 0), (0, 0), (0, width - second)))
    parts = block.reshape(count, first, width // PANEL, PANEL).transpose(0, 2, 1, 3)
    return parts.reshape(count, (width // PANEL) * first, PANEL)


def unpanels(rows, first, second):
    count = rows.shape[0]
    width = -(-second // PANEL) * PANEL
    parts = rows.reshape(count, width // PANEL, first, PANEL).transpose(0, 2, 1, 3)
    return parts.reshape(count, first, width)[:, :, :second]


def pack(pieces):
    blocks, places, row = [], [], 0
    for piece in pieces:
        block = panels(piece)
        extra = -block.shape[1] % ROW_TILE
        if extra:
            block = jnp.pad(block, ((0, 0), (0, extra), (0, 0)))
        places.append((row, piece.shape[1], piece.shape[2]))
        blocks.append(block)
        row += block.shape[1]
    extra = -row % ROW_GROUP
    if extra:
        blocks.append(jnp.zeros((pieces[0].shape[0], extra, PANEL), pieces[0].dtype))
    return jnp.concatenate(blocks, axis=1), places


def unpack(packed, place):
    row, first, second = place
    count = -(-second // PANEL) * first
    return unpanels(packed[:, row : row + count, :], first, second)


def local_block(w, kind):
    return (w.T if kind == "cols" else w)[None]


def gather_weights(weights, gains, items, heads):
    count = items * heads
    pieces = [rounded(local_block(w, kind)) for w, kind in zip(weights, WEIGHT_KINDS)]
    pieces.append(rounded(jnp.concatenate(gains)).reshape(1, 1, -1))
    packed, places = pack(pieces)
    local_rows = packed.shape[1]
    gathered = lax.all_gather(packed[0], ALL, axis=0, tiled=True).reshape(count, local_rows, PANEL)
    whole_weights = []
    for kind, place in zip(WEIGHT_KINDS, places):
        whole_weights.append(assemble(unpack(gathered, place), kind, items, heads))
    gain_blocks = unpack(gathered, places[-1]).reshape(count, len(gains), -1)
    whole_gains = [widened(gain_blocks[:, k, :].reshape(-1)) for k in range(len(gains))]
    return whole_weights, whole_gains


def reduce_grads(weight_grads, gain_grads, items, heads):
    count = items * heads
    pieces = []
    for g, kind in zip(weight_grads, WEIGHT_KINDS):
        pieces.append(rounded(disassemble(g, kind, items, heads)))
    gain_stack = jnp.stack([g.reshape(count, -1) for g in gain_grads], axis=1)
    pieces.append(rounded(gain_stack).reshape(count, 1, -1))
    packed, places = pack(pieces)
    local_rows = packed.shape[1]
    mine = lax.psum_scatter(
        packed.reshape(count * local_rows, PANEL), ALL, scatter_dimension=0, tiled=True
    ).reshape(1, local_rows, PANEL)
    out = []
    for kind, place in zip(WEIGHT_KINDS, places):
        block = widened(unpack(mine, place)[0])
        out.append(block.T if kind == "cols" else block)
    gain_part = widened(unpack(mine, places[-1])[0]).reshape(len(gain_grads), -1)
    out += [gain_part[k] for k in range(len(gain_grads))]
    return out


def mlp_block(residual, gain_vec, up_w, down_w):
    normed = rounded(norm_rows(residual, gain_vec))
    before = product(normed, up_w)
    hidden = rounded(jax.nn.gelu(before))
    return residual + product(hidden, down_w), (normed, before, hidden)


def mlp_block_back(residual, gain_vec, up_w, down_w, saved, grad_out):
    normed, before, hidden = saved
    grad_round = rounded(grad_out)
    grad_down = product_tn(hidden, grad_round)
    grad_hidden = product_nt(grad_round, down_w)
    unused, gelu_back = jax.vjp(jax.nn.gelu, before)
    grad_before = rounded(gelu_back(grad_hidden)[0])
    grad_up = product_tn(normed, grad_before)
    grad_normed = product_nt(grad_before, up_w)
    grad_residual, grad_gain = norm_backward(residual, gain_vec, grad_normed)
    return grad_out + grad_residual, grad_up, grad_down, grad_gain


def exchange_rows(rows, split):
    if split == 1:
        return [rows]
    heads = lax.axis_size("heads")
    out = [rows]
    for shift in range(1, split):
        pairs = []
        for h in range(heads):
            base, pos = (h // split) * split, h % split
            pairs.append((h, base + (pos - shift) % split))
        out.append(lax.ppermute(rows, "heads", pairs))
    return out


def return_rows(parts, split):
    total = parts[0]
    heads = lax.axis_size("heads")
    for shift in range(1, split):
        pairs = []
        for h in range(heads):
            base, pos = (h // split) * split, h % split
            pairs.append((h, base + (pos + shift) % split))
        total = total + lax.ppermute(parts[shift], "heads", pairs)
    return total


def attention_block(residual, gain_vec, weight_set, split):
    query_w, key_w, value_w, out_w = weight_set
    rows = residual.shape[0]
    heads_n = query_w.shape[1] // HEAD
    normed = rounded(norm_rows(residual, gain_vec))
    query_rows = rounded(product(normed, query_w))
    key_rows = rounded(product(normed, key_w))
    value_rows = rounded(product(normed, value_w))
    key_all = jnp.concatenate(exchange_rows(key_rows, split), axis=0)
    value_all = jnp.concatenate(exchange_rows(value_rows, split), axis=0)
    keys = key_all.shape[0]
    q4 = query_rows.reshape(rows, heads_n, HEAD)
    k4 = key_all.reshape(keys, heads_n, HEAD)
    v4 = value_all.reshape(keys, heads_n, HEAD)
    scores = jnp.einsum("qhd,khd->hqk", q4, k4, preferred_element_type=jnp.float32) * (
        1.0 / math.sqrt(HEAD)
    )
    row_top = jnp.max(scores, axis=-1, keepdims=True)
    raw_weights = jnp.exp(scores - row_top)
    row_total = jnp.sum(raw_weights, axis=-1, keepdims=True)
    weights = raw_weights / row_total
    mixed = jnp.einsum("hqk,khd->qhd", rounded(weights), v4, preferred_element_type=jnp.float32)
    mixed = rounded(mixed.reshape(rows, heads_n * HEAD))
    saved = (normed, q4, k4, v4, weights, mixed)
    return residual + product(mixed, out_w), saved


def attention_block_back(residual, gain_vec, weight_set, split, saved, grad_out):
    query_w, key_w, value_w, out_w = weight_set
    normed, q4, k4, v4, weights, mixed = saved
    rows = residual.shape[0]
    keys = k4.shape[0]
    scale = 1.0 / math.sqrt(HEAD)
    grad_round = rounded(grad_out)
    grad_out_w = product_tn(mixed, grad_round)
    grad_mixed = rounded(product_nt(grad_round, out_w)).reshape(q4.shape)
    grad_value = jnp.einsum(
        "hqk,qhd->khd", rounded(weights), grad_mixed, preferred_element_type=jnp.float32
    ).reshape(keys, -1)
    grad_weights = jnp.einsum("qhd,khd->hqk", grad_mixed, v4, preferred_element_type=jnp.float32)
    grad_scores = weights * (grad_weights - jnp.sum(grad_weights * weights, axis=-1, keepdims=True))
    grad_scores = rounded(grad_scores)
    grad_query = jnp.einsum("hqk,khd->qhd", grad_scores, k4, preferred_element_type=jnp.float32)
    grad_query = rounded((grad_query * scale).reshape(rows, -1))
    grad_key = jnp.einsum("hqk,qhd->khd", grad_scores, q4, preferred_element_type=jnp.float32)
    grad_key = (grad_key * scale).reshape(keys, -1)
    if split > 1:
        grad_key = return_rows(jnp.split(grad_key, split, axis=0), split)
        grad_value = return_rows(jnp.split(grad_value, split, axis=0), split)
    grad_key = rounded(grad_key)
    grad_value = rounded(grad_value)
    grad_query_w = product_tn(normed, grad_query)
    grad_key_w = product_tn(normed, grad_key)
    grad_value_w = product_tn(normed, grad_value)
    grad_normed = (
        product_nt(grad_query, query_w)
        + product_nt(grad_key, key_w)
        + product_nt(grad_value, value_w)
    )
    grad_residual, grad_gain = norm_backward(residual, gain_vec, grad_normed)
    return (grad_out + grad_residual, grad_query_w, grad_key_w, grad_value_w, grad_out_w, grad_gain)


def pixel_window(pixels, item_ids, item):
    count = pixels.shape[1]
    width = min(count, -(-PIX_MOST // LANE) * LANE + LANE)
    start = jnp.sum((item_ids < item).astype(jnp.int32))
    first = jnp.clip((start // LANE) * LANE, 0, count - width)
    window = lax.dynamic_slice_in_dim(pixels, first, width, axis=1)
    ids = lax.dynamic_slice_in_dim(item_ids, first, width, axis=0)
    return window, ids == item


def cross_block(residual, gain_vec, query_w, key_w, value_w, out_w, pixel_norm, allowed):
    scale = 1.0 / math.sqrt(query_w.shape[1])
    normed = rounded(norm_rows(residual, gain_vec))
    query_rows = rounded(product(normed, query_w))
    query_keyed = rounded(product(query_rows, key_w) * scale)
    scores = jnp.where(allowed[None, :], product(query_keyed, pixel_norm), MASKED)
    row_top = jnp.max(scores, axis=-1, keepdims=True)
    raw_weights = jnp.exp(scores - row_top)
    row_total = jnp.sum(raw_weights, axis=-1, keepdims=True)
    weights = raw_weights / row_total
    weights_low = rounded(weights)
    pixel_mix = product_nt(weights_low, pixel_norm)
    mixed = rounded(split_product(pixel_mix, value_w, product_nt))
    saved = (normed, query_rows, weights, pixel_mix, mixed)
    return residual + product(mixed, out_w), saved


def cross_block_back(
    residual, gain_vec, query_w, key_w, value_w, out_w, pixel_norm, saved, grad_out
):
    normed, query_rows, weights, pixel_mix, mixed = saved
    scale = 1.0 / math.sqrt(query_w.shape[1])
    grad_round = rounded(grad_out)
    grad_out_w = product_tn(mixed, grad_round)
    grad_mixed = rounded(product_nt(grad_round, out_w))
    grad_keyed = rounded(product(grad_mixed, value_w))
    grad_weights = product(grad_keyed, pixel_norm)
    grad_scores = weights * (grad_weights - jnp.sum(grad_weights * weights, axis=-1, keepdims=True))
    grad_scores = rounded(grad_scores)
    score_mix = product_nt(grad_scores, pixel_norm)
    grad_query = rounded(split_product(score_mix, key_w, product_nt) * scale)
    grad_query_w = product_tn(normed, grad_query)
    grad_key_w = split_product_right(query_rows, score_mix) * scale
    grad_value_w = split_product_right(grad_mixed, pixel_mix)
    grad_normed = product_nt(grad_query, query_w)
    grad_residual, grad_gain = norm_backward(residual, gain_vec, grad_normed)
    return (grad_out + grad_residual, grad_query_w, grad_key_w, grad_value_w, grad_out_w, grad_gain)


def local(latents, pixels, pixel_item, cotangent, *params):
    weights, gains = params[:12], params[12:]
    items = lax.axis_size("items")
    heads = lax.axis_size("heads")
    rows = latents.shape[0]
    split = max(1, NLAT // rows)
    (
        query_cross,
        key_cross,
        value_cross,
        out_cross,
        up_cross,
        down_cross,
        query_self,
        key_self,
        value_self,
        out_self,
        up_self,
        down_self,
    ), gain_list = gather_weights(weights, gains, items, heads)
    attention_set = (query_self, key_self, value_self, out_self)

    item = (lax.axis_index("heads") * rows) // NLAT
    window, allowed = pixel_window(pixels, pixel_item[0], item)
    pixel_norm = rounded(norm_pixels(widened(window)))

    start_rows = widened(latents)
    after_cross, saved_cross = cross_block(
        start_rows, gain_list[0], query_cross, key_cross, value_cross, out_cross, pixel_norm, allowed
    )
    after_mlp_one, saved_mlp_one = mlp_block(after_cross, gain_list[1], up_cross, down_cross)
    after_self, saved_self = attention_block(after_mlp_one, gain_list[2], attention_set, split)
    final_rows, saved_mlp_two = mlp_block(after_self, gain_list[3], up_self, down_self)

    grad_final = widened(cotangent)
    grad_after_self, grad_self_up, grad_self_down, grad_gain_four = mlp_block_back(
        after_self, gain_list[3], up_self, down_self, saved_mlp_two, grad_final
    )
    (
        grad_after_mlp,
        grad_self_query,
        grad_self_key,
        grad_self_value,
        grad_self_out,
        grad_gain_three,
    ) = attention_block_back(
        after_mlp_one, gain_list[2], attention_set, split, saved_self, grad_after_self
    )
    grad_after_cross, grad_cross_up, grad_cross_down, grad_gain_two = mlp_block_back(
        after_cross, gain_list[1], up_cross, down_cross, saved_mlp_one, grad_after_mlp
    )
    (
        latents_grad,
        grad_cross_query,
        grad_cross_key,
        grad_cross_value,
        grad_cross_out,
        grad_gain_one,
    ) = cross_block_back(
        start_rows,
        gain_list[0],
        query_cross,
        key_cross,
        value_cross,
        out_cross,
        pixel_norm,
        saved_cross,
        grad_after_cross,
    )
    weight_grads = (
        grad_cross_query,
        grad_cross_key,
        grad_cross_value,
        grad_cross_out,
        grad_cross_up,
        grad_cross_down,
        grad_self_query,
        grad_self_key,
        grad_self_value,
        grad_self_out,
        grad_self_up,
        grad_self_down,
    )
    gain_grads = (grad_gain_one, grad_gain_two, grad_gain_three, grad_gain_four)
    reduced = reduce_grads(weight_grads, gain_grads, items, heads)
    shaped = [r.reshape(w.shape) for r, w in zip(reduced[:12], weights)]
    shaped += [r.reshape(g.shape) for r, g in zip(reduced[12:], gains)]
    return (rounded(final_rows), latents_grad, *shaped)


def solution(mesh):
    weight_specs = (
        P(ALL, None),
        P(None, ALL),
        P(None, ALL),
        P(ALL, None),
        P("items", "heads"),
        P("heads", "items"),
        P("items", "heads"),
        P("items", "heads"),
        P("items", "heads"),
        P("heads", "items"),
        P("items", "heads"),
        P("heads", "items"),
    )
    gain_specs = (P(ALL),) * 4
    placed = (P(ALL, None), P(None, "items"), P("items", None), P(ALL, None)) + weight_specs + gain_specs
    return jax.shard_map(
        local,
        mesh=mesh,
        in_specs=placed,
        out_specs=(P(ALL, None), P(ALL, None)) + weight_specs + gain_specs,
        check_vma=False,
    )
```

```python
import math

import jax
import jax.numpy as jnp
from jax import lax
from jax.sharding import PartitionSpec as P

HEAD = 128
NLAT = 512
PIX_MOST = 6144
LANE = 128

EPSILON = 1e-05
MASKED = -1e30
ALL = ("items", "heads")


def rounded(values):
    return values.astype(jnp.bfloat16)


def widened(values):
    return values.astype(jnp.float32)


def product(left_side, right_side):
    return jnp.dot(left_side, right_side, preferred_element_type=jnp.float32)


def product_tn(left_side, right_side):
    return lax.dot_general(
        left_side, right_side, (((0,), (0,)), ((), ())), preferred_element_type=jnp.float32
    )


def product_nt(left_side, right_side):
    return lax.dot_general(
        left_side, right_side, (((1,), (1,)), ((), ())), preferred_element_type=jnp.float32
    )


def split_parts(values):
    high = rounded(values)
    return high, rounded(values - widened(high))


def split_apply_t(values_f32, weight):
    high, low = split_parts(values_f32)
    return apply_t(high, weight) + apply_t(low, weight)


def norm_rows(values, gain_vec):
    centre = values - jnp.mean(values, axis=-1, keepdims=True)
    spread = jnp.mean(centre * centre, axis=-1, keepdims=True)
    return centre * lax.rsqrt(spread + EPSILON) * gain_vec


def norm_pixels(values):
    centre = values - jnp.mean(values, axis=0, keepdims=True)
    spread = jnp.mean(centre * centre, axis=0, keepdims=True)
    return centre * lax.rsqrt(spread + EPSILON)


def norm_backward(residual, gain_vec, grad_normed):
    unused, norm_back = jax.vjp(norm_rows, residual, gain_vec)
    return norm_back(grad_normed)


WEIGHT_KINDS = (
    "rows",
    "cols",
    "cols",
    "rows",
    "ih",
    "hi",
    "ih",
    "ih",
    "ih",
    "hi",
    "ih",
    "hi",
)

PANEL = 128
ROW_TILE = 16
ROW_GROUP = 48


def contract(left, right, left_dims, right_dims):
    return lax.dot_general(
        left, right, ((left_dims, right_dims), ((), ())), preferred_element_type=jnp.float32
    )


def lane_pad(values, width):
    panels = -(-width // PANEL)
    if panels * PANEL != width:
        pad = [(0, 0)] * (values.ndim - 1) + [(0, panels * PANEL - width)]
        values = jnp.pad(values, pad)
    return values.reshape(values.shape[:-1] + (panels, PANEL))


def lane_cut(values, width):
    values = values.reshape(values.shape[:-2] + (-1,))
    return values if values.shape[-1] == width else values[..., :width]


def local_panels(block):
    rows, width = block.shape
    parts = lane_pad(block, width).transpose(1, 0, 2)
    return parts.reshape(-1, PANEL)


def padded_rows(rows):
    return -(-rows // ROW_TILE) * ROW_TILE


def local_shape(w, kind):
    return (w.shape[1], w.shape[0]) if kind == "cols" else w.shape


def make_weight(piece, kind, shape, items, heads):
    rows, width = shape
    panels = -(-width // PANEL)
    blocks = piece[:, : panels * rows, :].reshape(items * heads, panels, rows, PANEL)
    if kind in ("ih", "hi"):
        blocks = blocks.reshape(items, heads, panels, rows, PANEL)
    return kind, blocks, width


def apply(values, weight):
    kind, blocks, width = weight
    count = values.shape[0]
    if kind in ("rows", "cols"):
        devices, panels, rows, lanes = blocks.shape
        out = contract(values.reshape(count, devices, rows), blocks, (1, 2), (0, 2))
        return lane_cut(out, width)
    items, heads, panels, rows, lanes = blocks.shape
    if kind == "ih":
        out = contract(values.reshape(count, items, rows), blocks, (1, 2), (0, 3))
    else:
        out = contract(values.reshape(count, heads, rows), blocks, (1, 2), (1, 3))
    return lane_cut(out, width).reshape(count, -1)


def apply_t(values, weight):
    kind, blocks, width = weight
    count = values.shape[0]
    if kind in ("rows", "cols"):
        devices, panels, rows, lanes = blocks.shape
        out = contract(lane_pad(values, width), blocks, (1, 2), (1, 3))
        return out.reshape(count, devices * rows)
    items, heads, panels, rows, lanes = blocks.shape
    if kind == "ih":
        spread = lane_pad(values.reshape(count, heads, width), width)
        out = contract(spread, blocks, (1, 2, 3), (1, 2, 4))
        return out.reshape(count, items * rows)
    spread = lane_pad(values.reshape(count, items, width), width)
    out = contract(spread, blocks, (1, 2, 3), (0, 2, 4))
    return out.reshape(count, heads * rows)


def grad_blocks(values, grads, weight):
    kind, blocks, width = weight
    count = values.shape[0]
    if kind in ("rows", "cols"):
        devices, panels, rows, lanes = blocks.shape
        out = contract(values.reshape(count, devices, rows), lane_pad(grads, width), (0,), (0,))
        out = out.transpose(0, 2, 1, 3)
    else:
        items, heads, panels, rows, lanes = blocks.shape
        devices = items * heads
        if kind == "ih":
            spread = lane_pad(grads.reshape(count, heads, width), width)
            out = contract(values.reshape(count, items, rows), spread, (0,), (0,))
            out = out.transpose(0, 2, 3, 1, 4)
        else:
            spread = lane_pad(grads.reshape(count, items, width), width)
            out = contract(values.reshape(count, heads, rows), spread, (0,), (0,))
            out = out.transpose(2, 0, 3, 1, 4)
    return out.reshape(devices, -1, PANEL)


def split_grad_blocks(values, grads_f32, weight):
    high, low = split_parts(grads_f32)
    return grad_blocks(values, high, weight) + grad_blocks(values, low, weight)


def pad_rows(block, rows):
    extra = rows - block.shape[-2]
    if extra == 0:
        return block
    pad = [(0, 0)] * (block.ndim - 2) + [(0, extra), (0, 0)]
    return jnp.pad(block, pad)


def gather_weights(weights, gains, items, heads):
    count = items * heads
    pieces, places, row = [], [], 0
    for w, kind in zip(weights, WEIGHT_KINDS):
        block = local_panels(rounded(w.T if kind == "cols" else w))
        rows = padded_rows(block.shape[0])
        pieces.append(pad_rows(block, rows))
        places.append((row, rows))
        row += rows
    gain_row = rounded(jnp.concatenate(gains)).reshape(1, -1)
    gain_block = local_panels(gain_row)
    pieces.append(pad_rows(gain_block, padded_rows(gain_block.shape[0])))
    places.append((row, pieces[-1].shape[0]))
    row += pieces[-1].shape[0]
    total = -(-row // ROW_GROUP) * ROW_GROUP
    packed = pad_rows(jnp.concatenate(pieces, axis=0), total)
    gathered = lax.all_gather(packed, ALL, axis=0, tiled=True).reshape(count, total, PANEL)
    out = []
    for w, kind, (first, rows) in zip(weights, WEIGHT_KINDS, places):
        piece = gathered[:, first : first + rows, :]
        out.append(make_weight(piece, kind, local_shape(w, kind), items, heads))
    first, rows = places[-1]
    gain_all = gathered[:, first : first + rows, :].reshape(count, -1)[:, : gain_row.shape[1]]
    gain_all = gain_all.reshape(count, len(gains), -1)
    whole_gains = [widened(gain_all[:, k, :].reshape(-1)) for k in range(len(gains))]
    return out, whole_gains


def reduce_grads(grad_parts, gain_grads, weights, items, heads):
    count = items * heads
    pieces, places, row = [], [], 0
    for part in grad_parts:
        rows = padded_rows(part.shape[1])
        pieces.append(pad_rows(rounded(part), rows))
        places.append((row, part.shape[1]))
        row += rows
    gain_stack = jnp.stack([g.reshape(count, -1) for g in gain_grads], axis=1).reshape(count, 1, -1)
    gain_block = lane_pad(gain_stack, gain_stack.shape[-1]).reshape(count, -1, PANEL)
    pieces.append(pad_rows(rounded(gain_block), padded_rows(gain_block.shape[1])))
    places.append((row, gain_block.shape[1]))
    row += pieces[-1].shape[1]
    total = -(-row // ROW_GROUP) * ROW_GROUP
    packed = pad_rows(jnp.concatenate(pieces, axis=1), total)
    mine = lax.psum_scatter(
        packed.reshape(count * total, PANEL), ALL, scatter_dimension=0, tiled=True
    )
    out = []
    for w, kind, (first, rows) in zip(weights, WEIGHT_KINDS, places):
        r, width = local_shape(w, kind)
        panels = -(-width // PANEL)
        block = mine[first : first + rows].reshape(panels, r, PANEL).transpose(1, 0, 2)
        block = widened(lane_cut(block, width))
        out.append(block.T if kind == "cols" else block)
    first, rows = places[-1]
    gain_part = widened(mine[first : first + rows].reshape(-1)[: gain_stack.shape[-1]])
    gain_part = gain_part.reshape(len(gain_grads), -1)
    out += [gain_part[k] for k in range(len(gain_grads))]
    return out


def mlp_block(residual, gain_vec, up_w, down_w):
    normed = rounded(norm_rows(residual, gain_vec))
    before = apply(normed, up_w)
    hidden = rounded(jax.nn.gelu(before))
    return residual + apply(hidden, down_w), (normed, before, hidden)


def mlp_block_back(residual, gain_vec, up_w, down_w, saved, grad_out):
    normed, before, hidden = saved
    grad_round = rounded(grad_out)
    grad_down = grad_blocks(hidden, grad_round, down_w)
    grad_hidden = apply_t(grad_round, down_w)
    unused, gelu_back = jax.vjp(jax.nn.gelu, before)
    grad_before = rounded(gelu_back(grad_hidden)[0])
    grad_up = grad_blocks(normed, grad_before, up_w)
    grad_normed = apply_t(grad_before, up_w)
    grad_residual, grad_gain = norm_backward(residual, gain_vec, grad_normed)
    return grad_out + grad_residual, grad_up, grad_down, grad_gain


def exchange_rows(rows, split):
    if split == 1:
        return [rows]
    heads = lax.axis_size("heads")
    out = [rows]
    for shift in range(1, split):
        pairs = []
        for h in range(heads):
            base, pos = (h // split) * split, h % split
            pairs.append((h, base + (pos - shift) % split))
        out.append(lax.ppermute(rows, "heads", pairs))
    return out


def return_rows(parts, split):
    total = parts[0]
    heads = lax.axis_size("heads")
    for shift in range(1, split):
        pairs = []
        for h in range(heads):
            base, pos = (h // split) * split, h % split
            pairs.append((h, base + (pos + shift) % split))
        total = total + lax.ppermute(parts[shift], "heads", pairs)
    return total


def attention_block(residual, gain_vec, weight_set, split):
    query_w, key_w, value_w, out_w = weight_set
    rows = residual.shape[0]
    normed = rounded(norm_rows(residual, gain_vec))
    query_rows = rounded(apply(normed, query_w))
    key_rows = rounded(apply(normed, key_w))
    value_rows = rounded(apply(normed, value_w))
    heads_n = query_rows.shape[1] // HEAD
    key_all = jnp.concatenate(exchange_rows(key_rows, split), axis=0)
    value_all = jnp.concatenate(exchange_rows(value_rows, split), axis=0)
    keys = key_all.shape[0]
    q4 = query_rows.reshape(rows, heads_n, HEAD)
    k4 = key_all.reshape(keys, heads_n, HEAD)
    v4 = value_all.reshape(keys, heads_n, HEAD)
    scores = jnp.einsum("qhd,khd->hqk", q4, k4, preferred_element_type=jnp.float32) * (
        1.0 / math.sqrt(HEAD)
    )
    row_top = jnp.max(scores, axis=-1, keepdims=True)
    raw_weights = jnp.exp(scores - row_top)
    row_total = jnp.sum(raw_weights, axis=-1, keepdims=True)
    weights = raw_weights / row_total
    mixed = jnp.einsum("hqk,khd->qhd", rounded(weights), v4, preferred_element_type=jnp.float32)
    mixed = rounded(mixed.reshape(rows, heads_n * HEAD))
    saved = (normed, q4, k4, v4, weights, mixed)
    return residual + apply(mixed, out_w), saved


def attention_block_back(residual, gain_vec, weight_set, split, saved, grad_out):
    query_w, key_w, value_w, out_w = weight_set
    normed, q4, k4, v4, weights, mixed = saved
    rows = residual.shape[0]
    keys = k4.shape[0]
    scale = 1.0 / math.sqrt(HEAD)
    grad_round = rounded(grad_out)
    grad_out_w = grad_blocks(mixed, grad_round, out_w)
    grad_mixed = rounded(apply_t(grad_round, out_w)).reshape(q4.shape)
    grad_value = jnp.einsum(
        "hqk,qhd->khd", rounded(weights), grad_mixed, preferred_element_type=jnp.float32
    ).reshape(keys, -1)
    grad_weights = jnp.einsum("qhd,khd->hqk", grad_mixed, v4, preferred_element_type=jnp.float32)
    grad_scores = weights * (grad_weights - jnp.sum(grad_weights * weights, axis=-1, keepdims=True))
    grad_scores = rounded(grad_scores)
    grad_query = jnp.einsum("hqk,khd->qhd", grad_scores, k4, preferred_element_type=jnp.float32)
    grad_query = rounded((grad_query * scale).reshape(rows, -1))
    grad_key = jnp.einsum("hqk,qhd->khd", grad_scores, q4, preferred_element_type=jnp.float32)
    grad_key = (grad_key * scale).reshape(keys, -1)
    if split > 1:
        grad_key = return_rows(jnp.split(grad_key, split, axis=0), split)
        grad_value = return_rows(jnp.split(grad_value, split, axis=0), split)
    grad_key = rounded(grad_key)
    grad_value = rounded(grad_value)
    grad_query_w = grad_blocks(normed, grad_query, query_w)
    grad_key_w = grad_blocks(normed, grad_key, key_w)
    grad_value_w = grad_blocks(normed, grad_value, value_w)
    grad_normed = (
        apply_t(grad_query, query_w) + apply_t(grad_key, key_w) + apply_t(grad_value, value_w)
    )
    grad_residual, grad_gain = norm_backward(residual, gain_vec, grad_normed)
    return (grad_out + grad_residual, grad_query_w, grad_key_w, grad_value_w, grad_out_w, grad_gain)


def pixel_window(pixels, item_ids, item):
    count = pixels.shape[1]
    width = min(count, -(-PIX_MOST // LANE) * LANE + LANE)
    start = jnp.sum((item_ids < item).astype(jnp.int32))
    first = jnp.clip((start // LANE) * LANE, 0, count - width)
    window = lax.dynamic_slice_in_dim(pixels, first, width, axis=1)
    ids = lax.dynamic_slice_in_dim(item_ids, first, width, axis=0)
    return window, ids == item


def cross_block(residual, gain_vec, query_w, key_w, value_w, out_w, pixel_norm, allowed):
    scale = 1.0 / math.sqrt(residual.shape[1])
    normed = rounded(norm_rows(residual, gain_vec))
    query_rows = rounded(apply(normed, query_w))
    query_keyed = rounded(apply(query_rows, key_w) * scale)
    scores = jnp.where(allowed[None, :], product(query_keyed, pixel_norm), MASKED)
    row_top = jnp.max(scores, axis=-1, keepdims=True)
    raw_weights = jnp.exp(scores - row_top)
    row_total = jnp.sum(raw_weights, axis=-1, keepdims=True)
    weights = raw_weights / row_total
    weights_low = rounded(weights)
    pixel_mix = product_nt(weights_low, pixel_norm)
    mixed = rounded(split_apply_t(pixel_mix, value_w))
    saved = (normed, query_rows, weights, pixel_mix, mixed)
    return residual + apply(mixed, out_w), saved


def cross_block_back(
    residual, gain_vec, query_w, key_w, value_w, out_w, pixel_norm, saved, grad_out
):
    normed, query_rows, weights, pixel_mix, mixed = saved
    scale = 1.0 / math.sqrt(residual.shape[1])
    grad_round = rounded(grad_out)
    grad_out_w = grad_blocks(mixed, grad_round, out_w)
    grad_mixed = rounded(apply_t(grad_round, out_w))
    grad_keyed = rounded(apply(grad_mixed, value_w))
    grad_weights = product(grad_keyed, pixel_norm)
    grad_scores = weights * (grad_weights - jnp.sum(grad_weights * weights, axis=-1, keepdims=True))
    grad_scores = rounded(grad_scores)
    score_mix = product_nt(grad_scores, pixel_norm)
    grad_query = rounded(split_apply_t(score_mix, key_w) * scale)
    grad_query_w = grad_blocks(normed, grad_query, query_w)
    grad_key_w = split_grad_blocks(query_rows, score_mix, key_w) * scale
    grad_value_w = split_grad_blocks(grad_mixed, pixel_mix, value_w)
    grad_normed = apply_t(grad_query, query_w)
    grad_residual, grad_gain = norm_backward(residual, gain_vec, grad_normed)
    return (grad_out + grad_residual, grad_query_w, grad_key_w, grad_value_w, grad_out_w, grad_gain)


def local(latents, pixels, pixel_item, cotangent, *params):
    weights, gains = params[:12], params[12:]
    items = lax.axis_size("items")
    heads = lax.axis_size("heads")
    rows = latents.shape[0]
    split = max(1, NLAT // rows)
    (
        query_cross,
        key_cross,
        value_cross,
        out_cross,
        up_cross,
        down_cross,
        query_self,
        key_self,
        value_self,
        out_self,
        up_self,
        down_self,
    ), gain_list = gather_weights(weights, gains, items, heads)
    attention_set = (query_self, key_self, value_self, out_self)

    item = (lax.axis_index("heads") * rows) // NLAT
    window, allowed = pixel_window(pixels, pixel_item[0], item)
    pixel_norm = rounded(norm_pixels(widened(window)))

    start_rows = widened(latents)
    after_cross, saved_cross = cross_block(
        start_rows, gain_list[0], query_cross, key_cross, value_cross, out_cross, pixel_norm, allowed
    )
    after_mlp_one, saved_mlp_one = mlp_block(after_cross, gain_list[1], up_cross, down_cross)
    after_self, saved_self = attention_block(after_mlp_one, gain_list[2], attention_set, split)
    final_rows, saved_mlp_two = mlp_block(after_self, gain_list[3], up_self, down_self)

    grad_final = widened(cotangent)
    grad_after_self, grad_self_up, grad_self_down, grad_gain_four = mlp_block_back(
        after_self, gain_list[3], up_self, down_self, saved_mlp_two, grad_final
    )
    (
        grad_after_mlp,
        grad_self_query,
        grad_self_key,
        grad_self_value,
        grad_self_out,
        grad_gain_three,
    ) = attention_block_back(
        after_mlp_one, gain_list[2], attention_set, split, saved_self, grad_after_self
    )
    grad_after_cross, grad_cross_up, grad_cross_down, grad_gain_two = mlp_block_back(
        after_cross, gain_list[1], up_cross, down_cross, saved_mlp_one, grad_after_mlp
    )
    (
        latents_grad,
        grad_cross_query,
        grad_cross_key,
        grad_cross_value,
        grad_cross_out,
        grad_gain_one,
    ) = cross_block_back(
        start_rows,
        gain_list[0],
        query_cross,
        key_cross,
        value_cross,
        out_cross,
        pixel_norm,
        saved_cross,
        grad_after_cross,
    )
    weight_grads = (
        grad_cross_query,
        grad_cross_key,
        grad_cross_value,
        grad_cross_out,
        grad_cross_up,
        grad_cross_down,
        grad_self_query,
        grad_self_key,
        grad_self_value,
        grad_self_out,
        grad_self_up,
        grad_self_down,
    )
    gain_grads = (grad_gain_one, grad_gain_two, grad_gain_three, grad_gain_four)
    reduced = reduce_grads(weight_grads, gain_grads, weights, items, heads)
    shaped = [r.reshape(w.shape) for r, w in zip(reduced[:12], weights)]
    shaped += [r.reshape(g.shape) for r, g in zip(reduced[12:], gains)]
    return (rounded(final_rows), latents_grad, *shaped)


def solution(mesh):
    weight_specs = (
        P(ALL, None),
        P(None, ALL),
        P(None, ALL),
        P(ALL, None),
        P("items", "heads"),
        P("heads", "items"),
        P("items", "heads"),
        P("items", "heads"),
        P("items", "heads"),
        P("heads", "items"),
        P("items", "heads"),
        P("heads", "items"),
    )
    gain_specs = (P(ALL),) * 4
    placed = (P(ALL, None), P(None, "items"), P("items", None), P(ALL, None)) + weight_specs + gain_specs
    return jax.shard_map(
        local,
        mesh=mesh,
        in_specs=placed,
        out_specs=(P(ALL, None), P(ALL, None)) + weight_specs + gain_specs,
        check_vma=False,
    )
```

```python
import math

import jax
import jax.numpy as jnp
from jax import lax
from jax.sharding import PartitionSpec as P

HEAD = 128
NLAT = 512
PIX_MOST = 6144
LANE = 128

EPSILON = 1e-05
MASKED = -1e30
ALL = ("items", "heads")


def rounded(values):
    return values.astype(jnp.bfloat16)


def widened(values):
    return values.astype(jnp.float32)


def product(left_side, right_side):
    return jnp.dot(left_side, right_side, preferred_element_type=jnp.float32)


def product_tn(left_side, right_side):
    return lax.dot_general(
        left_side, right_side, (((0,), (0,)), ((), ())), preferred_element_type=jnp.float32
    )


def product_nt(left_side, right_side):
    return lax.dot_general(
        left_side, right_side, (((1,), (1,)), ((), ())), preferred_element_type=jnp.float32
    )


def split_parts(values):
    high = rounded(values)
    return high, rounded(values - widened(high))


def split_apply_t(values_f32, weight):
    high, low = split_parts(values_f32)
    return apply_t(high, weight) + apply_t(low, weight)


def norm_rows(values, gain_vec):
    centre = values - jnp.mean(values, axis=-1, keepdims=True)
    spread = jnp.mean(centre * centre, axis=-1, keepdims=True)
    return centre * lax.rsqrt(spread + EPSILON) * gain_vec


def norm_pixels(values):
    centre = values - jnp.mean(values, axis=0, keepdims=True)
    spread = jnp.mean(centre * centre, axis=0, keepdims=True)
    return centre * lax.rsqrt(spread + EPSILON)


def norm_backward(residual, gain_vec, grad_normed):
    unused, norm_back = jax.vjp(norm_rows, residual, gain_vec)
    return norm_back(grad_normed)


WEIGHT_KINDS = (
    "rows",
    "cols",
    "cols",
    "rows",
    "ih",
    "hi",
    "ih",
    "ih",
    "ih",
    "hi",
    "ih",
    "hi",
)

PANEL = 128
ROW_TILE = 16
ROW_GROUP = 48


def contract(left, right, left_dims, right_dims):
    return lax.dot_general(
        left, right, ((left_dims, right_dims), ((), ())), preferred_element_type=jnp.float32
    )


def lane_pad(values, width):
    panels = -(-width // PANEL)
    if panels * PANEL != width:
        pad = [(0, 0)] * (values.ndim - 1) + [(0, panels * PANEL - width)]
        values = jnp.pad(values, pad)
    return values.reshape(values.shape[:-1] + (panels, PANEL))


def lane_cut(values, width):
    values = values.reshape(values.shape[:-2] + (-1,))
    return values if values.shape[-1] == width else values[..., :width]


def local_panels(block):
    rows, width = block.shape
    parts = lane_pad(block, width).transpose(1, 0, 2)
    return parts.reshape(-1, PANEL)


def padded_rows(rows):
    return -(-rows // ROW_TILE) * ROW_TILE


def local_shape(w, kind):
    return (w.shape[1], w.shape[0]) if kind == "cols" else w.shape


def make_weight(piece, kind, shape, items, heads):
    rows, width = shape
    panels = -(-width // PANEL)
    blocks = piece[:, : panels * rows, :].reshape(items * heads, panels, rows, PANEL)
    if kind in ("ih", "hi"):
        blocks = blocks.reshape(items, heads, panels, rows, PANEL)
    return kind, blocks, width


def apply(values, weight):
    kind, blocks, width = weight
    count = values.shape[0]
    if kind in ("rows", "cols"):
        devices, panels, rows, lanes = blocks.shape
        out = contract(values.reshape(count, devices, rows), blocks, (1, 2), (0, 2))
        return lane_cut(out, width)
    items, heads, panels, rows, lanes = blocks.shape
    if kind == "ih":
        out = contract(values.reshape(count, items, rows), blocks, (1, 2), (0, 3))
    else:
        out = contract(values.reshape(count, heads, rows), blocks, (1, 2), (1, 3))
    return lane_cut(out, width).reshape(count, -1)


def apply_t(values, weight):
    kind, blocks, width = weight
    count = values.shape[0]
    if kind in ("rows", "cols"):
        devices, panels, rows, lanes = blocks.shape
        out = contract(lane_pad(values, width), blocks, (1, 2), (1, 3))
        return out.reshape(count, devices * rows)
    items, heads, panels, rows, lanes = blocks.shape
    if kind == "ih":
        spread = lane_pad(values.reshape(count, heads, width), width)
        out = contract(spread, blocks, (1, 2, 3), (1, 2, 4))
        return out.reshape(count, items * rows)
    spread = lane_pad(values.reshape(count, items, width), width)
    out = contract(spread, blocks, (1, 2, 3), (0, 2, 4))
    return out.reshape(count, heads * rows)


def grad_blocks(values, grads, weight):
    kind, blocks, width = weight
    count = values.shape[0]
    if kind in ("rows", "cols"):
        devices, panels, rows, lanes = blocks.shape
        out = contract(values.reshape(count, devices, rows), lane_pad(grads, width), (0,), (0,))
        out = out.transpose(0, 2, 1, 3)
    else:
        items, heads, panels, rows, lanes = blocks.shape
        devices = items * heads
        if kind == "ih":
            spread = lane_pad(grads.reshape(count, heads, width), width)
            out = contract(values.reshape(count, items, rows), spread, (0,), (0,))
            out = out.transpose(0, 2, 3, 1, 4)
        else:
            spread = lane_pad(grads.reshape(count, items, width), width)
            out = contract(values.reshape(count, heads, rows), spread, (0,), (0,))
            out = out.transpose(2, 0, 3, 1, 4)
    return out.reshape(devices, -1, PANEL)


def split_grad_blocks(values, grads_f32, weight):
    high, low = split_parts(grads_f32)
    return grad_blocks(values, high, weight) + grad_blocks(values, low, weight)


def pad_rows(block, rows):
    extra = rows - block.shape[-2]
    if extra == 0:
        return block
    pad = [(0, 0)] * (block.ndim - 2) + [(0, extra), (0, 0)]
    return jnp.pad(block, pad)


def gather_weights(weights, gains, items, heads):
    count = items * heads
    pieces, places, row = [], [], 0
    for w, kind in zip(weights, WEIGHT_KINDS):
        block = local_panels(rounded(w.T if kind == "cols" else w))
        rows = padded_rows(block.shape[0])
        pieces.append(pad_rows(block, rows))
        places.append((row, rows))
        row += rows
    gain_row = rounded(jnp.concatenate(gains)).reshape(1, -1)
    gain_block = local_panels(gain_row)
    total = -(-(row + gain_block.shape[0]) // ROW_GROUP) * ROW_GROUP
    pieces.append(pad_rows(gain_block, total - row))
    places.append((row, gain_block.shape[0]))
    packed = jnp.concatenate(pieces, axis=0)
    gathered = lax.all_gather(packed, ALL, axis=0, tiled=True).reshape(count, total, PANEL)
    out = []
    for w, kind, (first, rows) in zip(weights, WEIGHT_KINDS, places):
        piece = gathered[:, first : first + rows, :]
        out.append(make_weight(piece, kind, local_shape(w, kind), items, heads))
    first, rows = places[-1]
    gain_all = gathered[:, first : first + rows, :].reshape(count, -1)[:, : gain_row.shape[1]]
    gain_all = gain_all.reshape(count, len(gains), -1)
    whole_gains = [widened(gain_all[:, k, :].reshape(-1)) for k in range(len(gains))]
    return out, whole_gains


def reduce_grads(grad_parts, gain_grads, weights, items, heads):
    count = items * heads
    pieces, places, row = [], [], 0
    for part in grad_parts:
        rows = padded_rows(part.shape[1])
        pieces.append(pad_rows(rounded(part), rows))
        places.append((row, part.shape[1]))
        row += rows
    gain_stack = jnp.stack([g.reshape(count, -1) for g in gain_grads], axis=1).reshape(count, 1, -1)
    gain_block = lane_pad(gain_stack, gain_stack.shape[-1]).reshape(count, -1, PANEL)
    total = -(-(row + gain_block.shape[1]) // ROW_GROUP) * ROW_GROUP
    pieces.append(pad_rows(rounded(gain_block), total - row))
    places.append((row, gain_block.shape[1]))
    packed = jnp.concatenate(pieces, axis=1)
    mine = lax.psum_scatter(
        packed.reshape(count * total, PANEL), ALL, scatter_dimension=0, tiled=True
    )
    out = []
    for w, kind, (first, rows) in zip(weights, WEIGHT_KINDS, places):
        r, width = local_shape(w, kind)
        panels = -(-width // PANEL)
        block = mine[first : first + rows].reshape(panels, r, PANEL).transpose(1, 0, 2)
        block = widened(lane_cut(block, width))
        out.append(block.T if kind == "cols" else block)
    first, rows = places[-1]
    gain_part = widened(mine[first : first + rows].reshape(-1)[: gain_stack.shape[-1]])
    gain_part = gain_part.reshape(len(gain_grads), -1)
    out += [gain_part[k] for k in range(len(gain_grads))]
    return out


def mlp_block(residual, gain_vec, up_w, down_w):
    normed = rounded(norm_rows(residual, gain_vec))
    before = apply(normed, up_w)
    hidden = rounded(jax.nn.gelu(before))
    return residual + apply(hidden, down_w), (normed, before, hidden)


def mlp_block_back(residual, gain_vec, up_w, down_w, saved, grad_out):
    normed, before, hidden = saved
    grad_round = rounded(grad_out)
    grad_down = grad_blocks(hidden, grad_round, down_w)
    grad_hidden = apply_t(grad_round, down_w)
    unused, gelu_back = jax.vjp(jax.nn.gelu, before)
    grad_before = rounded(gelu_back(grad_hidden)[0])
    grad_up = grad_blocks(normed, grad_before, up_w)
    grad_normed = apply_t(grad_before, up_w)
    grad_residual, grad_gain = norm_backward(residual, gain_vec, grad_normed)
    return grad_out + grad_residual, grad_up, grad_down, grad_gain


def exchange_rows(rows, split):
    if split == 1:
        return [rows]
    heads = lax.axis_size("heads")
    out = [rows]
    for shift in range(1, split):
        pairs = []
        for h in range(heads):
            base, pos = (h // split) * split, h % split
            pairs.append((h, base + (pos - shift) % split))
        out.append(lax.ppermute(rows, "heads", pairs))
    return out


def return_rows(parts, split):
    total = parts[0]
    heads = lax.axis_size("heads")
    for shift in range(1, split):
        pairs = []
        for h in range(heads):
            base, pos = (h // split) * split, h % split
            pairs.append((h, base + (pos + shift) % split))
        total = total + lax.ppermute(parts[shift], "heads", pairs)
    return total


def attention_block(residual, gain_vec, weight_set, split):
    query_w, key_w, value_w, out_w = weight_set
    rows = residual.shape[0]
    normed = rounded(norm_rows(residual, gain_vec))
    query_rows = rounded(apply(normed, query_w))
    key_rows = rounded(apply(normed, key_w))
    value_rows = rounded(apply(normed, value_w))
    heads_n = query_rows.shape[1] // HEAD
    key_all = jnp.concatenate(exchange_rows(key_rows, split), axis=0)
    value_all = jnp.concatenate(exchange_rows(value_rows, split), axis=0)
    keys = key_all.shape[0]
    q4 = query_rows.reshape(rows, heads_n, HEAD)
    k4 = key_all.reshape(keys, heads_n, HEAD)
    v4 = value_all.reshape(keys, heads_n, HEAD)
    scores = jnp.einsum("qhd,khd->hqk", q4, k4, preferred_element_type=jnp.float32) * (
        1.0 / math.sqrt(HEAD)
    )
    row_top = jnp.max(scores, axis=-1, keepdims=True)
    raw_weights = jnp.exp(scores - row_top)
    row_total = jnp.sum(raw_weights, axis=-1, keepdims=True)
    weights = raw_weights / row_total
    mixed = jnp.einsum("hqk,khd->qhd", rounded(weights), v4, preferred_element_type=jnp.float32)
    mixed = rounded(mixed.reshape(rows, heads_n * HEAD))
    saved = (normed, q4, k4, v4, weights, mixed)
    return residual + apply(mixed, out_w), saved


def attention_block_back(residual, gain_vec, weight_set, split, saved, grad_out):
    query_w, key_w, value_w, out_w = weight_set
    normed, q4, k4, v4, weights, mixed = saved
    rows = residual.shape[0]
    keys = k4.shape[0]
    scale = 1.0 / math.sqrt(HEAD)
    grad_round = rounded(grad_out)
    grad_out_w = grad_blocks(mixed, grad_round, out_w)
    grad_mixed = rounded(apply_t(grad_round, out_w)).reshape(q4.shape)
    grad_value = jnp.einsum(
        "hqk,qhd->khd", rounded(weights), grad_mixed, preferred_element_type=jnp.float32
    ).reshape(keys, -1)
    grad_weights = jnp.einsum("qhd,khd->hqk", grad_mixed, v4, preferred_element_type=jnp.float32)
    grad_scores = weights * (grad_weights - jnp.sum(grad_weights * weights, axis=-1, keepdims=True))
    grad_scores = rounded(grad_scores)
    grad_query = jnp.einsum("hqk,khd->qhd", grad_scores, k4, preferred_element_type=jnp.float32)
    grad_query = rounded((grad_query * scale).reshape(rows, -1))
    grad_key = jnp.einsum("hqk,qhd->khd", grad_scores, q4, preferred_element_type=jnp.float32)
    grad_key = (grad_key * scale).reshape(keys, -1)
    if split > 1:
        grad_key = return_rows(jnp.split(grad_key, split, axis=0), split)
        grad_value = return_rows(jnp.split(grad_value, split, axis=0), split)
    grad_key = rounded(grad_key)
    grad_value = rounded(grad_value)
    grad_query_w = grad_blocks(normed, grad_query, query_w)
    grad_key_w = grad_blocks(normed, grad_key, key_w)
    grad_value_w = grad_blocks(normed, grad_value, value_w)
    grad_normed = (
        apply_t(grad_query, query_w) + apply_t(grad_key, key_w) + apply_t(grad_value, value_w)
    )
    grad_residual, grad_gain = norm_backward(residual, gain_vec, grad_normed)
    return (grad_out + grad_residual, grad_query_w, grad_key_w, grad_value_w, grad_out_w, grad_gain)


def pixel_window(pixels, item_ids, item):
    count = pixels.shape[1]
    width = min(count, -(-PIX_MOST // LANE) * LANE + LANE)
    start = jnp.sum((item_ids < item).astype(jnp.int32))
    first = jnp.clip((start // LANE) * LANE, 0, count - width)
    window = lax.dynamic_slice_in_dim(pixels, first, width, axis=1)
    ids = lax.dynamic_slice_in_dim(item_ids, first, width, axis=0)
    return window, ids == item


def cross_block(residual, gain_vec, query_w, key_w, value_w, out_w, pixel_norm, allowed):
    scale = 1.0 / math.sqrt(residual.shape[1])
    normed = rounded(norm_rows(residual, gain_vec))
    query_rows = rounded(apply(normed, query_w))
    query_keyed = rounded(apply(query_rows, key_w) * scale)
    scores = jnp.where(allowed[None, :], product(query_keyed, pixel_norm), MASKED)
    row_top = jnp.max(scores, axis=-1, keepdims=True)
    raw_weights = jnp.exp(scores - row_top)
    row_total = jnp.sum(raw_weights, axis=-1, keepdims=True)
    weights = raw_weights / row_total
    weights_low = rounded(weights)
    pixel_mix = product_nt(weights_low, pixel_norm)
    mixed = rounded(split_apply_t(pixel_mix, value_w))
    saved = (normed, query_rows, weights, pixel_mix, mixed)
    return residual + apply(mixed, out_w), saved


def cross_block_back(
    residual, gain_vec, query_w, key_w, value_w, out_w, pixel_norm, saved, grad_out
):
    normed, query_rows, weights, pixel_mix, mixed = saved
    scale = 1.0 / math.sqrt(residual.shape[1])
    grad_round = rounded(grad_out)
    grad_out_w = grad_blocks(mixed, grad_round, out_w)
    grad_mixed = rounded(apply_t(grad_round, out_w))
    grad_keyed = rounded(apply(grad_mixed, value_w))
    grad_weights = product(grad_keyed, pixel_norm)
    grad_scores = weights * (grad_weights - jnp.sum(grad_weights * weights, axis=-1, keepdims=True))
    grad_scores = rounded(grad_scores)
    score_mix = product_nt(grad_scores, pixel_norm)
    grad_query = rounded(split_apply_t(score_mix, key_w) * scale)
    grad_query_w = grad_blocks(normed, grad_query, query_w)
    grad_key_w = split_grad_blocks(query_rows, score_mix, key_w) * scale
    grad_value_w = split_grad_blocks(grad_mixed, pixel_mix, value_w)
    grad_normed = apply_t(grad_query, query_w)
    grad_residual, grad_gain = norm_backward(residual, gain_vec, grad_normed)
    return (grad_out + grad_residual, grad_query_w, grad_key_w, grad_value_w, grad_out_w, grad_gain)


def local(latents, pixels, pixel_item, cotangent, *params):
    weights, gains = params[:12], params[12:]
    items = lax.axis_size("items")
    heads = lax.axis_size("heads")
    rows = latents.shape[0]
    split = max(1, NLAT // rows)
    (
        query_cross,
        key_cross,
        value_cross,
        out_cross,
        up_cross,
        down_cross,
        query_self,
        key_self,
        value_self,
        out_self,
        up_self,
        down_self,
    ), gain_list = gather_weights(weights, gains, items, heads)
    attention_set = (query_self, key_self, value_self, out_self)

    item = (lax.axis_index("heads") * rows) // NLAT
    window, allowed = pixel_window(pixels, pixel_item[0], item)
    pixel_norm = rounded(norm_pixels(widened(window)))

    start_rows = widened(latents)
    after_cross, saved_cross = cross_block(
        start_rows, gain_list[0], query_cross, key_cross, value_cross, out_cross, pixel_norm, allowed
    )
    after_mlp_one, saved_mlp_one = mlp_block(after_cross, gain_list[1], up_cross, down_cross)
    after_self, saved_self = attention_block(after_mlp_one, gain_list[2], attention_set, split)
    final_rows, saved_mlp_two = mlp_block(after_self, gain_list[3], up_self, down_self)

    grad_final = widened(cotangent)
    grad_after_self, grad_self_up, grad_self_down, grad_gain_four = mlp_block_back(
        after_self, gain_list[3], up_self, down_self, saved_mlp_two, grad_final
    )
    (
        grad_after_mlp,
        grad_self_query,
        grad_self_key,
        grad_self_value,
        grad_self_out,
        grad_gain_three,
    ) = attention_block_back(
        after_mlp_one, gain_list[2], attention_set, split, saved_self, grad_after_self
    )
    grad_after_cross, grad_cross_up, grad_cross_down, grad_gain_two = mlp_block_back(
        after_cross, gain_list[1], up_cross, down_cross, saved_mlp_one, grad_after_mlp
    )
    (
        latents_grad,
        grad_cross_query,
        grad_cross_key,
        grad_cross_value,
        grad_cross_out,
        grad_gain_one,
    ) = cross_block_back(
        start_rows,
        gain_list[0],
        query_cross,
        key_cross,
        value_cross,
        out_cross,
        pixel_norm,
        saved_cross,
        grad_after_cross,
    )
    weight_grads = (
        grad_cross_query,
        grad_cross_key,
        grad_cross_value,
        grad_cross_out,
        grad_cross_up,
        grad_cross_down,
        grad_self_query,
        grad_self_key,
        grad_self_value,
        grad_self_out,
        grad_self_up,
        grad_self_down,
    )
    gain_grads = (grad_gain_one, grad_gain_two, grad_gain_three, grad_gain_four)
    reduced = reduce_grads(weight_grads, gain_grads, weights, items, heads)
    shaped = [r.reshape(w.shape) for r, w in zip(reduced[:12], weights)]
    shaped += [r.reshape(g.shape) for r, g in zip(reduced[12:], gains)]
    return (rounded(final_rows), latents_grad, *shaped)


def solution(mesh):
    weight_specs = (
        P(ALL, None),
        P(None, ALL),
        P(None, ALL),
        P(ALL, None),
        P("items", "heads"),
        P("heads", "items"),
        P("items", "heads"),
        P("items", "heads"),
        P("items", "heads"),
        P("heads", "items"),
        P("items", "heads"),
        P("heads", "items"),
    )
    gain_specs = (P(ALL),) * 4
    placed = (P(ALL, None), P(None, "items"), P("items", None), P(ALL, None)) + weight_specs + gain_specs
    return jax.shard_map(
        local,
        mesh=mesh,
        in_specs=placed,
        out_specs=(P(ALL, None), P(ALL, None)) + weight_specs + gain_specs,
        check_vma=False,
    )
```

```python
import math

import jax
import jax.numpy as jnp
from jax import lax
from jax.sharding import PartitionSpec as P

HEAD = 128
NLAT = 512
PIX_MOST = 6144
LANE = 128

EPSILON = 1e-05
MASKED = -1e30
ALL = ("items", "heads")


def rounded(values):
    return values.astype(jnp.bfloat16)


def widened(values):
    return values.astype(jnp.float32)


def product(left_side, right_side):
    return jnp.dot(left_side, right_side, preferred_element_type=jnp.float32)


def product_tn(left_side, right_side):
    return lax.dot_general(
        left_side, right_side, (((0,), (0,)), ((), ())), preferred_element_type=jnp.float32
    )


def product_nt(left_side, right_side):
    return lax.dot_general(
        left_side, right_side, (((1,), (1,)), ((), ())), preferred_element_type=jnp.float32
    )


def split_parts(values):
    high = rounded(values)
    return high, rounded(values - widened(high))


def split_apply_t(values_f32, weight):
    high, low = split_parts(values_f32)
    return apply_t(high, weight) + apply_t(low, weight)


def norm_rows(values, gain_vec):
    centre = values - jnp.mean(values, axis=-1, keepdims=True)
    spread = jnp.mean(centre * centre, axis=-1, keepdims=True)
    return centre * lax.rsqrt(spread + EPSILON) * gain_vec


def norm_pixels(values):
    centre = values - jnp.mean(values, axis=0, keepdims=True)
    spread = jnp.mean(centre * centre, axis=0, keepdims=True)
    return centre * lax.rsqrt(spread + EPSILON)


def norm_backward(residual, gain_vec, grad_normed):
    unused, norm_back = jax.vjp(norm_rows, residual, gain_vec)
    return norm_back(grad_normed)


WEIGHT_KINDS = (
    "rows",
    "cols",
    "cols",
    "rows",
    "ih",
    "hi",
    "ih",
    "ih",
    "ih",
    "hi",
    "ih",
    "hi",
)

PANEL = 128
ROW_TILE = 16
ROW_GROUP = 48


def contract(left, right, left_dims, right_dims):
    return lax.dot_general(
        left, right, ((left_dims, right_dims), ((), ())), preferred_element_type=jnp.float32
    )


def lane_pad(values, width):
    panels = -(-width // PANEL)
    if panels * PANEL != width:
        pad = [(0, 0)] * (values.ndim - 1) + [(0, panels * PANEL - width)]
        values = jnp.pad(values, pad)
    return values.reshape(values.shape[:-1] + (panels, PANEL))


def lane_cut(values, width):
    values = values.reshape(values.shape[:-2] + (-1,))
    return values if values.shape[-1] == width else values[..., :width]


def local_panels(block):
    rows, width = block.shape
    parts = lane_pad(block, width).transpose(1, 0, 2)
    return parts.reshape(-1, PANEL)


def padded_rows(rows):
    return -(-rows // ROW_TILE) * ROW_TILE


def local_shape(w, kind):
    return (w.shape[1], w.shape[0]) if kind == "cols" else w.shape


def make_weight(piece, kind, shape, items, heads):
    rows, width = shape
    panels = -(-width // PANEL)
    blocks = piece[:, : panels * rows, :].reshape(items * heads, panels, rows, PANEL)
    if kind in ("ih", "hi"):
        blocks = blocks.reshape(items, heads, panels, rows, PANEL)
    return kind, blocks, width


def apply(values, weight):
    kind, blocks, width = weight
    count = values.shape[0]
    if kind in ("rows", "cols"):
        devices, panels, rows, lanes = blocks.shape
        out = contract(values.reshape(count, devices, rows), blocks, (1, 2), (0, 2))
        return lane_cut(out, width)
    items, heads, panels, rows, lanes = blocks.shape
    if kind == "ih":
        out = contract(values.reshape(count, items, rows), blocks, (1, 2), (0, 3))
    else:
        out = contract(values.reshape(count, heads, rows), blocks, (1, 2), (1, 3))
    return lane_cut(out, width).reshape(count, -1)


def apply_t(values, weight):
    kind, blocks, width = weight
    count = values.shape[0]
    if kind in ("rows", "cols"):
        devices, panels, rows, lanes = blocks.shape
        out = contract(lane_pad(values, width), blocks, (1, 2), (1, 3))
        return out.reshape(count, devices * rows)
    items, heads, panels, rows, lanes = blocks.shape
    if kind == "ih":
        spread = lane_pad(values.reshape(count, heads, width), width)
        out = contract(spread, blocks, (1, 2, 3), (1, 2, 4))
        return out.reshape(count, items * rows)
    spread = lane_pad(values.reshape(count, items, width), width)
    out = contract(spread, blocks, (1, 2, 3), (0, 2, 4))
    return out.reshape(count, heads * rows)


def grad_blocks(values, grads, weight):
    kind, blocks, width = weight
    count = values.shape[0]
    if kind in ("rows", "cols"):
        devices, panels, rows, lanes = blocks.shape
        out = contract(values.reshape(count, devices, rows), lane_pad(grads, width), (0,), (0,))
        out = out.transpose(0, 2, 1, 3)
    else:
        items, heads, panels, rows, lanes = blocks.shape
        devices = items * heads
        if kind == "ih":
            spread = lane_pad(grads.reshape(count, heads, width), width)
            out = contract(values.reshape(count, items, rows), spread, (0,), (0,))
            out = out.transpose(0, 2, 3, 1, 4)
        else:
            spread = lane_pad(grads.reshape(count, items, width), width)
            out = contract(values.reshape(count, heads, rows), spread, (0,), (0,))
            out = out.transpose(2, 0, 3, 1, 4)
    return out.reshape(devices, -1, PANEL)


def split_grad_blocks(values, grads_f32, weight):
    high, low = split_parts(grads_f32)
    return grad_blocks(values, high, weight) + grad_blocks(values, low, weight)


def pad_rows(block, rows):
    extra = rows - block.shape[-2]
    if extra == 0:
        return block
    pad = [(0, 0)] * (block.ndim - 2) + [(0, extra), (0, 0)]
    return jnp.pad(block, pad)


def gather_weights(weights, gains, items, heads):
    count = items * heads
    pieces, places, row = [], [], 0
    for w, kind in zip(weights, WEIGHT_KINDS):
        block = local_panels(rounded(w.T if kind == "cols" else w))
        rows = padded_rows(block.shape[0])
        pieces.append(pad_rows(block, rows))
        places.append((row, rows))
        row += rows
    gain_row = rounded(jnp.concatenate(gains)).reshape(1, -1)
    gain_block = local_panels(gain_row)
    total = -(-(row + gain_block.shape[0]) // ROW_GROUP) * ROW_GROUP
    pieces.append(pad_rows(gain_block, total - row))
    places.append((row, gain_block.shape[0]))
    packed = jnp.concatenate(pieces, axis=0)
    gathered = lax.all_gather(packed, ALL, axis=0, tiled=True).reshape(count, total, PANEL)
    out = []
    for w, kind, (first, rows) in zip(weights, WEIGHT_KINDS, places):
        piece = gathered[:, first : first + rows, :]
        out.append(make_weight(piece, kind, local_shape(w, kind), items, heads))
    first, rows = places[-1]
    gain_all = gathered[:, first : first + rows, :].reshape(count, -1)[:, : gain_row.shape[1]]
    gain_all = gain_all.reshape(count, len(gains), -1)
    whole_gains = [widened(gain_all[:, k, :].reshape(-1)) for k in range(len(gains))]
    return out, whole_gains


def reduce_grads(grad_parts, gain_grads, weights, items, heads):
    count = items * heads
    pieces, places, row = [], [], 0
    for part in grad_parts:
        rows = padded_rows(part.shape[1])
        pieces.append(pad_rows(rounded(part), rows))
        places.append((row, part.shape[1]))
        row += rows
    gain_stack = jnp.stack([g.reshape(count, -1) for g in gain_grads], axis=1).reshape(count, 1, -1)
    gain_block = lane_pad(gain_stack, gain_stack.shape[-1]).reshape(count, -1, PANEL)
    total = -(-(row + gain_block.shape[1]) // ROW_GROUP) * ROW_GROUP
    pieces.append(pad_rows(rounded(gain_block), total - row))
    places.append((row, gain_block.shape[1]))
    packed = jnp.concatenate(pieces, axis=1)
    mine = lax.psum_scatter(
        packed.reshape(count * total, PANEL), "items", scatter_dimension=0, tiled=True
    )
    mine = lax.psum_scatter(mine, "heads", scatter_dimension=0, tiled=True)
    out = []
    for w, kind, (first, rows) in zip(weights, WEIGHT_KINDS, places):
        r, width = local_shape(w, kind)
        panels = -(-width // PANEL)
        block = mine[first : first + rows].reshape(panels, r, PANEL).transpose(1, 0, 2)
        block = widened(lane_cut(block, width))
        out.append(block.T if kind == "cols" else block)
    first, rows = places[-1]
    gain_part = widened(mine[first : first + rows].reshape(-1)[: gain_stack.shape[-1]])
    gain_part = gain_part.reshape(len(gain_grads), -1)
    out += [gain_part[k] for k in range(len(gain_grads))]
    return out


def mlp_block(residual, gain_vec, up_w, down_w):
    normed = rounded(norm_rows(residual, gain_vec))
    before = apply(normed, up_w)
    hidden = rounded(jax.nn.gelu(before))
    return residual + apply(hidden, down_w), (normed, before, hidden)


def mlp_block_back(residual, gain_vec, up_w, down_w, saved, grad_out):
    normed, before, hidden = saved
    grad_round = rounded(grad_out)
    grad_down = grad_blocks(hidden, grad_round, down_w)
    grad_hidden = apply_t(grad_round, down_w)
    unused, gelu_back = jax.vjp(jax.nn.gelu, before)
    grad_before = rounded(gelu_back(grad_hidden)[0])
    grad_up = grad_blocks(normed, grad_before, up_w)
    grad_normed = apply_t(grad_before, up_w)
    grad_residual, grad_gain = norm_backward(residual, gain_vec, grad_normed)
    return grad_out + grad_residual, grad_up, grad_down, grad_gain


def exchange_rows(rows, split):
    if split == 1:
        return [rows]
    heads = lax.axis_size("heads")
    out = [rows]
    for shift in range(1, split):
        pairs = []
        for h in range(heads):
            base, pos = (h // split) * split, h % split
            pairs.append((h, base + (pos - shift) % split))
        out.append(lax.ppermute(rows, "heads", pairs))
    return out


def return_rows(parts, split):
    total = parts[0]
    heads = lax.axis_size("heads")
    for shift in range(1, split):
        pairs = []
        for h in range(heads):
            base, pos = (h // split) * split, h % split
            pairs.append((h, base + (pos + shift) % split))
        total = total + lax.ppermute(parts[shift], "heads", pairs)
    return total


def attention_block(residual, gain_vec, weight_set, split):
    query_w, key_w, value_w, out_w = weight_set
    rows = residual.shape[0]
    normed = rounded(norm_rows(residual, gain_vec))
    query_rows = rounded(apply(normed, query_w))
    key_rows = rounded(apply(normed, key_w))
    value_rows = rounded(apply(normed, value_w))
    heads_n = query_rows.shape[1] // HEAD
    key_all = jnp.concatenate(exchange_rows(key_rows, split), axis=0)
    value_all = jnp.concatenate(exchange_rows(value_rows, split), axis=0)
    keys = key_all.shape[0]
    q4 = query_rows.reshape(rows, heads_n, HEAD)
    k4 = key_all.reshape(keys, heads_n, HEAD)
    v4 = value_all.reshape(keys, heads_n, HEAD)
    scores = jnp.einsum("qhd,khd->hqk", q4, k4, preferred_element_type=jnp.float32) * (
        1.0 / math.sqrt(HEAD)
    )
    row_top = jnp.max(scores, axis=-1, keepdims=True)
    raw_weights = jnp.exp(scores - row_top)
    row_total = jnp.sum(raw_weights, axis=-1, keepdims=True)
    weights = raw_weights / row_total
    mixed = jnp.einsum("hqk,khd->qhd", rounded(weights), v4, preferred_element_type=jnp.float32)
    mixed = rounded(mixed.reshape(rows, heads_n * HEAD))
    saved = (normed, q4, k4, v4, weights, mixed)
    return residual + apply(mixed, out_w), saved


def attention_block_back(residual, gain_vec, weight_set, split, saved, grad_out):
    query_w, key_w, value_w, out_w = weight_set
    normed, q4, k4, v4, weights, mixed = saved
    rows = residual.shape[0]
    keys = k4.shape[0]
    scale = 1.0 / math.sqrt(HEAD)
    grad_round = rounded(grad_out)
    grad_out_w = grad_blocks(mixed, grad_round, out_w)
    grad_mixed = rounded(apply_t(grad_round, out_w)).reshape(q4.shape)
    grad_value = jnp.einsum(
        "hqk,qhd->khd", rounded(weights), grad_mixed, preferred_element_type=jnp.float32
    ).reshape(keys, -1)
    grad_weights = jnp.einsum("qhd,khd->hqk", grad_mixed, v4, preferred_element_type=jnp.float32)
    grad_scores = weights * (grad_weights - jnp.sum(grad_weights * weights, axis=-1, keepdims=True))
    grad_scores = rounded(grad_scores)
    grad_query = jnp.einsum("hqk,khd->qhd", grad_scores, k4, preferred_element_type=jnp.float32)
    grad_query = rounded((grad_query * scale).reshape(rows, -1))
    grad_key = jnp.einsum("hqk,qhd->khd", grad_scores, q4, preferred_element_type=jnp.float32)
    grad_key = (grad_key * scale).reshape(keys, -1)
    if split > 1:
        grad_key = return_rows(jnp.split(grad_key, split, axis=0), split)
        grad_value = return_rows(jnp.split(grad_value, split, axis=0), split)
    grad_key = rounded(grad_key)
    grad_value = rounded(grad_value)
    grad_query_w = grad_blocks(normed, grad_query, query_w)
    grad_key_w = grad_blocks(normed, grad_key, key_w)
    grad_value_w = grad_blocks(normed, grad_value, value_w)
    grad_normed = (
        apply_t(grad_query, query_w) + apply_t(grad_key, key_w) + apply_t(grad_value, value_w)
    )
    grad_residual, grad_gain = norm_backward(residual, gain_vec, grad_normed)
    return (grad_out + grad_residual, grad_query_w, grad_key_w, grad_value_w, grad_out_w, grad_gain)


def pixel_window(pixels, item_ids, item):
    count = pixels.shape[1]
    width = min(count, -(-PIX_MOST // LANE) * LANE + LANE)
    start = jnp.sum((item_ids < item).astype(jnp.int32))
    first = jnp.clip((start // LANE) * LANE, 0, count - width)
    window = lax.dynamic_slice_in_dim(pixels, first, width, axis=1)
    ids = lax.dynamic_slice_in_dim(item_ids, first, width, axis=0)
    return window, ids == item


def cross_block(residual, gain_vec, query_w, key_w, value_w, out_w, pixel_norm, allowed):
    scale = 1.0 / math.sqrt(residual.shape[1])
    normed = rounded(norm_rows(residual, gain_vec))
    query_rows = rounded(apply(normed, query_w))
    query_keyed = rounded(apply(query_rows, key_w) * scale)
    scores = jnp.where(allowed[None, :], product(query_keyed, pixel_norm), MASKED)
    row_top = jnp.max(scores, axis=-1, keepdims=True)
    raw_weights = jnp.exp(scores - row_top)
    row_total = jnp.sum(raw_weights, axis=-1, keepdims=True)
    weights = raw_weights / row_total
    weights_low = rounded(weights)
    pixel_mix = product_nt(weights_low, pixel_norm)
    mixed = rounded(split_apply_t(pixel_mix, value_w))
    saved = (normed, query_rows, weights, pixel_mix, mixed)
    return residual + apply(mixed, out_w), saved


def cross_block_back(
    residual, gain_vec, query_w, key_w, value_w, out_w, pixel_norm, saved, grad_out
):
    normed, query_rows, weights, pixel_mix, mixed = saved
    scale = 1.0 / math.sqrt(residual.shape[1])
    grad_round = rounded(grad_out)
    grad_out_w = grad_blocks(mixed, grad_round, out_w)
    grad_mixed = rounded(apply_t(grad_round, out_w))
    grad_keyed = rounded(apply(grad_mixed, value_w))
    grad_weights = product(grad_keyed, pixel_norm)
    grad_scores = weights * (grad_weights - jnp.sum(grad_weights * weights, axis=-1, keepdims=True))
    grad_scores = rounded(grad_scores)
    score_mix = product_nt(grad_scores, pixel_norm)
    grad_query = rounded(split_apply_t(score_mix, key_w) * scale)
    grad_query_w = grad_blocks(normed, grad_query, query_w)
    grad_key_w = split_grad_blocks(query_rows, score_mix, key_w) * scale
    grad_value_w = split_grad_blocks(grad_mixed, pixel_mix, value_w)
    grad_normed = apply_t(grad_query, query_w)
    grad_residual, grad_gain = norm_backward(residual, gain_vec, grad_normed)
    return (grad_out + grad_residual, grad_query_w, grad_key_w, grad_value_w, grad_out_w, grad_gain)


def local(latents, pixels, pixel_item, cotangent, *params):
    weights, gains = params[:12], params[12:]
    items = lax.axis_size("items")
    heads = lax.axis_size("heads")
    rows = latents.shape[0]
    split = max(1, NLAT // rows)
    (
        query_cross,
        key_cross,
        value_cross,
        out_cross,
        up_cross,
        down_cross,
        query_self,
        key_self,
        value_self,
        out_self,
        up_self,
        down_self,
    ), gain_list = gather_weights(weights, gains, items, heads)
    attention_set = (query_self, key_self, value_self, out_self)

    item = (lax.axis_index("heads") * rows) // NLAT
    window, allowed = pixel_window(pixels, pixel_item[0], item)
    pixel_norm = rounded(norm_pixels(widened(window)))

    start_rows = widened(latents)
    after_cross, saved_cross = cross_block(
        start_rows, gain_list[0], query_cross, key_cross, value_cross, out_cross, pixel_norm, allowed
    )
    after_mlp_one, saved_mlp_one = mlp_block(after_cross, gain_list[1], up_cross, down_cross)
    after_self, saved_self = attention_block(after_mlp_one, gain_list[2], attention_set, split)
    final_rows, saved_mlp_two = mlp_block(after_self, gain_list[3], up_self, down_self)

    grad_final = widened(cotangent)
    grad_after_self, grad_self_up, grad_self_down, grad_gain_four = mlp_block_back(
        after_self, gain_list[3], up_self, down_self, saved_mlp_two, grad_final
    )
    (
        grad_after_mlp,
        grad_self_query,
        grad_self_key,
        grad_self_value,
        grad_self_out,
        grad_gain_three,
    ) = attention_block_back(
        after_mlp_one, gain_list[2], attention_set, split, saved_self, grad_after_self
    )
    grad_after_cross, grad_cross_up, grad_cross_down, grad_gain_two = mlp_block_back(
        after_cross, gain_list[1], up_cross, down_cross, saved_mlp_one, grad_after_mlp
    )
    (
        latents_grad,
        grad_cross_query,
        grad_cross_key,
        grad_cross_value,
        grad_cross_out,
        grad_gain_one,
    ) = cross_block_back(
        start_rows,
        gain_list[0],
        query_cross,
        key_cross,
        value_cross,
        out_cross,
        pixel_norm,
        saved_cross,
        grad_after_cross,
    )
    weight_grads = (
        grad_cross_query,
        grad_cross_key,
        grad_cross_value,
        grad_cross_out,
        grad_cross_up,
        grad_cross_down,
        grad_self_query,
        grad_self_key,
        grad_self_value,
        grad_self_out,
        grad_self_up,
        grad_self_down,
    )
    gain_grads = (grad_gain_one, grad_gain_two, grad_gain_three, grad_gain_four)
    reduced = reduce_grads(weight_grads, gain_grads, weights, items, heads)
    shaped = [r.reshape(w.shape) for r, w in zip(reduced[:12], weights)]
    shaped += [r.reshape(g.shape) for r, g in zip(reduced[12:], gains)]
    return (rounded(final_rows), latents_grad, *shaped)


def solution(mesh):
    weight_specs = (
        P(ALL, None),
        P(None, ALL),
        P(None, ALL),
        P(ALL, None),
        P("items", "heads"),
        P("heads", "items"),
        P("items", "heads"),
        P("items", "heads"),
        P("items", "heads"),
        P("heads", "items"),
        P("items", "heads"),
        P("heads", "items"),
    )
    gain_specs = (P(ALL),) * 4
    placed = (P(ALL, None), P(None, "items"), P("items", None), P(ALL, None)) + weight_specs + gain_specs
    return jax.shard_map(
        local,
        mesh=mesh,
        in_specs=placed,
        out_specs=(P(ALL, None), P(ALL, None)) + weight_specs + gain_specs,
        check_vma=False,
    )
```

```python
import math

import jax
import jax.numpy as jnp
from jax import lax
from jax.sharding import PartitionSpec as P

HEAD = 128
NLAT = 512
PIX_MOST = 6144
LANE = 128

EPSILON = 1e-05
MASKED = -1e30
ALL = ("items", "heads")


def rounded(values):
    return values.astype(jnp.bfloat16)


def widened(values):
    return values.astype(jnp.float32)


def product(left_side, right_side):
    return jnp.dot(left_side, right_side, preferred_element_type=jnp.float32)


def product_tn(left_side, right_side):
    return lax.dot_general(
        left_side, right_side, (((0,), (0,)), ((), ())), preferred_element_type=jnp.float32
    )


def product_nt(left_side, right_side):
    return lax.dot_general(
        left_side, right_side, (((1,), (1,)), ((), ())), preferred_element_type=jnp.float32
    )


def split_parts(values):
    high = rounded(values)
    return high, rounded(values - widened(high))


def split_apply_t(values_f32, weight):
    high, low = split_parts(values_f32)
    return apply_t(high, weight) + apply_t(low, weight)


def norm_rows(values, gain_vec):
    centre = values - jnp.mean(values, axis=-1, keepdims=True)
    spread = jnp.mean(centre * centre, axis=-1, keepdims=True)
    return centre * lax.rsqrt(spread + EPSILON) * gain_vec


def norm_pixels(values):
    centre = values - jnp.mean(values, axis=0, keepdims=True)
    spread = jnp.mean(centre * centre, axis=0, keepdims=True)
    return centre * lax.rsqrt(spread + EPSILON)


def norm_backward(residual, gain_vec, grad_normed):
    unused, norm_back = jax.vjp(norm_rows, residual, gain_vec)
    return norm_back(grad_normed)


WEIGHT_KINDS = (
    "rows",
    "cols",
    "cols",
    "rows",
    "ih",
    "hi",
    "ih",
    "ih",
    "ih",
    "hi",
    "ih",
    "hi",
)

PANEL = 128
ROW_TILE = 16
ROW_GROUP = 48


def contract(left, right, left_dims, right_dims):
    return lax.dot_general(
        left, right, ((left_dims, right_dims), ((), ())), preferred_element_type=jnp.float32
    )


def lane_pad(values, width):
    panels = -(-width // PANEL)
    if panels * PANEL != width:
        pad = [(0, 0)] * (values.ndim - 1) + [(0, panels * PANEL - width)]
        values = jnp.pad(values, pad)
    return values.reshape(values.shape[:-1] + (panels, PANEL))


def lane_cut(values, width):
    values = values.reshape(values.shape[:-2] + (-1,))
    return values if values.shape[-1] == width else values[..., :width]


def local_panels(block):
    rows, width = block.shape
    parts = lane_pad(block, width).transpose(1, 0, 2)
    return parts.reshape(-1, PANEL)


def padded_rows(rows):
    return -(-rows // ROW_TILE) * ROW_TILE


def local_shape(w, kind):
    return (w.shape[1], w.shape[0]) if kind == "cols" else w.shape


def make_weight(piece, kind, shape, items, heads):
    rows, width = shape
    panels = -(-width // PANEL)
    blocks = piece[:, : panels * rows, :].reshape(items * heads, panels, rows, PANEL)
    if kind in ("ih", "hi"):
        blocks = blocks.reshape(items, heads, panels, rows, PANEL)
    return kind, blocks, width


def apply(values, weight):
    kind, blocks, width = weight
    count = values.shape[0]
    if kind in ("rows", "cols"):
        devices, panels, rows, lanes = blocks.shape
        out = contract(values.reshape(count, devices, rows), blocks, (1, 2), (0, 2))
        return lane_cut(out, width)
    items, heads, panels, rows, lanes = blocks.shape
    if kind == "ih":
        out = contract(values.reshape(count, items, rows), blocks, (1, 2), (0, 3))
    else:
        out = contract(values.reshape(count, heads, rows), blocks, (1, 2), (1, 3))
    return lane_cut(out, width).reshape(count, -1)


def apply_t(values, weight):
    kind, blocks, width = weight
    count = values.shape[0]
    if kind in ("rows", "cols"):
        devices, panels, rows, lanes = blocks.shape
        out = contract(lane_pad(values, width), blocks, (1, 2), (1, 3))
        return out.reshape(count, devices * rows)
    items, heads, panels, rows, lanes = blocks.shape
    if kind == "ih":
        spread = lane_pad(values.reshape(count, heads, width), width)
        out = contract(spread, blocks, (1, 2, 3), (1, 2, 4))
        return out.reshape(count, items * rows)
    spread = lane_pad(values.reshape(count, items, width), width)
    out = contract(spread, blocks, (1, 2, 3), (0, 2, 4))
    return out.reshape(count, heads * rows)


def grad_blocks(values, grads, weight):
    kind, blocks, width = weight
    count = values.shape[0]
    if kind in ("rows", "cols"):
        devices, panels, rows, lanes = blocks.shape
        out = contract(values.reshape(count, devices, rows), lane_pad(grads, width), (0,), (0,))
        out = out.transpose(0, 2, 1, 3)
    else:
        items, heads, panels, rows, lanes = blocks.shape
        devices = items * heads
        if kind == "ih":
            spread = lane_pad(grads.reshape(count, heads, width), width)
            out = contract(values.reshape(count, items, rows), spread, (0,), (0,))
            out = out.transpose(0, 2, 3, 1, 4)
        else:
            spread = lane_pad(grads.reshape(count, items, width), width)
            out = contract(values.reshape(count, heads, rows), spread, (0,), (0,))
            out = out.transpose(2, 0, 3, 1, 4)
    return out.reshape(devices, -1, PANEL)


def split_grad_blocks(values, grads_f32, weight):
    high, low = split_parts(grads_f32)
    return grad_blocks(values, high, weight) + grad_blocks(values, low, weight)


def pad_rows(block, rows):
    extra = rows - block.shape[-2]
    if extra == 0:
        return block
    pad = [(0, 0)] * (block.ndim - 2) + [(0, extra), (0, 0)]
    return jnp.pad(block, pad)


def gather_weights(weights, gains, items, heads):
    count = items * heads
    pieces, places, row = [], [], 0
    for w, kind in zip(weights, WEIGHT_KINDS):
        block = local_panels(rounded(w.T if kind == "cols" else w))
        rows = padded_rows(block.shape[0])
        pieces.append(pad_rows(block, rows))
        places.append((row, rows))
        row += rows
    gain_row = rounded(jnp.concatenate(gains)).reshape(1, -1)
    gain_block = local_panels(gain_row)
    total = -(-(row + gain_block.shape[0]) // ROW_GROUP) * ROW_GROUP
    pieces.append(pad_rows(gain_block, total - row))
    places.append((row, gain_block.shape[0]))
    packed = jnp.concatenate(pieces, axis=0)
    gathered = lax.all_gather(packed, ALL, axis=0, tiled=True).reshape(count, total, PANEL)
    out = []
    for w, kind, (first, rows) in zip(weights, WEIGHT_KINDS, places):
        piece = gathered[:, first : first + rows, :]
        out.append(make_weight(piece, kind, local_shape(w, kind), items, heads))
    first, rows = places[-1]
    gain_all = gathered[:, first : first + rows, :].reshape(count, -1)[:, : gain_row.shape[1]]
    gain_all = gain_all.reshape(count, len(gains), -1)
    whole_gains = [widened(gain_all[:, k, :].reshape(-1)) for k in range(len(gains))]
    return out, whole_gains


def reduce_grads(grad_parts, gain_grads, weights, items, heads):
    count = items * heads
    pieces, places, row = [], [], 0
    for part in grad_parts:
        rows = padded_rows(part.shape[1])
        pieces.append(pad_rows(rounded(part), rows))
        places.append((row, part.shape[1]))
        row += rows
    gain_stack = jnp.stack([g.reshape(count, -1) for g in gain_grads], axis=1).reshape(count, 1, -1)
    gain_block = lane_pad(gain_stack, gain_stack.shape[-1]).reshape(count, -1, PANEL)
    total = -(-(row + gain_block.shape[1]) // ROW_GROUP) * ROW_GROUP
    pieces.append(pad_rows(rounded(gain_block), total - row))
    places.append((row, gain_block.shape[1]))
    packed = jnp.concatenate(pieces, axis=1)
    mine = lax.psum_scatter(
        packed.reshape(count * total, PANEL), "items", scatter_dimension=0, tiled=True
    )
    mine = lax.psum_scatter(mine, "heads", scatter_dimension=0, tiled=True)
    out = []
    for w, kind, (first, rows) in zip(weights, WEIGHT_KINDS, places):
        r, width = local_shape(w, kind)
        panels = -(-width // PANEL)
        block = mine[first : first + rows].reshape(panels, r, PANEL).transpose(1, 0, 2)
        block = widened(lane_cut(block, width))
        out.append(block.T if kind == "cols" else block)
    first, rows = places[-1]
    gain_part = widened(mine[first : first + rows].reshape(-1)[: gain_stack.shape[-1]])
    gain_part = gain_part.reshape(len(gain_grads), -1)
    out += [gain_part[k] for k in range(len(gain_grads))]
    return out


def mlp_block(residual, gain_vec, up_w, down_w):
    normed = rounded(norm_rows(residual, gain_vec))
    before = apply(normed, up_w)
    hidden = rounded(jax.nn.gelu(before))
    return residual + apply(hidden, down_w), (normed, before, hidden)


def mlp_block_back(residual, gain_vec, up_w, down_w, saved, grad_out):
    normed, before, hidden = saved
    grad_round = rounded(grad_out)
    grad_down = grad_blocks(hidden, grad_round, down_w)
    grad_hidden = apply_t(grad_round, down_w)
    unused, gelu_back = jax.vjp(jax.nn.gelu, before)
    grad_before = rounded(gelu_back(grad_hidden)[0])
    grad_up = grad_blocks(normed, grad_before, up_w)
    grad_normed = apply_t(grad_before, up_w)
    grad_residual, grad_gain = norm_backward(residual, gain_vec, grad_normed)
    return grad_out + grad_residual, grad_up, grad_down, grad_gain


def exchange_rows(rows, split):
    if split == 1:
        return [rows]
    heads = lax.axis_size("heads")
    out = [rows]
    for shift in range(1, split):
        pairs = []
        for h in range(heads):
            base, pos = (h // split) * split, h % split
            pairs.append((h, base + (pos - shift) % split))
        out.append(lax.ppermute(rows, "heads", pairs))
    return out


def return_rows(parts, split):
    total = parts[0]
    heads = lax.axis_size("heads")
    for shift in range(1, split):
        pairs = []
        for h in range(heads):
            base, pos = (h // split) * split, h % split
            pairs.append((h, base + (pos + shift) % split))
        total = total + lax.ppermute(parts[shift], "heads", pairs)
    return total


def attention_block(residual, gain_vec, weight_set, split):
    query_w, key_w, value_w, out_w = weight_set
    rows = residual.shape[0]
    normed = rounded(norm_rows(residual, gain_vec))
    query_rows = rounded(apply(normed, query_w))
    key_rows = rounded(apply(normed, key_w))
    value_rows = rounded(apply(normed, value_w))
    heads_n = query_rows.shape[1] // HEAD
    key_all = jnp.concatenate(exchange_rows(key_rows, split), axis=0)
    value_all = jnp.concatenate(exchange_rows(value_rows, split), axis=0)
    keys = key_all.shape[0]
    q4 = query_rows.reshape(rows, heads_n, HEAD)
    k4 = key_all.reshape(keys, heads_n, HEAD)
    v4 = value_all.reshape(keys, heads_n, HEAD)
    scores = jnp.einsum("qhd,khd->hqk", q4, k4, preferred_element_type=jnp.float32) * (
        1.0 / math.sqrt(HEAD)
    )
    row_top = jnp.max(scores, axis=-1, keepdims=True)
    raw_weights = jnp.exp(scores - row_top)
    row_total = jnp.sum(raw_weights, axis=-1, keepdims=True)
    weights_low = rounded(raw_weights / row_total)
    mixed_full = jnp.einsum("hqk,khd->qhd", weights_low, v4, preferred_element_type=jnp.float32)
    mixed = rounded(mixed_full.reshape(rows, heads_n * HEAD))
    saved = (normed, q4, k4, v4, weights_low, mixed_full, mixed)
    return residual + apply(mixed, out_w), saved


def attention_block_back(residual, gain_vec, weight_set, split, saved, grad_out):
    query_w, key_w, value_w, out_w = weight_set
    normed, q4, k4, v4, weights_low, mixed_full, mixed = saved
    rows = residual.shape[0]
    keys = k4.shape[0]
    scale = 1.0 / math.sqrt(HEAD)
    grad_round = rounded(grad_out)
    grad_out_w = grad_blocks(mixed, grad_round, out_w)
    grad_mixed = rounded(apply_t(grad_round, out_w)).reshape(q4.shape)
    grad_value = jnp.einsum(
        "hqk,qhd->khd", weights_low, grad_mixed, preferred_element_type=jnp.float32
    ).reshape(keys, -1)
    row_dot = jnp.sum(widened(grad_mixed) * mixed_full, axis=-1).T[:, :, None]
    grad_weights = jnp.einsum("qhd,khd->hqk", grad_mixed, v4, preferred_element_type=jnp.float32)
    grad_scores = rounded(widened(weights_low) * (grad_weights - row_dot))
    grad_query = jnp.einsum("hqk,khd->qhd", grad_scores, k4, preferred_element_type=jnp.float32)
    grad_query = rounded((grad_query * scale).reshape(rows, -1))
    grad_key = jnp.einsum("hqk,qhd->khd", grad_scores, q4, preferred_element_type=jnp.float32)
    grad_key = (grad_key * scale).reshape(keys, -1)
    if split > 1:
        grad_key = return_rows(jnp.split(grad_key, split, axis=0), split)
        grad_value = return_rows(jnp.split(grad_value, split, axis=0), split)
    grad_key = rounded(grad_key)
    grad_value = rounded(grad_value)
    grad_query_w = grad_blocks(normed, grad_query, query_w)
    grad_key_w = grad_blocks(normed, grad_key, key_w)
    grad_value_w = grad_blocks(normed, grad_value, value_w)
    grad_normed = (
        apply_t(grad_query, query_w) + apply_t(grad_key, key_w) + apply_t(grad_value, value_w)
    )
    grad_residual, grad_gain = norm_backward(residual, gain_vec, grad_normed)
    return (grad_out + grad_residual, grad_query_w, grad_key_w, grad_value_w, grad_out_w, grad_gain)


def pixel_window(pixels, item_ids, item):
    count = pixels.shape[1]
    width = min(count, -(-PIX_MOST // LANE) * LANE + LANE)
    start = jnp.sum((item_ids < item).astype(jnp.int32))
    first = jnp.clip((start // LANE) * LANE, 0, count - width)
    window = lax.dynamic_slice_in_dim(pixels, first, width, axis=1)
    ids = lax.dynamic_slice_in_dim(item_ids, first, width, axis=0)
    return window, ids == item


def cross_block(residual, gain_vec, query_w, key_w, value_w, out_w, pixel_norm, allowed):
    scale = 1.0 / math.sqrt(residual.shape[1])
    normed = rounded(norm_rows(residual, gain_vec))
    query_rows = rounded(apply(normed, query_w))
    query_keyed = rounded(apply(query_rows, key_w) * scale)
    scores = jnp.where(allowed[None, :], product(query_keyed, pixel_norm), MASKED)
    row_top = jnp.max(scores, axis=-1, keepdims=True)
    raw_weights = jnp.exp(scores - row_top)
    row_total = jnp.sum(raw_weights, axis=-1, keepdims=True)
    weights_low = rounded(raw_weights / row_total)
    pixel_mix = product_nt(weights_low, pixel_norm)
    mixed = rounded(split_apply_t(pixel_mix, value_w))
    saved = (normed, query_rows, weights_low, pixel_mix, mixed)
    return residual + apply(mixed, out_w), saved


def cross_block_back(
    residual, gain_vec, query_w, key_w, value_w, out_w, pixel_norm, saved, grad_out
):
    normed, query_rows, weights_low, pixel_mix, mixed = saved
    scale = 1.0 / math.sqrt(residual.shape[1])
    grad_round = rounded(grad_out)
    grad_out_w = grad_blocks(mixed, grad_round, out_w)
    grad_mixed = rounded(apply_t(grad_round, out_w))
    grad_keyed = rounded(apply(grad_mixed, value_w))
    row_dot = jnp.sum(widened(grad_keyed) * pixel_mix, axis=-1, keepdims=True)
    grad_weights = product(grad_keyed, pixel_norm)
    grad_scores = rounded(widened(weights_low) * (grad_weights - row_dot))
    score_mix = product_nt(grad_scores, pixel_norm)
    grad_query = rounded(split_apply_t(score_mix, key_w) * scale)
    grad_query_w = grad_blocks(normed, grad_query, query_w)
    grad_key_w = split_grad_blocks(query_rows, score_mix, key_w) * scale
    grad_value_w = split_grad_blocks(grad_mixed, pixel_mix, value_w)
    grad_normed = apply_t(grad_query, query_w)
    grad_residual, grad_gain = norm_backward(residual, gain_vec, grad_normed)
    return (grad_out + grad_residual, grad_query_w, grad_key_w, grad_value_w, grad_out_w, grad_gain)


def local(latents, pixels, pixel_item, cotangent, *params):
    weights, gains = params[:12], params[12:]
    items = lax.axis_size("items")
    heads = lax.axis_size("heads")
    rows = latents.shape[0]
    split = max(1, NLAT // rows)
    (
        query_cross,
        key_cross,
        value_cross,
        out_cross,
        up_cross,
        down_cross,
        query_self,
        key_self,
        value_self,
        out_self,
        up_self,
        down_self,
    ), gain_list = gather_weights(weights, gains, items, heads)
    attention_set = (query_self, key_self, value_self, out_self)

    item = (lax.axis_index("heads") * rows) // NLAT
    window, allowed = pixel_window(pixels, pixel_item[0], item)
    pixel_norm = rounded(norm_pixels(widened(window)))

    start_rows = widened(latents)
    after_cross, saved_cross = cross_block(
        start_rows, gain_list[0], query_cross, key_cross, value_cross, out_cross, pixel_norm, allowed
    )
    after_mlp_one, saved_mlp_one = mlp_block(after_cross, gain_list[1], up_cross, down_cross)
    after_self, saved_self = attention_block(after_mlp_one, gain_list[2], attention_set, split)
    final_rows, saved_mlp_two = mlp_block(after_self, gain_list[3], up_self, down_self)

    grad_final = widened(cotangent)
    grad_after_self, grad_self_up, grad_self_down, grad_gain_four = mlp_block_back(
        after_self, gain_list[3], up_self, down_self, saved_mlp_two, grad_final
    )
    (
        grad_after_mlp,
        grad_self_query,
        grad_self_key,
        grad_self_value,
        grad_self_out,
        grad_gain_three,
    ) = attention_block_back(
        after_mlp_one, gain_list[2], attention_set, split, saved_self, grad_after_self
    )
    grad_after_cross, grad_cross_up, grad_cross_down, grad_gain_two = mlp_block_back(
        after_cross, gain_list[1], up_cross, down_cross, saved_mlp_one, grad_after_mlp
    )
    (
        latents_grad,
        grad_cross_query,
        grad_cross_key,
        grad_cross_value,
        grad_cross_out,
        grad_gain_one,
    ) = cross_block_back(
        start_rows,
        gain_list[0],
        query_cross,
        key_cross,
        value_cross,
        out_cross,
        pixel_norm,
        saved_cross,
        grad_after_cross,
    )
    weight_grads = (
        grad_cross_query,
        grad_cross_key,
        grad_cross_value,
        grad_cross_out,
        grad_cross_up,
        grad_cross_down,
        grad_self_query,
        grad_self_key,
        grad_self_value,
        grad_self_out,
        grad_self_up,
        grad_self_down,
    )
    gain_grads = (grad_gain_one, grad_gain_two, grad_gain_three, grad_gain_four)
    reduced = reduce_grads(weight_grads, gain_grads, weights, items, heads)
    shaped = [r.reshape(w.shape) for r, w in zip(reduced[:12], weights)]
    shaped += [r.reshape(g.shape) for r, g in zip(reduced[12:], gains)]
    return (rounded(final_rows), latents_grad, *shaped)


def solution(mesh):
    weight_specs = (
        P(ALL, None),
        P(None, ALL),
        P(None, ALL),
        P(ALL, None),
        P("items", "heads"),
        P("heads", "items"),
        P("items", "heads"),
        P("items", "heads"),
        P("items", "heads"),
        P("heads", "items"),
        P("items", "heads"),
        P("heads", "items"),
    )
    gain_specs = (P(ALL),) * 4
    placed = (P(ALL, None), P(None, "items"), P("items", None), P(ALL, None)) + weight_specs + gain_specs
    return jax.shard_map(
        local,
        mesh=mesh,
        in_specs=placed,
        out_specs=(P(ALL, None), P(ALL, None)) + weight_specs + gain_specs,
        check_vma=False,
    )
```

```python
import math

import jax
import jax.numpy as jnp
from jax import lax
from jax.sharding import PartitionSpec as P

HEAD = 128
NLAT = 512
PIX_MOST = 6144
LANE = 128

EPSILON = 1e-05
MASKED = -1e30
ALL = ("items", "heads")


def rounded(values):
    return values.astype(jnp.bfloat16)


def widened(values):
    return values.astype(jnp.float32)


def product(left_side, right_side):
    return jnp.dot(left_side, right_side, preferred_element_type=jnp.float32)


def product_tn(left_side, right_side):
    return lax.dot_general(
        left_side, right_side, (((0,), (0,)), ((), ())), preferred_element_type=jnp.float32
    )


def product_nt(left_side, right_side):
    return lax.dot_general(
        left_side, right_side, (((1,), (1,)), ((), ())), preferred_element_type=jnp.float32
    )


def split_parts(values):
    high = rounded(values)
    return high, rounded(values - widened(high))


def split_apply_t(values_f32, weight):
    high, low = split_parts(values_f32)
    return apply_t(high, weight) + apply_t(low, weight)


def norm_rows(values, gain_vec):
    centre = values - jnp.mean(values, axis=-1, keepdims=True)
    spread = jnp.mean(centre * centre, axis=-1, keepdims=True)
    return centre * lax.rsqrt(spread + EPSILON) * gain_vec


def norm_pixels(values):
    centre = values - jnp.mean(values, axis=0, keepdims=True)
    spread = jnp.mean(centre * centre, axis=0, keepdims=True)
    return centre * lax.rsqrt(spread + EPSILON)


def norm_backward(residual, gain_vec, grad_normed):
    unused, norm_back = jax.vjp(norm_rows, residual, gain_vec)
    return norm_back(grad_normed)


WEIGHT_KINDS = (
    "rows",
    "cols",
    "cols",
    "rows",
    "ih",
    "hi",
    "ih",
    "ih",
    "ih",
    "hi",
    "ih",
    "hi",
)

PANEL = 128
ROW_TILE = 16
ROW_GROUP = 48


def contract(left, right, left_dims, right_dims):
    return lax.dot_general(
        left, right, ((left_dims, right_dims), ((), ())), preferred_element_type=jnp.float32
    )


def lane_pad(values, width):
    panels = -(-width // PANEL)
    if panels * PANEL != width:
        pad = [(0, 0)] * (values.ndim - 1) + [(0, panels * PANEL - width)]
        values = jnp.pad(values, pad)
    return values.reshape(values.shape[:-1] + (panels, PANEL))


def lane_cut(values, width):
    values = values.reshape(values.shape[:-2] + (-1,))
    return values if values.shape[-1] == width else values[..., :width]


def local_panels(block):
    rows, width = block.shape
    parts = lane_pad(block, width).transpose(1, 0, 2)
    return parts.reshape(-1, PANEL)


def padded_rows(rows):
    return -(-rows // ROW_TILE) * ROW_TILE


def local_shape(w, kind):
    return (w.shape[1], w.shape[0]) if kind == "cols" else w.shape


def make_weight(piece, kind, shape, items, heads):
    rows, width = shape
    panels = -(-width // PANEL)
    blocks = piece[:, : panels * rows, :].reshape(items * heads, panels, rows, PANEL)
    if kind in ("ih", "hi"):
        blocks = blocks.reshape(items, heads, panels, rows, PANEL)
    return kind, blocks, width


def apply(values, weight):
    kind, blocks, width = weight
    count = values.shape[0]
    if kind in ("rows", "cols"):
        devices, panels, rows, lanes = blocks.shape
        out = contract(values.reshape(count, devices, rows), blocks, (1, 2), (0, 2))
        return lane_cut(out, width)
    items, heads, panels, rows, lanes = blocks.shape
    if kind == "ih":
        out = contract(values.reshape(count, items, rows), blocks, (1, 2), (0, 3))
    else:
        out = contract(values.reshape(count, heads, rows), blocks, (1, 2), (1, 3))
    return lane_cut(out, width).reshape(count, -1)


def apply_t(values, weight):
    kind, blocks, width = weight
    count = values.shape[0]
    if kind in ("rows", "cols"):
        devices, panels, rows, lanes = blocks.shape
        out = contract(lane_pad(values, width), blocks, (1, 2), (1, 3))
        return out.reshape(count, devices * rows)
    items, heads, panels, rows, lanes = blocks.shape
    if kind == "ih":
        spread = lane_pad(values.reshape(count, heads, width), width)
        out = contract(spread, blocks, (1, 2, 3), (1, 2, 4))
        return out.reshape(count, items * rows)
    spread = lane_pad(values.reshape(count, items, width), width)
    out = contract(spread, blocks, (1, 2, 3), (0, 2, 4))
    return out.reshape(count, heads * rows)


def grad_blocks(values, grads, weight):
    kind, blocks, width = weight
    count = values.shape[0]
    if kind in ("rows", "cols"):
        devices, panels, rows, lanes = blocks.shape
        out = contract(values.reshape(count, devices, rows), lane_pad(grads, width), (0,), (0,))
        out = out.transpose(0, 2, 1, 3)
    else:
        items, heads, panels, rows, lanes = blocks.shape
        devices = items * heads
        if kind == "ih":
            spread = lane_pad(grads.reshape(count, heads, width), width)
            out = contract(values.reshape(count, items, rows), spread, (0,), (0,))
            out = out.transpose(0, 2, 3, 1, 4)
        else:
            spread = lane_pad(grads.reshape(count, items, width), width)
            out = contract(values.reshape(count, heads, rows), spread, (0,), (0,))
            out = out.transpose(2, 0, 3, 1, 4)
    return out.reshape(devices, -1, PANEL)


def split_grad_blocks(values, grads_f32, weight):
    high, low = split_parts(grads_f32)
    return grad_blocks(values, high, weight) + grad_blocks(values, low, weight)


def pad_rows(block, rows):
    extra = rows - block.shape[-2]
    if extra == 0:
        return block
    pad = [(0, 0)] * (block.ndim - 2) + [(0, extra), (0, 0)]
    return jnp.pad(block, pad)


def gather_weights(weights, gains, items, heads):
    count = items * heads
    pieces, places, row = [], [], 0
    for w, kind in zip(weights, WEIGHT_KINDS):
        block = local_panels(rounded(w.T if kind == "cols" else w))
        rows = padded_rows(block.shape[0])
        pieces.append(pad_rows(block, rows))
        places.append((row, rows))
        row += rows
    gain_row = rounded(jnp.concatenate(gains)).reshape(1, -1)
    gain_block = local_panels(gain_row)
    total = -(-(row + gain_block.shape[0]) // ROW_GROUP) * ROW_GROUP
    pieces.append(pad_rows(gain_block, total - row))
    places.append((row, gain_block.shape[0]))
    packed = jnp.concatenate(pieces, axis=0)
    gathered = lax.all_gather(packed, ALL, axis=0, tiled=True).reshape(count, total, PANEL)
    out = []
    for w, kind, (first, rows) in zip(weights, WEIGHT_KINDS, places):
        piece = gathered[:, first : first + rows, :]
        out.append(make_weight(piece, kind, local_shape(w, kind), items, heads))
    first, rows = places[-1]
    gain_all = gathered[:, first : first + rows, :].reshape(count, -1)[:, : gain_row.shape[1]]
    gain_all = gain_all.reshape(count, len(gains), -1)
    whole_gains = [widened(gain_all[:, k, :].reshape(-1)) for k in range(len(gains))]
    return out, whole_gains


def reduce_grads(grad_parts, gain_grads, weights, items, heads):
    count = items * heads
    pieces, places, row = [], [], 0
    for part in grad_parts:
        rows = padded_rows(part.shape[1])
        pieces.append(pad_rows(rounded(part), rows))
        places.append((row, part.shape[1]))
        row += rows
    gain_stack = jnp.stack([g.reshape(count, -1) for g in gain_grads], axis=1).reshape(count, 1, -1)
    gain_block = lane_pad(gain_stack, gain_stack.shape[-1]).reshape(count, -1, PANEL)
    total = -(-(row + gain_block.shape[1]) // ROW_GROUP) * ROW_GROUP
    pieces.append(pad_rows(rounded(gain_block), total - row))
    places.append((row, gain_block.shape[1]))
    packed = jnp.concatenate(pieces, axis=1)
    mine = lax.psum_scatter(
        packed.reshape(count * total, PANEL), "items", scatter_dimension=0, tiled=True
    )
    mine = lax.psum_scatter(mine, "heads", scatter_dimension=0, tiled=True)
    out = []
    for w, kind, (first, rows) in zip(weights, WEIGHT_KINDS, places):
        r, width = local_shape(w, kind)
        panels = -(-width // PANEL)
        block = mine[first : first + rows].reshape(panels, r, PANEL).transpose(1, 0, 2)
        block = widened(lane_cut(block, width))
        out.append(block.T if kind == "cols" else block)
    first, rows = places[-1]
    gain_part = widened(mine[first : first + rows].reshape(-1)[: gain_stack.shape[-1]])
    gain_part = gain_part.reshape(len(gain_grads), -1)
    out += [gain_part[k] for k in range(len(gain_grads))]
    return out


def mlp_block(residual, gain_vec, up_w, down_w):
    normed = rounded(norm_rows(residual, gain_vec))
    before = apply(normed, up_w)
    hidden = rounded(jax.nn.gelu(before))
    return residual + apply(hidden, down_w), (normed, before, hidden)


def mlp_block_back(residual, gain_vec, up_w, down_w, saved, grad_out):
    normed, before, hidden = saved
    grad_round = rounded(grad_out)
    grad_down = grad_blocks(hidden, grad_round, down_w)
    grad_hidden = apply_t(grad_round, down_w)
    unused, gelu_back = jax.vjp(jax.nn.gelu, before)
    grad_before = rounded(gelu_back(grad_hidden)[0])
    grad_up = grad_blocks(normed, grad_before, up_w)
    grad_normed = apply_t(grad_before, up_w)
    grad_residual, grad_gain = norm_backward(residual, gain_vec, grad_normed)
    return grad_out + grad_residual, grad_up, grad_down, grad_gain


def exchange_rows(rows, split):
    if split == 1:
        return [rows]
    heads = lax.axis_size("heads")
    out = [rows]
    for shift in range(1, split):
        pairs = []
        for h in range(heads):
            base, pos = (h // split) * split, h % split
            pairs.append((h, base + (pos - shift) % split))
        out.append(lax.ppermute(rows, "heads", pairs))
    return out


def return_rows(parts, split):
    total = parts[0]
    heads = lax.axis_size("heads")
    for shift in range(1, split):
        pairs = []
        for h in range(heads):
            base, pos = (h // split) * split, h % split
            pairs.append((h, base + (pos + shift) % split))
        total = total + lax.ppermute(parts[shift], "heads", pairs)
    return total


def attention_block(residual, gain_vec, weight_set, split):
    query_w, key_w, value_w, out_w = weight_set
    rows = residual.shape[0]
    normed = rounded(norm_rows(residual, gain_vec))
    query_rows = rounded(apply(normed, query_w))
    key_rows = rounded(apply(normed, key_w))
    value_rows = rounded(apply(normed, value_w))
    heads_n = query_rows.shape[1] // HEAD
    key_all = jnp.concatenate(exchange_rows(key_rows, split), axis=0)
    value_all = jnp.concatenate(exchange_rows(value_rows, split), axis=0)
    keys = key_all.shape[0]
    q4 = query_rows.reshape(rows, heads_n, HEAD)
    k4 = key_all.reshape(keys, heads_n, HEAD)
    v4 = value_all.reshape(keys, heads_n, HEAD)
    scores = jnp.einsum("qhd,khd->hqk", q4, k4, preferred_element_type=jnp.float32) * (
        1.0 / math.sqrt(HEAD)
    )
    row_top = jnp.max(scores, axis=-1, keepdims=True)
    raw_weights = jnp.exp(scores - row_top)
    row_total = jnp.sum(raw_weights, axis=-1, keepdims=True)
    weights_low = rounded(raw_weights / row_total)
    mixed_full = jnp.einsum("hqk,khd->qhd", weights_low, v4, preferred_element_type=jnp.float32)
    mixed = rounded(mixed_full.reshape(rows, heads_n * HEAD))
    saved = (normed, q4, k4, v4, weights_low, mixed_full, mixed)
    return residual + apply(mixed, out_w), saved


def attention_block_back(residual, gain_vec, weight_set, split, saved, grad_out):
    query_w, key_w, value_w, out_w = weight_set
    normed, q4, k4, v4, weights_low, mixed_full, mixed = saved
    rows = residual.shape[0]
    keys = k4.shape[0]
    scale = 1.0 / math.sqrt(HEAD)
    grad_round = rounded(grad_out)
    grad_out_w = grad_blocks(mixed, grad_round, out_w)
    grad_mixed = rounded(apply_t(grad_round, out_w)).reshape(q4.shape)
    grad_value = jnp.einsum(
        "hqk,qhd->khd", weights_low, grad_mixed, preferred_element_type=jnp.float32
    ).reshape(keys, -1)
    row_dot = jnp.sum(widened(grad_mixed) * mixed_full, axis=-1).T[:, :, None]
    grad_weights = jnp.einsum("qhd,khd->hqk", grad_mixed, v4, preferred_element_type=jnp.float32)
    grad_scores = rounded(widened(weights_low) * (grad_weights - row_dot))
    grad_query = jnp.einsum("hqk,khd->qhd", grad_scores, k4, preferred_element_type=jnp.float32)
    grad_query = rounded((grad_query * scale).reshape(rows, -1))
    grad_key = jnp.einsum("hqk,qhd->khd", grad_scores, q4, preferred_element_type=jnp.float32)
    grad_key = (grad_key * scale).reshape(keys, -1)
    if split > 1:
        grad_key = return_rows(jnp.split(grad_key, split, axis=0), split)
        grad_value = return_rows(jnp.split(grad_value, split, axis=0), split)
    grad_key = rounded(grad_key)
    grad_value = rounded(grad_value)
    grad_query_w = grad_blocks(normed, grad_query, query_w)
    grad_key_w = grad_blocks(normed, grad_key, key_w)
    grad_value_w = grad_blocks(normed, grad_value, value_w)
    grad_normed = (
        apply_t(grad_query, query_w) + apply_t(grad_key, key_w) + apply_t(grad_value, value_w)
    )
    grad_residual, grad_gain = norm_backward(residual, gain_vec, grad_normed)
    return (grad_out + grad_residual, grad_query_w, grad_key_w, grad_value_w, grad_out_w, grad_gain)


def pixel_window(pixels, item_ids, item):
    count = pixels.shape[1]
    width = min(count, -(-PIX_MOST // LANE) * LANE + LANE)
    start = jnp.sum((item_ids < item).astype(jnp.int32))
    first = jnp.clip((start // LANE) * LANE, 0, count - width)
    window = lax.dynamic_slice_in_dim(pixels, first, width, axis=1)
    ids = lax.dynamic_slice_in_dim(item_ids, first, width, axis=0)
    return window, ids == item


def cross_block(residual, gain_vec, query_w, key_w, value_w, out_w, pixel_norm, allowed):
    scale = 1.0 / math.sqrt(residual.shape[1])
    normed = rounded(norm_rows(residual, gain_vec))
    query_rows = rounded(apply(normed, query_w))
    query_keyed = rounded(apply(query_rows, key_w) * scale)
    scores = jnp.where(allowed[None, :], product(query_keyed, pixel_norm), MASKED)
    row_top = jnp.max(scores, axis=-1, keepdims=True)
    raw_weights = jnp.exp(scores - row_top)
    row_total = jnp.sum(raw_weights, axis=-1, keepdims=True)
    weights_low = rounded(raw_weights / row_total)
    pixel_mix = product_nt(weights_low, pixel_norm)
    mixed = rounded(split_apply_t(pixel_mix, value_w))
    saved = (normed, query_rows, weights_low, pixel_mix, mixed)
    return residual + apply(mixed, out_w), saved


def cross_block_back(
    residual, gain_vec, query_w, key_w, value_w, out_w, pixel_norm, saved, grad_out
):
    normed, query_rows, weights_low, pixel_mix, mixed = saved
    scale = 1.0 / math.sqrt(residual.shape[1])
    grad_round = rounded(grad_out)
    grad_out_w = grad_blocks(mixed, grad_round, out_w)
    grad_mixed = rounded(apply_t(grad_round, out_w))
    grad_keyed = rounded(apply(grad_mixed, value_w))
    row_dot = jnp.sum(widened(grad_keyed) * pixel_mix, axis=-1, keepdims=True)
    grad_weights = product(grad_keyed, pixel_norm)
    grad_scores = rounded(widened(weights_low) * (grad_weights - row_dot))
    score_mix = product_nt(grad_scores, pixel_norm)
    grad_query = rounded(split_apply_t(score_mix, key_w) * scale)
    grad_query_w = grad_blocks(normed, grad_query, query_w)
    grad_key_w = split_grad_blocks(query_rows, score_mix, key_w) * scale
    grad_value_w = split_grad_blocks(grad_mixed, pixel_mix, value_w)
    grad_normed = apply_t(grad_query, query_w)
    grad_residual, grad_gain = norm_backward(residual, gain_vec, grad_normed)
    return (grad_out + grad_residual, grad_query_w, grad_key_w, grad_value_w, grad_out_w, grad_gain)


def local(latents, pixels, pixel_item, cotangent, *params):
    weights, gains = params[:12], params[12:]
    items = lax.axis_size("items")
    heads = lax.axis_size("heads")
    rows = latents.shape[0]
    split = max(1, NLAT // rows)
    (
        query_cross,
        key_cross,
        value_cross,
        out_cross,
        up_cross,
        down_cross,
        query_self,
        key_self,
        value_self,
        out_self,
        up_self,
        down_self,
    ), gain_list = gather_weights(weights, gains, items, heads)
    attention_set = (query_self, key_self, value_self, out_self)

    item = (lax.axis_index("heads") * rows) // NLAT
    window, allowed = pixel_window(pixels, pixel_item[0], item)
    pixel_norm = lax.optimization_barrier(rounded(norm_pixels(widened(window))))

    start_rows = widened(latents)
    after_cross, saved_cross = cross_block(
        start_rows, gain_list[0], query_cross, key_cross, value_cross, out_cross, pixel_norm, allowed
    )
    after_mlp_one, saved_mlp_one = mlp_block(after_cross, gain_list[1], up_cross, down_cross)
    after_self, saved_self = attention_block(after_mlp_one, gain_list[2], attention_set, split)
    final_rows, saved_mlp_two = mlp_block(after_self, gain_list[3], up_self, down_self)

    grad_final = widened(cotangent)
    grad_after_self, grad_self_up, grad_self_down, grad_gain_four = mlp_block_back(
        after_self, gain_list[3], up_self, down_self, saved_mlp_two, grad_final
    )
    (
        grad_after_mlp,
        grad_self_query,
        grad_self_key,
        grad_self_value,
        grad_self_out,
        grad_gain_three,
    ) = attention_block_back(
        after_mlp_one, gain_list[2], attention_set, split, saved_self, grad_after_self
    )
    grad_after_cross, grad_cross_up, grad_cross_down, grad_gain_two = mlp_block_back(
        after_cross, gain_list[1], up_cross, down_cross, saved_mlp_one, grad_after_mlp
    )
    (
        latents_grad,
        grad_cross_query,
        grad_cross_key,
        grad_cross_value,
        grad_cross_out,
        grad_gain_one,
    ) = cross_block_back(
        start_rows,
        gain_list[0],
        query_cross,
        key_cross,
        value_cross,
        out_cross,
        pixel_norm,
        saved_cross,
        grad_after_cross,
    )
    weight_grads = (
        grad_cross_query,
        grad_cross_key,
        grad_cross_value,
        grad_cross_out,
        grad_cross_up,
        grad_cross_down,
        grad_self_query,
        grad_self_key,
        grad_self_value,
        grad_self_out,
        grad_self_up,
        grad_self_down,
    )
    gain_grads = (grad_gain_one, grad_gain_two, grad_gain_three, grad_gain_four)
    reduced = reduce_grads(weight_grads, gain_grads, weights, items, heads)
    shaped = [r.reshape(w.shape) for r, w in zip(reduced[:12], weights)]
    shaped += [r.reshape(g.shape) for r, g in zip(reduced[12:], gains)]
    return (rounded(final_rows), latents_grad, *shaped)


def solution(mesh):
    weight_specs = (
        P(ALL, None),
        P(None, ALL),
        P(None, ALL),
        P(ALL, None),
        P("items", "heads"),
        P("heads", "items"),
        P("items", "heads"),
        P("items", "heads"),
        P("items", "heads"),
        P("heads", "items"),
        P("items", "heads"),
        P("heads", "items"),
    )
    gain_specs = (P(ALL),) * 4
    placed = (P(ALL, None), P(None, "items"), P("items", None), P(ALL, None)) + weight_specs + gain_specs
    return jax.shard_map(
        local,
        mesh=mesh,
        in_specs=placed,
        out_specs=(P(ALL, None), P(ALL, None)) + weight_specs + gain_specs,
        check_vma=False,
    )
```

```python
import math

import jax
import jax.numpy as jnp
from jax import lax
from jax.sharding import PartitionSpec as P

HEAD = 128
NLAT = 512
PIX_MOST = 6144
LANE = 128

EPSILON = 1e-05
MASKED = -1e30
ALL = ("items", "heads")


def rounded(values):
    return values.astype(jnp.bfloat16)


def widened(values):
    return values.astype(jnp.float32)


def product(left_side, right_side):
    return jnp.dot(left_side, right_side, preferred_element_type=jnp.float32)


def product_tn(left_side, right_side):
    return lax.dot_general(
        left_side, right_side, (((0,), (0,)), ((), ())), preferred_element_type=jnp.float32
    )


def product_nt(left_side, right_side):
    return lax.dot_general(
        left_side, right_side, (((1,), (1,)), ((), ())), preferred_element_type=jnp.float32
    )


def split_parts(values):
    high = rounded(values)
    return high, rounded(values - widened(high))


def split_apply_t(values_f32, weight):
    high, low = split_parts(values_f32)
    return apply_t(high, weight) + apply_t(low, weight)


def norm_rows(values, gain_vec):
    centre = values - jnp.mean(values, axis=-1, keepdims=True)
    spread = jnp.mean(centre * centre, axis=-1, keepdims=True)
    return centre * lax.rsqrt(spread + EPSILON) * gain_vec


def norm_pixels(values):
    centre = values - jnp.mean(values, axis=0, keepdims=True)
    spread = jnp.mean(centre * centre, axis=0, keepdims=True)
    return centre * lax.rsqrt(spread + EPSILON)


def norm_backward(residual, gain_vec, grad_normed):
    unused, norm_back = jax.vjp(norm_rows, residual, gain_vec)
    return norm_back(grad_normed)


WEIGHT_KINDS = (
    "rows",
    "cols",
    "cols",
    "rows",
    "ih",
    "hi",
    "ih",
    "ih",
    "ih",
    "hi",
    "ih",
    "hi",
)

PANEL = 128
ROW_TILE = 16
ROW_GROUP = 48


def contract(left, right, left_dims, right_dims):
    return lax.dot_general(
        left, right, ((left_dims, right_dims), ((), ())), preferred_element_type=jnp.float32
    )


def lane_pad(values, width):
    panels = -(-width // PANEL)
    if panels * PANEL != width:
        pad = [(0, 0)] * (values.ndim - 1) + [(0, panels * PANEL - width)]
        values = jnp.pad(values, pad)
    return values.reshape(values.shape[:-1] + (panels, PANEL))


def lane_cut(values, width):
    values = values.reshape(values.shape[:-2] + (-1,))
    return values if values.shape[-1] == width else values[..., :width]


def local_panels(block):
    rows, width = block.shape
    parts = lane_pad(block, width).transpose(1, 0, 2)
    return parts.reshape(-1, PANEL)


def padded_rows(rows):
    return -(-rows // ROW_TILE) * ROW_TILE


def local_shape(w, kind):
    return (w.shape[1], w.shape[0]) if kind == "cols" else w.shape


def make_weight(piece, kind, shape, items, heads):
    rows, width = shape
    panels = -(-width // PANEL)
    blocks = piece[:, : panels * rows, :].reshape(items * heads, panels, rows, PANEL)
    if kind in ("ih", "hi"):
        blocks = blocks.reshape(items, heads, panels, rows, PANEL)
    return kind, blocks, width


def apply(values, weight):
    kind, blocks, width = weight
    count = values.shape[0]
    if kind in ("rows", "cols"):
        devices, panels, rows, lanes = blocks.shape
        out = contract(values.reshape(count, devices, rows), blocks, (1, 2), (0, 2))
        return lane_cut(out, width)
    items, heads, panels, rows, lanes = blocks.shape
    if kind == "ih":
        out = contract(values.reshape(count, items, rows), blocks, (1, 2), (0, 3))
    else:
        out = contract(values.reshape(count, heads, rows), blocks, (1, 2), (1, 3))
    return lane_cut(out, width).reshape(count, -1)


def apply_t(values, weight):
    kind, blocks, width = weight
    count = values.shape[0]
    if kind in ("rows", "cols"):
        devices, panels, rows, lanes = blocks.shape
        out = contract(lane_pad(values, width), blocks, (1, 2), (1, 3))
        return out.reshape(count, devices * rows)
    items, heads, panels, rows, lanes = blocks.shape
    if kind == "ih":
        spread = lane_pad(values.reshape(count, heads, width), width)
        out = contract(spread, blocks, (1, 2, 3), (1, 2, 4))
        return out.reshape(count, items * rows)
    spread = lane_pad(values.reshape(count, items, width), width)
    out = contract(spread, blocks, (1, 2, 3), (0, 2, 4))
    return out.reshape(count, heads * rows)


def grad_blocks(values, grads, weight):
    kind, blocks, width = weight
    count = values.shape[0]
    if kind in ("rows", "cols"):
        devices, panels, rows, lanes = blocks.shape
        out = contract(values.reshape(count, devices, rows), lane_pad(grads, width), (0,), (0,))
        out = out.transpose(0, 2, 1, 3)
    else:
        items, heads, panels, rows, lanes = blocks.shape
        devices = items * heads
        if kind == "ih":
            spread = lane_pad(grads.reshape(count, heads, width), width)
            out = contract(values.reshape(count, items, rows), spread, (0,), (0,))
            out = out.transpose(0, 2, 3, 1, 4)
        else:
            spread = lane_pad(grads.reshape(count, items, width), width)
            out = contract(values.reshape(count, heads, rows), spread, (0,), (0,))
            out = out.transpose(2, 0, 3, 1, 4)
    return out.reshape(devices, -1, PANEL)


def split_grad_blocks(values, grads_f32, weight):
    high, low = split_parts(grads_f32)
    return grad_blocks(values, high, weight) + grad_blocks(values, low, weight)


def pad_rows(block, rows):
    extra = rows - block.shape[-2]
    if extra == 0:
        return block
    pad = [(0, 0)] * (block.ndim - 2) + [(0, extra), (0, 0)]
    return jnp.pad(block, pad)


def gather_weights(weights, gains, items, heads):
    count = items * heads
    blocks = [local_panels(rounded(w.T if kind == "cols" else w)) for w, kind in zip(weights, WEIGHT_KINDS)]
    large = [k for k, kind in enumerate(WEIGHT_KINDS) if kind != "cols"]
    small = [k for k, kind in enumerate(WEIGHT_KINDS) if kind == "cols"]
    slot = padded_rows(max(blocks[k].shape[0] for k in large))
    gain_row = rounded(jnp.concatenate(gains)).reshape(1, -1)
    tail, places, row = [], {}, 0
    for k in small:
        places[k] = (row, blocks[k].shape[0])
        tail.append(blocks[k])
        row += blocks[k].shape[0]
    gain_place = (row, 1)
    tail.append(local_panels(gain_row))
    row += tail[-1].shape[0]
    tail_slots = -(-row // slot)
    tail_block = pad_rows(jnp.concatenate(tail, axis=0), tail_slots * slot)
    packed = jnp.stack([pad_rows(blocks[k], slot) for k in large] + list(tail_block.reshape(tail_slots, slot, PANEL)))
    gathered = lax.all_gather(packed, ALL, axis=1, tiled=False)
    out = [None] * len(weights)
    for position, k in enumerate(large):
        shape = local_shape(weights[k], WEIGHT_KINDS[k])
        out[k] = make_weight(gathered[position], WEIGHT_KINDS[k], shape, items, heads)
    rest = gathered[len(large) :].transpose(1, 0, 2, 3).reshape(count, tail_slots * slot, PANEL)
    for k in small:
        first, rows = places[k]
        shape = local_shape(weights[k], WEIGHT_KINDS[k])
        out[k] = make_weight(rest[:, first : first + rows, :], WEIGHT_KINDS[k], shape, items, heads)
    first, rows = gain_place
    gain_all = rest[:, first : first + rows, :].reshape(count, -1)[:, : gain_row.shape[1]]
    gain_all = gain_all.reshape(count, len(gains), -1)
    whole_gains = [widened(gain_all[:, k, :].reshape(-1)) for k in range(len(gains))]
    return out, whole_gains


def reduce_grads(grad_parts, gain_grads, weights, items, heads):
    count = items * heads
    pieces, places, row = [], [], 0
    for part in grad_parts:
        rows = padded_rows(part.shape[1])
        pieces.append(pad_rows(rounded(part), rows))
        places.append((row, part.shape[1]))
        row += rows
    gain_stack = jnp.stack([g.reshape(count, -1) for g in gain_grads], axis=1).reshape(count, 1, -1)
    gain_block = lane_pad(gain_stack, gain_stack.shape[-1]).reshape(count, -1, PANEL)
    total = -(-(row + gain_block.shape[1]) // ROW_GROUP) * ROW_GROUP
    pieces.append(pad_rows(rounded(gain_block), total - row))
    places.append((row, gain_block.shape[1]))
    packed = jnp.concatenate(pieces, axis=1)
    mine = lax.psum_scatter(
        packed.reshape(count * total, PANEL), "items", scatter_dimension=0, tiled=True
    )
    mine = lax.psum_scatter(mine, "heads", scatter_dimension=0, tiled=True)
    out = []
    for w, kind, (first, rows) in zip(weights, WEIGHT_KINDS, places):
        r, width = local_shape(w, kind)
        panels = -(-width // PANEL)
        block = mine[first : first + rows].reshape(panels, r, PANEL).transpose(1, 0, 2)
        block = widened(lane_cut(block, width))
        out.append(block.T if kind == "cols" else block)
    first, rows = places[-1]
    gain_part = widened(mine[first : first + rows].reshape(-1)[: gain_stack.shape[-1]])
    gain_part = gain_part.reshape(len(gain_grads), -1)
    out += [gain_part[k] for k in range(len(gain_grads))]
    return out


def mlp_block(residual, gain_vec, up_w, down_w):
    normed = rounded(norm_rows(residual, gain_vec))
    before = apply(normed, up_w)
    hidden = rounded(jax.nn.gelu(before))
    return residual + apply(hidden, down_w), (normed, before, hidden)


def mlp_block_back(residual, gain_vec, up_w, down_w, saved, grad_out):
    normed, before, hidden = saved
    grad_round = rounded(grad_out)
    grad_down = grad_blocks(hidden, grad_round, down_w)
    grad_hidden = apply_t(grad_round, down_w)
    unused, gelu_back = jax.vjp(jax.nn.gelu, before)
    grad_before = rounded(gelu_back(grad_hidden)[0])
    grad_up = grad_blocks(normed, grad_before, up_w)
    grad_normed = apply_t(grad_before, up_w)
    grad_residual, grad_gain = norm_backward(residual, gain_vec, grad_normed)
    return grad_out + grad_residual, grad_up, grad_down, grad_gain


def exchange_rows(rows, split):
    if split == 1:
        return [rows]
    heads = lax.axis_size("heads")
    out = [rows]
    for shift in range(1, split):
        pairs = []
        for h in range(heads):
            base, pos = (h // split) * split, h % split
            pairs.append((h, base + (pos - shift) % split))
        out.append(lax.ppermute(rows, "heads", pairs))
    return out


def return_rows(parts, split):
    total = parts[0]
    heads = lax.axis_size("heads")
    for shift in range(1, split):
        pairs = []
        for h in range(heads):
            base, pos = (h // split) * split, h % split
            pairs.append((h, base + (pos + shift) % split))
        total = total + lax.ppermute(parts[shift], "heads", pairs)
    return total


def attention_block(residual, gain_vec, weight_set, split):
    query_w, key_w, value_w, out_w = weight_set
    rows = residual.shape[0]
    normed = rounded(norm_rows(residual, gain_vec))
    query_rows = rounded(apply(normed, query_w))
    key_rows = rounded(apply(normed, key_w))
    value_rows = rounded(apply(normed, value_w))
    heads_n = query_rows.shape[1] // HEAD
    key_all = jnp.concatenate(exchange_rows(key_rows, split), axis=0)
    value_all = jnp.concatenate(exchange_rows(value_rows, split), axis=0)
    keys = key_all.shape[0]
    q4 = query_rows.reshape(rows, heads_n, HEAD)
    k4 = key_all.reshape(keys, heads_n, HEAD)
    v4 = value_all.reshape(keys, heads_n, HEAD)
    scores = jnp.einsum("qhd,khd->hqk", q4, k4, preferred_element_type=jnp.float32) * (
        1.0 / math.sqrt(HEAD)
    )
    row_top = jnp.max(scores, axis=-1, keepdims=True)
    raw_weights = jnp.exp(scores - row_top)
    row_total = jnp.sum(raw_weights, axis=-1, keepdims=True)
    weights_low = rounded(raw_weights / row_total)
    mixed_full = jnp.einsum("hqk,khd->qhd", weights_low, v4, preferred_element_type=jnp.float32)
    mixed = rounded(mixed_full.reshape(rows, heads_n * HEAD))
    saved = (normed, q4, k4, v4, weights_low, mixed_full, mixed)
    return residual + apply(mixed, out_w), saved


def attention_block_back(residual, gain_vec, weight_set, split, saved, grad_out):
    query_w, key_w, value_w, out_w = weight_set
    normed, q4, k4, v4, weights_low, mixed_full, mixed = saved
    rows = residual.shape[0]
    keys = k4.shape[0]
    scale = 1.0 / math.sqrt(HEAD)
    grad_round = rounded(grad_out)
    grad_out_w = grad_blocks(mixed, grad_round, out_w)
    grad_mixed = rounded(apply_t(grad_round, out_w)).reshape(q4.shape)
    grad_value = jnp.einsum(
        "hqk,qhd->khd", weights_low, grad_mixed, preferred_element_type=jnp.float32
    ).reshape(keys, -1)
    row_dot = jnp.sum(widened(grad_mixed) * mixed_full, axis=-1).T[:, :, None]
    grad_weights = jnp.einsum("qhd,khd->hqk", grad_mixed, v4, preferred_element_type=jnp.float32)
    grad_scores = rounded(widened(weights_low) * (grad_weights - row_dot))
    grad_query = jnp.einsum("hqk,khd->qhd", grad_scores, k4, preferred_element_type=jnp.float32)
    grad_query = rounded((grad_query * scale).reshape(rows, -1))
    grad_key = jnp.einsum("hqk,qhd->khd", grad_scores, q4, preferred_element_type=jnp.float32)
    grad_key = (grad_key * scale).reshape(keys, -1)
    if split > 1:
        grad_key = return_rows(jnp.split(grad_key, split, axis=0), split)
        grad_value = return_rows(jnp.split(grad_value, split, axis=0), split)
    grad_key = rounded(grad_key)
    grad_value = rounded(grad_value)
    grad_query_w = grad_blocks(normed, grad_query, query_w)
    grad_key_w = grad_blocks(normed, grad_key, key_w)
    grad_value_w = grad_blocks(normed, grad_value, value_w)
    grad_normed = (
        apply_t(grad_query, query_w) + apply_t(grad_key, key_w) + apply_t(grad_value, value_w)
    )
    grad_residual, grad_gain = norm_backward(residual, gain_vec, grad_normed)
    return (grad_out + grad_residual, grad_query_w, grad_key_w, grad_value_w, grad_out_w, grad_gain)


def pixel_window(pixels, item_ids, item):
    count = pixels.shape[1]
    width = min(count, -(-PIX_MOST // LANE) * LANE + LANE)
    start = jnp.sum((item_ids < item).astype(jnp.int32))
    first = jnp.clip((start // LANE) * LANE, 0, count - width)
    window = lax.dynamic_slice_in_dim(pixels, first, width, axis=1)
    ids = lax.dynamic_slice_in_dim(item_ids, first, width, axis=0)
    return window, ids == item


def cross_block(residual, gain_vec, query_w, key_w, value_w, out_w, pixel_norm, allowed):
    scale = 1.0 / math.sqrt(residual.shape[1])
    normed = rounded(norm_rows(residual, gain_vec))
    query_rows = rounded(apply(normed, query_w))
    query_keyed = rounded(apply(query_rows, key_w) * scale)
    scores = jnp.where(allowed[None, :], product(query_keyed, pixel_norm), MASKED)
    row_top = jnp.max(scores, axis=-1, keepdims=True)
    raw_weights = jnp.exp(scores - row_top)
    row_total = jnp.sum(raw_weights, axis=-1, keepdims=True)
    weights_low = rounded(raw_weights / row_total)
    pixel_mix = product_nt(weights_low, pixel_norm)
    mixed = rounded(split_apply_t(pixel_mix, value_w))
    saved = (normed, query_rows, weights_low, pixel_mix, mixed)
    return residual + apply(mixed, out_w), saved


def cross_block_back(
    residual, gain_vec, query_w, key_w, value_w, out_w, pixel_norm, saved, grad_out
):
    normed, query_rows, weights_low, pixel_mix, mixed = saved
    scale = 1.0 / math.sqrt(residual.shape[1])
    grad_round = rounded(grad_out)
    grad_out_w = grad_blocks(mixed, grad_round, out_w)
    grad_mixed = rounded(apply_t(grad_round, out_w))
    grad_keyed = rounded(apply(grad_mixed, value_w))
    row_dot = jnp.sum(widened(grad_keyed) * pixel_mix, axis=-1, keepdims=True)
    grad_weights = product(grad_keyed, pixel_norm)
    grad_scores = rounded(widened(weights_low) * (grad_weights - row_dot))
    score_mix = product_nt(grad_scores, pixel_norm)
    grad_query = rounded(split_apply_t(score_mix, key_w) * scale)
    grad_query_w = grad_blocks(normed, grad_query, query_w)
    grad_key_w = split_grad_blocks(query_rows, score_mix, key_w) * scale
    grad_value_w = split_grad_blocks(grad_mixed, pixel_mix, value_w)
    grad_normed = apply_t(grad_query, query_w)
    grad_residual, grad_gain = norm_backward(residual, gain_vec, grad_normed)
    return (grad_out + grad_residual, grad_query_w, grad_key_w, grad_value_w, grad_out_w, grad_gain)


def local(latents, pixels, pixel_item, cotangent, *params):
    weights, gains = params[:12], params[12:]
    items = lax.axis_size("items")
    heads = lax.axis_size("heads")
    rows = latents.shape[0]
    split = max(1, NLAT // rows)
    (
        query_cross,
        key_cross,
        value_cross,
        out_cross,
        up_cross,
        down_cross,
        query_self,
        key_self,
        value_self,
        out_self,
        up_self,
        down_self,
    ), gain_list = gather_weights(weights, gains, items, heads)
    attention_set = (query_self, key_self, value_self, out_self)

    item = (lax.axis_index("heads") * rows) // NLAT
    window, allowed = pixel_window(pixels, pixel_item[0], item)
    pixel_norm = lax.optimization_barrier(rounded(norm_pixels(widened(window))))

    start_rows = widened(latents)
    after_cross, saved_cross = cross_block(
        start_rows, gain_list[0], query_cross, key_cross, value_cross, out_cross, pixel_norm, allowed
    )
    after_mlp_one, saved_mlp_one = mlp_block(after_cross, gain_list[1], up_cross, down_cross)
    after_self, saved_self = attention_block(after_mlp_one, gain_list[2], attention_set, split)
    final_rows, saved_mlp_two = mlp_block(after_self, gain_list[3], up_self, down_self)

    grad_final = widened(cotangent)
    grad_after_self, grad_self_up, grad_self_down, grad_gain_four = mlp_block_back(
        after_self, gain_list[3], up_self, down_self, saved_mlp_two, grad_final
    )
    (
        grad_after_mlp,
        grad_self_query,
        grad_self_key,
        grad_self_value,
        grad_self_out,
        grad_gain_three,
    ) = attention_block_back(
        after_mlp_one, gain_list[2], attention_set, split, saved_self, grad_after_self
    )
    grad_after_cross, grad_cross_up, grad_cross_down, grad_gain_two = mlp_block_back(
        after_cross, gain_list[1], up_cross, down_cross, saved_mlp_one, grad_after_mlp
    )
    (
        latents_grad,
        grad_cross_query,
        grad_cross_key,
        grad_cross_value,
        grad_cross_out,
        grad_gain_one,
    ) = cross_block_back(
        start_rows,
        gain_list[0],
        query_cross,
        key_cross,
        value_cross,
        out_cross,
        pixel_norm,
        saved_cross,
        grad_after_cross,
    )
    weight_grads = (
        grad_cross_query,
        grad_cross_key,
        grad_cross_value,
        grad_cross_out,
        grad_cross_up,
        grad_cross_down,
        grad_self_query,
        grad_self_key,
        grad_self_value,
        grad_self_out,
        grad_self_up,
        grad_self_down,
    )
    gain_grads = (grad_gain_one, grad_gain_two, grad_gain_three, grad_gain_four)
    reduced = reduce_grads(weight_grads, gain_grads, weights, items, heads)
    shaped = [r.reshape(w.shape) for r, w in zip(reduced[:12], weights)]
    shaped += [r.reshape(g.shape) for r, g in zip(reduced[12:], gains)]
    return (rounded(final_rows), latents_grad, *shaped)


def solution(mesh):
    weight_specs = (
        P(ALL, None),
        P(None, ALL),
        P(None, ALL),
        P(ALL, None),
        P("items", "heads"),
        P("heads", "items"),
        P("items", "heads"),
        P("items", "heads"),
        P("items", "heads"),
        P("heads", "items"),
        P("items", "heads"),
        P("heads", "items"),
    )
    gain_specs = (P(ALL),) * 4
    placed = (P(ALL, None), P(None, "items"), P("items", None), P(ALL, None)) + weight_specs + gain_specs
    return jax.shard_map(
        local,
        mesh=mesh,
        in_specs=placed,
        out_specs=(P(ALL, None), P(ALL, None)) + weight_specs + gain_specs,
        check_vma=False,
    )
```

```python
import math

import jax
import jax.numpy as jnp
from jax import lax
from jax.experimental import pallas as pl
from jax.experimental.pallas import tpu as pltpu
from jax.sharding import PartitionSpec as P

HEAD = 128
NLAT = 512
PIX_MOST = 6144
LANE = 128

EPSILON = 1e-05
MASKED = -1e30
ALL = ("items", "heads")


def rounded(values):
    return values.astype(jnp.bfloat16)


def widened(values):
    return values.astype(jnp.float32)


def product(left_side, right_side):
    return jnp.dot(left_side, right_side, preferred_element_type=jnp.float32)


def product_tn(left_side, right_side):
    return lax.dot_general(
        left_side, right_side, (((0,), (0,)), ((), ())), preferred_element_type=jnp.float32
    )


def product_nt(left_side, right_side):
    return lax.dot_general(
        left_side, right_side, (((1,), (1,)), ((), ())), preferred_element_type=jnp.float32
    )


def split_parts(values):
    high = rounded(values)
    return high, rounded(values - widened(high))


def split_apply_t(values_f32, weight):
    high, low = split_parts(values_f32)
    return apply_t(high, weight) + apply_t(low, weight)


def norm_rows(values, gain_vec):
    centre = values - jnp.mean(values, axis=-1, keepdims=True)
    spread = jnp.mean(centre * centre, axis=-1, keepdims=True)
    return centre * lax.rsqrt(spread + EPSILON) * gain_vec


def norm_pixels(values):
    centre = values - jnp.mean(values, axis=0, keepdims=True)
    spread = jnp.mean(centre * centre, axis=0, keepdims=True)
    return centre * lax.rsqrt(spread + EPSILON)


def norm_backward(residual, gain_vec, grad_normed):
    unused, norm_back = jax.vjp(norm_rows, residual, gain_vec)
    return norm_back(grad_normed)


WEIGHT_KINDS = (
    "rows",
    "cols",
    "cols",
    "rows",
    "ih",
    "hi",
    "ih",
    "ih",
    "ih",
    "hi",
    "ih",
    "hi",
)

PANEL = 128
ROW_TILE = 16
ROW_GROUP = 48


def contract(left, right, left_dims, right_dims):
    return lax.dot_general(
        left, right, ((left_dims, right_dims), ((), ())), preferred_element_type=jnp.float32
    )


def lane_pad(values, width):
    panels = -(-width // PANEL)
    if panels * PANEL != width:
        pad = [(0, 0)] * (values.ndim - 1) + [(0, panels * PANEL - width)]
        values = jnp.pad(values, pad)
    return values.reshape(values.shape[:-1] + (panels, PANEL))


def lane_cut(values, width):
    values = values.reshape(values.shape[:-2] + (-1,))
    return values if values.shape[-1] == width else values[..., :width]


def local_panels(block):
    rows, width = block.shape
    parts = lane_pad(block, width).transpose(1, 0, 2)
    return parts.reshape(-1, PANEL)


def padded_rows(rows):
    return -(-rows // ROW_TILE) * ROW_TILE


def local_shape(w, kind):
    return (w.shape[1], w.shape[0]) if kind == "cols" else w.shape


def make_weight(piece, kind, shape, items, heads):
    rows, width = shape
    panels = -(-width // PANEL)
    blocks = piece[:, : panels * rows, :].reshape(items * heads, panels, rows, PANEL)
    if kind in ("ih", "hi"):
        blocks = blocks.reshape(items, heads, panels, rows, PANEL)
    return kind, blocks, width


def apply(values, weight):
    kind, blocks, width = weight
    count = values.shape[0]
    if kind in ("rows", "cols"):
        devices, panels, rows, lanes = blocks.shape
        out = contract(values.reshape(count, devices, rows), blocks, (1, 2), (0, 2))
        return lane_cut(out, width)
    items, heads, panels, rows, lanes = blocks.shape
    if kind == "ih":
        out = contract(values.reshape(count, items, rows), blocks, (1, 2), (0, 3))
    else:
        out = contract(values.reshape(count, heads, rows), blocks, (1, 2), (1, 3))
    return lane_cut(out, width).reshape(count, -1)


def apply_t(values, weight):
    kind, blocks, width = weight
    count = values.shape[0]
    if kind in ("rows", "cols"):
        devices, panels, rows, lanes = blocks.shape
        out = contract(lane_pad(values, width), blocks, (1, 2), (1, 3))
        return out.reshape(count, devices * rows)
    items, heads, panels, rows, lanes = blocks.shape
    if kind == "ih":
        spread = lane_pad(values.reshape(count, heads, width), width)
        out = contract(spread, blocks, (1, 2, 3), (1, 2, 4))
        return out.reshape(count, items * rows)
    spread = lane_pad(values.reshape(count, items, width), width)
    out = contract(spread, blocks, (1, 2, 3), (0, 2, 4))
    return out.reshape(count, heads * rows)


def grad_blocks(values, grads, weight):
    kind, blocks, width = weight
    count = values.shape[0]
    if kind in ("rows", "cols"):
        devices, panels, rows, lanes = blocks.shape
        out = contract(values.reshape(count, devices, rows), lane_pad(grads, width), (0,), (0,))
        out = out.transpose(0, 2, 1, 3)
    else:
        items, heads, panels, rows, lanes = blocks.shape
        devices = items * heads
        if kind == "ih":
            spread = lane_pad(grads.reshape(count, heads, width), width)
            out = contract(values.reshape(count, items, rows), spread, (0,), (0,))
            out = out.transpose(0, 2, 3, 1, 4)
        else:
            spread = lane_pad(grads.reshape(count, items, width), width)
            out = contract(values.reshape(count, heads, rows), spread, (0,), (0,))
            out = out.transpose(2, 0, 3, 1, 4)
    return out.reshape(devices, -1, PANEL)


def split_grad_blocks(values, grads_f32, weight):
    high, low = split_parts(grads_f32)
    return grad_blocks(values, high, weight) + grad_blocks(values, low, weight)


def pad_rows(block, rows):
    extra = rows - block.shape[-2]
    if extra == 0:
        return block
    pad = [(0, 0)] * (block.ndim - 2) + [(0, extra), (0, 0)]
    return jnp.pad(block, pad)


def gather_weights(weights, gains, items, heads):
    count = items * heads
    pieces, places, row = [], [], 0
    for w, kind in zip(weights, WEIGHT_KINDS):
        block = local_panels(rounded(w.T if kind == "cols" else w))
        rows = padded_rows(block.shape[0])
        pieces.append(pad_rows(block, rows))
        places.append((row, rows))
        row += rows
    gain_row = rounded(jnp.concatenate(gains)).reshape(1, -1)
    gain_block = local_panels(gain_row)
    total = -(-(row + gain_block.shape[0]) // ROW_GROUP) * ROW_GROUP
    pieces.append(pad_rows(gain_block, total - row))
    places.append((row, gain_block.shape[0]))
    packed = jnp.concatenate(pieces, axis=0)
    gathered = lax.all_gather(packed, ALL, axis=0, tiled=True).reshape(count, total, PANEL)
    out = []
    for w, kind, (first, rows) in zip(weights, WEIGHT_KINDS, places):
        piece = gathered[:, first : first + rows, :]
        out.append(make_weight(piece, kind, local_shape(w, kind), items, heads))
    first, rows = places[-1]
    gain_all = gathered[:, first : first + rows, :].reshape(count, -1)[:, : gain_row.shape[1]]
    gain_all = gain_all.reshape(count, len(gains), -1)
    whole_gains = [widened(gain_all[:, k, :].reshape(-1)) for k in range(len(gains))]
    return out, whole_gains


def reduce_grads(grad_parts, gain_grads, weights, items, heads):
    count = items * heads
    pieces, places, row = [], [], 0
    for part in grad_parts:
        rows = padded_rows(part.shape[1])
        pieces.append(pad_rows(rounded(part), rows))
        places.append((row, part.shape[1]))
        row += rows
    gain_stack = jnp.stack([g.reshape(count, -1) for g in gain_grads], axis=1).reshape(count, 1, -1)
    gain_block = lane_pad(gain_stack, gain_stack.shape[-1]).reshape(count, -1, PANEL)
    total = -(-(row + gain_block.shape[1]) // ROW_GROUP) * ROW_GROUP
    pieces.append(pad_rows(rounded(gain_block), total - row))
    places.append((row, gain_block.shape[1]))
    packed = jnp.concatenate(pieces, axis=1)
    mine = lax.psum_scatter(
        packed.reshape(count * total, PANEL), "items", scatter_dimension=0, tiled=True
    )
    mine = lax.psum_scatter(mine, "heads", scatter_dimension=0, tiled=True)
    out = []
    for w, kind, (first, rows) in zip(weights, WEIGHT_KINDS, places):
        r, width = local_shape(w, kind)
        panels = -(-width // PANEL)
        block = mine[first : first + rows].reshape(panels, r, PANEL).transpose(1, 0, 2)
        block = widened(lane_cut(block, width))
        out.append(block.T if kind == "cols" else block)
    first, rows = places[-1]
    gain_part = widened(mine[first : first + rows].reshape(-1)[: gain_stack.shape[-1]])
    gain_part = gain_part.reshape(len(gain_grads), -1)
    out += [gain_part[k] for k in range(len(gain_grads))]
    return out


def mlp_block(residual, gain_vec, up_w, down_w):
    normed = rounded(norm_rows(residual, gain_vec))
    before = apply(normed, up_w)
    hidden = rounded(jax.nn.gelu(before))
    return residual + apply(hidden, down_w), (normed, before, hidden)


def mlp_block_back(residual, gain_vec, up_w, down_w, saved, grad_out):
    normed, before, hidden = saved
    grad_round = rounded(grad_out)
    grad_down = grad_blocks(hidden, grad_round, down_w)
    grad_hidden = apply_t(grad_round, down_w)
    unused, gelu_back = jax.vjp(jax.nn.gelu, before)
    grad_before = rounded(gelu_back(grad_hidden)[0])
    grad_up = grad_blocks(normed, grad_before, up_w)
    grad_normed = apply_t(grad_before, up_w)
    grad_residual, grad_gain = norm_backward(residual, gain_vec, grad_normed)
    return grad_out + grad_residual, grad_up, grad_down, grad_gain


def exchange_rows(rows, split):
    if split == 1:
        return [rows]
    heads = lax.axis_size("heads")
    out = [rows]
    for shift in range(1, split):
        pairs = []
        for h in range(heads):
            base, pos = (h // split) * split, h % split
            pairs.append((h, base + (pos - shift) % split))
        out.append(lax.ppermute(rows, "heads", pairs))
    return out


def return_rows(parts, split):
    total = parts[0]
    heads = lax.axis_size("heads")
    for shift in range(1, split):
        pairs = []
        for h in range(heads):
            base, pos = (h // split) * split, h % split
            pairs.append((h, base + (pos + shift) % split))
        total = total + lax.ppermute(parts[shift], "heads", pairs)
    return total


def attention_block(residual, gain_vec, weight_set, split):
    query_w, key_w, value_w, out_w = weight_set
    rows = residual.shape[0]
    normed = rounded(norm_rows(residual, gain_vec))
    query_rows = rounded(apply(normed, query_w))
    key_rows = rounded(apply(normed, key_w))
    value_rows = rounded(apply(normed, value_w))
    heads_n = query_rows.shape[1] // HEAD
    key_all = jnp.concatenate(exchange_rows(key_rows, split), axis=0)
    value_all = jnp.concatenate(exchange_rows(value_rows, split), axis=0)
    keys = key_all.shape[0]
    q4 = query_rows.reshape(rows, heads_n, HEAD)
    k4 = key_all.reshape(keys, heads_n, HEAD)
    v4 = value_all.reshape(keys, heads_n, HEAD)
    scores = jnp.einsum("qhd,khd->hqk", q4, k4, preferred_element_type=jnp.float32) * (
        1.0 / math.sqrt(HEAD)
    )
    row_top = jnp.max(scores, axis=-1, keepdims=True)
    raw_weights = jnp.exp(scores - row_top)
    row_total = jnp.sum(raw_weights, axis=-1, keepdims=True)
    weights_low = rounded(raw_weights / row_total)
    mixed_full = jnp.einsum("hqk,khd->qhd", weights_low, v4, preferred_element_type=jnp.float32)
    mixed = rounded(mixed_full.reshape(rows, heads_n * HEAD))
    saved = (normed, q4, k4, v4, weights_low, mixed_full, mixed)
    return residual + apply(mixed, out_w), saved


def attention_block_back(residual, gain_vec, weight_set, split, saved, grad_out):
    query_w, key_w, value_w, out_w = weight_set
    normed, q4, k4, v4, weights_low, mixed_full, mixed = saved
    rows = residual.shape[0]
    keys = k4.shape[0]
    scale = 1.0 / math.sqrt(HEAD)
    grad_round = rounded(grad_out)
    grad_out_w = grad_blocks(mixed, grad_round, out_w)
    grad_mixed = rounded(apply_t(grad_round, out_w)).reshape(q4.shape)
    grad_value = jnp.einsum(
        "hqk,qhd->khd", weights_low, grad_mixed, preferred_element_type=jnp.float32
    ).reshape(keys, -1)
    row_dot = jnp.sum(widened(grad_mixed) * mixed_full, axis=-1).T[:, :, None]
    grad_weights = jnp.einsum("qhd,khd->hqk", grad_mixed, v4, preferred_element_type=jnp.float32)
    grad_scores = rounded(widened(weights_low) * (grad_weights - row_dot))
    grad_query = jnp.einsum("hqk,khd->qhd", grad_scores, k4, preferred_element_type=jnp.float32)
    grad_query = rounded((grad_query * scale).reshape(rows, -1))
    grad_key = jnp.einsum("hqk,qhd->khd", grad_scores, q4, preferred_element_type=jnp.float32)
    grad_key = (grad_key * scale).reshape(keys, -1)
    if split > 1:
        grad_key = return_rows(jnp.split(grad_key, split, axis=0), split)
        grad_value = return_rows(jnp.split(grad_value, split, axis=0), split)
    grad_key = rounded(grad_key)
    grad_value = rounded(grad_value)
    grad_query_w = grad_blocks(normed, grad_query, query_w)
    grad_key_w = grad_blocks(normed, grad_key, key_w)
    grad_value_w = grad_blocks(normed, grad_value, value_w)
    grad_normed = (
        apply_t(grad_query, query_w) + apply_t(grad_key, key_w) + apply_t(grad_value, value_w)
    )
    grad_residual, grad_gain = norm_backward(residual, gain_vec, grad_normed)
    return (grad_out + grad_residual, grad_query_w, grad_key_w, grad_value_w, grad_out_w, grad_gain)


def pixel_window(pixels, item_ids, item):
    count = pixels.shape[1]
    width = min(count, -(-PIX_MOST // LANE) * LANE + LANE)
    start = jnp.sum((item_ids < item).astype(jnp.int32))
    first = jnp.clip((start // LANE) * LANE, 0, count - width)
    window = lax.dynamic_slice_in_dim(pixels, first, width, axis=1)
    ids = lax.dynamic_slice_in_dim(item_ids, first, width, axis=0)
    return window, ids == item


SOFTMAX_ROWS = 128


def softmax_mix_kernel(keyed_ref, pixel_ref, mask_ref, weights_ref, mix_ref):
    scores = jnp.dot(keyed_ref[...], pixel_ref[...], preferred_element_type=jnp.float32)
    scores = jnp.where(mask_ref[...] > 0.0, scores, MASKED)
    row_top = jnp.max(scores, axis=-1, keepdims=True)
    raw = jnp.exp(scores - row_top)
    row_total = jnp.sum(raw, axis=-1, keepdims=True)
    weights = (raw / row_total).astype(jnp.bfloat16)
    weights_ref[...] = weights
    mix_ref[...] = lax.dot_general(
        weights, pixel_ref[...], (((1,), (1,)), ((), ())), preferred_element_type=jnp.float32
    )


def softmax_mix(keyed, pixel_pad, mask):
    rows, channels = keyed.shape
    width = pixel_pad.shape[1]
    block = min(SOFTMAX_ROWS, rows)
    cost = pl.CostEstimate(
        flops=4 * rows * channels * width,
        transcendentals=rows * width,
        bytes_accessed=2 * (rows * channels + channels * width + rows * width) + 4 * rows * channels,
    )
    return pl.pallas_call(
        softmax_mix_kernel,
        grid=(rows // block,),
        in_specs=[
            pl.BlockSpec((block, channels), lambda i: (i, 0)),
            pl.BlockSpec((channels, width), lambda i: (0, 0)),
            pl.BlockSpec((1, width), lambda i: (0, 0)),
        ],
        out_specs=[
            pl.BlockSpec((block, width), lambda i: (i, 0)),
            pl.BlockSpec((block, channels), lambda i: (i, 0)),
        ],
        out_shape=[
            jax.ShapeDtypeStruct((rows, width), jnp.bfloat16),
            jax.ShapeDtypeStruct((rows, channels), jnp.float32),
        ],
        compiler_params=pltpu.CompilerParams(vmem_limit_bytes=48 * 1024 * 1024),
        cost_estimate=cost,
    )(keyed, pixel_pad, mask)


def cross_block(residual, gain_vec, query_w, key_w, value_w, out_w, pixel_norm, allowed):
    scale = 1.0 / math.sqrt(residual.shape[1])
    normed = rounded(norm_rows(residual, gain_vec))
    query_rows = rounded(apply(normed, query_w))
    query_keyed = rounded(apply(query_rows, key_w) * scale)
    pixel_pad, mask = allowed
    channels = pixel_norm.shape[0]
    keyed_pad = jnp.pad(query_keyed, ((0, 0), (0, pixel_pad.shape[0] - channels)))
    weights_low, pixel_mix = softmax_mix(keyed_pad, pixel_pad, mask)
    pixel_mix = pixel_mix[:, :channels]
    mixed = rounded(split_apply_t(pixel_mix, value_w))
    saved = (normed, query_rows, weights_low, pixel_mix, mixed)
    return residual + apply(mixed, out_w), saved


def cross_block_back(
    residual, gain_vec, query_w, key_w, value_w, out_w, pixel_norm, saved, grad_out
):
    normed, query_rows, weights_low, pixel_mix, mixed = saved
    scale = 1.0 / math.sqrt(residual.shape[1])
    grad_round = rounded(grad_out)
    grad_out_w = grad_blocks(mixed, grad_round, out_w)
    grad_mixed = rounded(apply_t(grad_round, out_w))
    grad_keyed = rounded(apply(grad_mixed, value_w))
    row_dot = jnp.sum(widened(grad_keyed) * pixel_mix, axis=-1, keepdims=True)
    grad_weights = product(grad_keyed, pixel_norm)
    grad_scores = rounded(widened(weights_low) * (grad_weights - row_dot))
    score_mix = product_nt(grad_scores, pixel_norm)
    grad_query = rounded(split_apply_t(score_mix, key_w) * scale)
    grad_query_w = grad_blocks(normed, grad_query, query_w)
    grad_key_w = split_grad_blocks(query_rows, score_mix, key_w) * scale
    grad_value_w = split_grad_blocks(grad_mixed, pixel_mix, value_w)
    grad_normed = apply_t(grad_query, query_w)
    grad_residual, grad_gain = norm_backward(residual, gain_vec, grad_normed)
    return (grad_out + grad_residual, grad_query_w, grad_key_w, grad_value_w, grad_out_w, grad_gain)


def local(latents, pixels, pixel_item, cotangent, *params):
    weights, gains = params[:12], params[12:]
    items = lax.axis_size("items")
    heads = lax.axis_size("heads")
    rows = latents.shape[0]
    split = max(1, NLAT // rows)
    (
        query_cross,
        key_cross,
        value_cross,
        out_cross,
        up_cross,
        down_cross,
        query_self,
        key_self,
        value_self,
        out_self,
        up_self,
        down_self,
    ), gain_list = gather_weights(weights, gains, items, heads)
    attention_set = (query_self, key_self, value_self, out_self)

    item = (lax.axis_index("heads") * rows) // NLAT
    window, allowed = pixel_window(pixels, pixel_item[0], item)
    pixel_norm = rounded(norm_pixels(widened(window)))
    channels = pixel_norm.shape[0]
    pixel_pad = jnp.pad(pixel_norm, ((0, -channels % LANE), (0, 0)))
    mask = allowed.astype(jnp.float32)[None, :]
    pixel_norm, pixel_pad, mask = lax.optimization_barrier((pixel_norm, pixel_pad, mask))
    allowed = (pixel_pad, mask)

    start_rows = widened(latents)
    after_cross, saved_cross = cross_block(
        start_rows, gain_list[0], query_cross, key_cross, value_cross, out_cross, pixel_norm, allowed
    )
    after_mlp_one, saved_mlp_one = mlp_block(after_cross, gain_list[1], up_cross, down_cross)
    after_self, saved_self = attention_block(after_mlp_one, gain_list[2], attention_set, split)
    final_rows, saved_mlp_two = mlp_block(after_self, gain_list[3], up_self, down_self)

    grad_final = widened(cotangent)
    grad_after_self, grad_self_up, grad_self_down, grad_gain_four = mlp_block_back(
        after_self, gain_list[3], up_self, down_self, saved_mlp_two, grad_final
    )
    (
        grad_after_mlp,
        grad_self_query,
        grad_self_key,
        grad_self_value,
        grad_self_out,
        grad_gain_three,
    ) = attention_block_back(
        after_mlp_one, gain_list[2], attention_set, split, saved_self, grad_after_self
    )
    grad_after_cross, grad_cross_up, grad_cross_down, grad_gain_two = mlp_block_back(
        after_cross, gain_list[1], up_cross, down_cross, saved_mlp_one, grad_after_mlp
    )
    (
        latents_grad,
        grad_cross_query,
        grad_cross_key,
        grad_cross_value,
        grad_cross_out,
        grad_gain_one,
    ) = cross_block_back(
        start_rows,
        gain_list[0],
        query_cross,
        key_cross,
        value_cross,
        out_cross,
        pixel_norm,
        saved_cross,
        grad_after_cross,
    )
    weight_grads = (
        grad_cross_query,
        grad_cross_key,
        grad_cross_value,
        grad_cross_out,
        grad_cross_up,
        grad_cross_down,
        grad_self_query,
        grad_self_key,
        grad_self_value,
        grad_self_out,
        grad_self_up,
        grad_self_down,
    )
    gain_grads = (grad_gain_one, grad_gain_two, grad_gain_three, grad_gain_four)
    reduced = reduce_grads(weight_grads, gain_grads, weights, items, heads)
    shaped = [r.reshape(w.shape) for r, w in zip(reduced[:12], weights)]
    shaped += [r.reshape(g.shape) for r, g in zip(reduced[12:], gains)]
    return (rounded(final_rows), latents_grad, *shaped)


def solution(mesh):
    weight_specs = (
        P(ALL, None),
        P(None, ALL),
        P(None, ALL),
        P(ALL, None),
        P("items", "heads"),
        P("heads", "items"),
        P("items", "heads"),
        P("items", "heads"),
        P("items", "heads"),
        P("heads", "items"),
        P("items", "heads"),
        P("heads", "items"),
    )
    gain_specs = (P(ALL),) * 4
    placed = (P(ALL, None), P(None, "items"), P("items", None), P(ALL, None)) + weight_specs + gain_specs
    return jax.shard_map(
        local,
        mesh=mesh,
        in_specs=placed,
        out_specs=(P(ALL, None), P(ALL, None)) + weight_specs + gain_specs,
        check_vma=False,
    )
```

```python
import math

import jax
import jax.numpy as jnp
from jax import lax
from jax.experimental import pallas as pl
from jax.experimental.pallas import tpu as pltpu
from jax.sharding import PartitionSpec as P

HEAD = 128
NLAT = 512
PIX_MOST = 6144
LANE = 128

EPSILON = 1e-05
MASKED = -1e30
ALL = ("items", "heads")


def rounded(values):
    return values.astype(jnp.bfloat16)


def widened(values):
    return values.astype(jnp.float32)


def product(left_side, right_side):
    return jnp.dot(left_side, right_side, preferred_element_type=jnp.float32)


def product_tn(left_side, right_side):
    return lax.dot_general(
        left_side, right_side, (((0,), (0,)), ((), ())), preferred_element_type=jnp.float32
    )


def product_nt(left_side, right_side):
    return lax.dot_general(
        left_side, right_side, (((1,), (1,)), ((), ())), preferred_element_type=jnp.float32
    )


def split_parts(values):
    high = rounded(values)
    return high, rounded(values - widened(high))


def split_apply_t(values_f32, weight):
    high, low = split_parts(values_f32)
    return apply_t(high, weight) + apply_t(low, weight)


def norm_rows(values, gain_vec):
    centre = values - jnp.mean(values, axis=-1, keepdims=True)
    spread = jnp.mean(centre * centre, axis=-1, keepdims=True)
    return centre * lax.rsqrt(spread + EPSILON) * gain_vec


def norm_pixels(values):
    centre = values - jnp.mean(values, axis=0, keepdims=True)
    spread = jnp.mean(centre * centre, axis=0, keepdims=True)
    return centre * lax.rsqrt(spread + EPSILON)


def norm_backward(residual, gain_vec, grad_normed):
    unused, norm_back = jax.vjp(norm_rows, residual, gain_vec)
    return norm_back(grad_normed)


WEIGHT_KINDS = (
    "rows",
    "cols",
    "cols",
    "rows",
    "ih",
    "hi",
    "ih",
    "ih",
    "ih",
    "hi",
    "ih",
    "hi",
)

PANEL = 128
ROW_TILE = 16
ROW_GROUP = 48


def contract(left, right, left_dims, right_dims):
    return lax.dot_general(
        left, right, ((left_dims, right_dims), ((), ())), preferred_element_type=jnp.float32
    )


def lane_pad(values, width):
    panels = -(-width // PANEL)
    if panels * PANEL != width:
        pad = [(0, 0)] * (values.ndim - 1) + [(0, panels * PANEL - width)]
        values = jnp.pad(values, pad)
    return values.reshape(values.shape[:-1] + (panels, PANEL))


def lane_cut(values, width):
    values = values.reshape(values.shape[:-2] + (-1,))
    return values if values.shape[-1] == width else values[..., :width]


def local_panels(block):
    rows, width = block.shape
    parts = lane_pad(block, width).transpose(1, 0, 2)
    return parts.reshape(-1, PANEL)


def padded_rows(rows):
    return -(-rows // ROW_TILE) * ROW_TILE


def local_shape(w, kind):
    return (w.shape[1], w.shape[0]) if kind == "cols" else w.shape


def make_weight(piece, kind, shape, items, heads):
    rows, width = shape
    panels = -(-width // PANEL)
    blocks = piece[:, : panels * rows, :].reshape(items * heads, panels, rows, PANEL)
    if kind in ("ih", "hi"):
        blocks = blocks.reshape(items, heads, panels, rows, PANEL)
    return kind, blocks, width


def apply(values, weight):
    kind, blocks, width = weight
    count = values.shape[0]
    if kind in ("rows", "cols"):
        devices, panels, rows, lanes = blocks.shape
        out = contract(values.reshape(count, devices, rows), blocks, (1, 2), (0, 2))
        return lane_cut(out, width)
    items, heads, panels, rows, lanes = blocks.shape
    if kind == "ih":
        out = contract(values.reshape(count, items, rows), blocks, (1, 2), (0, 3))
    else:
        out = contract(values.reshape(count, heads, rows), blocks, (1, 2), (1, 3))
    return lane_cut(out, width).reshape(count, -1)


def apply_t(values, weight):
    kind, blocks, width = weight
    count = values.shape[0]
    if kind in ("rows", "cols"):
        devices, panels, rows, lanes = blocks.shape
        out = contract(lane_pad(values, width), blocks, (1, 2), (1, 3))
        return out.reshape(count, devices * rows)
    items, heads, panels, rows, lanes = blocks.shape
    if kind == "ih":
        spread = lane_pad(values.reshape(count, heads, width), width)
        out = contract(spread, blocks, (1, 2, 3), (1, 2, 4))
        return out.reshape(count, items * rows)
    spread = lane_pad(values.reshape(count, items, width), width)
    out = contract(spread, blocks, (1, 2, 3), (0, 2, 4))
    return out.reshape(count, heads * rows)


def grad_blocks(values, grads, weight):
    kind, blocks, width = weight
    count = values.shape[0]
    if kind in ("rows", "cols"):
        devices, panels, rows, lanes = blocks.shape
        out = contract(values.reshape(count, devices, rows), lane_pad(grads, width), (0,), (0,))
        out = out.transpose(0, 2, 1, 3)
    else:
        items, heads, panels, rows, lanes = blocks.shape
        devices = items * heads
        if kind == "ih":
            spread = lane_pad(grads.reshape(count, heads, width), width)
            out = contract(values.reshape(count, items, rows), spread, (0,), (0,))
            out = out.transpose(0, 2, 3, 1, 4)
        else:
            spread = lane_pad(grads.reshape(count, items, width), width)
            out = contract(values.reshape(count, heads, rows), spread, (0,), (0,))
            out = out.transpose(2, 0, 3, 1, 4)
    return out.reshape(devices, -1, PANEL)


def split_grad_blocks(values, grads_f32, weight):
    high, low = split_parts(grads_f32)
    return grad_blocks(values, high, weight) + grad_blocks(values, low, weight)


def pad_rows(block, rows):
    extra = rows - block.shape[-2]
    if extra == 0:
        return block
    pad = [(0, 0)] * (block.ndim - 2) + [(0, extra), (0, 0)]
    return jnp.pad(block, pad)


def gather_weights(weights, gains, items, heads):
    count = items * heads
    pieces, places, row = [], [], 0
    for w, kind in zip(weights, WEIGHT_KINDS):
        block = local_panels(rounded(w.T if kind == "cols" else w))
        rows = padded_rows(block.shape[0])
        pieces.append(pad_rows(block, rows))
        places.append((row, rows))
        row += rows
    gain_row = rounded(jnp.concatenate(gains)).reshape(1, -1)
    gain_block = local_panels(gain_row)
    total = -(-(row + gain_block.shape[0]) // ROW_GROUP) * ROW_GROUP
    pieces.append(pad_rows(gain_block, total - row))
    places.append((row, gain_block.shape[0]))
    packed = jnp.concatenate(pieces, axis=0)
    gathered = lax.all_gather(packed, ALL, axis=0, tiled=True).reshape(count, total, PANEL)
    out = []
    for w, kind, (first, rows) in zip(weights, WEIGHT_KINDS, places):
        piece = gathered[:, first : first + rows, :]
        out.append(make_weight(piece, kind, local_shape(w, kind), items, heads))
    first, rows = places[-1]
    gain_all = gathered[:, first : first + rows, :].reshape(count, -1)[:, : gain_row.shape[1]]
    gain_all = gain_all.reshape(count, len(gains), -1)
    whole_gains = [widened(gain_all[:, k, :].reshape(-1)) for k in range(len(gains))]
    return out, whole_gains


def reduce_grads(grad_parts, gain_grads, weights, items, heads):
    count = items * heads
    pieces, places, row = [], [], 0
    for part in grad_parts:
        rows = padded_rows(part.shape[1])
        pieces.append(pad_rows(rounded(part), rows))
        places.append((row, part.shape[1]))
        row += rows
    gain_stack = jnp.stack([g.reshape(count, -1) for g in gain_grads], axis=1).reshape(count, 1, -1)
    gain_block = lane_pad(gain_stack, gain_stack.shape[-1]).reshape(count, -1, PANEL)
    total = -(-(row + gain_block.shape[1]) // ROW_GROUP) * ROW_GROUP
    pieces.append(pad_rows(rounded(gain_block), total - row))
    places.append((row, gain_block.shape[1]))
    packed = jnp.concatenate(pieces, axis=1)
    mine = lax.psum_scatter(
        packed.reshape(count * total, PANEL), "items", scatter_dimension=0, tiled=True
    )
    mine = lax.psum_scatter(mine, "heads", scatter_dimension=0, tiled=True)
    out = []
    for w, kind, (first, rows) in zip(weights, WEIGHT_KINDS, places):
        r, width = local_shape(w, kind)
        panels = -(-width // PANEL)
        block = mine[first : first + rows].reshape(panels, r, PANEL).transpose(1, 0, 2)
        block = widened(lane_cut(block, width))
        out.append(block.T if kind == "cols" else block)
    first, rows = places[-1]
    gain_part = widened(mine[first : first + rows].reshape(-1)[: gain_stack.shape[-1]])
    gain_part = gain_part.reshape(len(gain_grads), -1)
    out += [gain_part[k] for k in range(len(gain_grads))]
    return out


def mlp_block(residual, gain_vec, up_w, down_w):
    normed = rounded(norm_rows(residual, gain_vec))
    before = apply(normed, up_w)
    hidden = rounded(jax.nn.gelu(before))
    return residual + apply(hidden, down_w), (normed, before, hidden)


def mlp_block_back(residual, gain_vec, up_w, down_w, saved, grad_out):
    normed, before, hidden = saved
    grad_round = rounded(grad_out)
    grad_down = grad_blocks(hidden, grad_round, down_w)
    grad_hidden = apply_t(grad_round, down_w)
    unused, gelu_back = jax.vjp(jax.nn.gelu, before)
    grad_before = rounded(gelu_back(grad_hidden)[0])
    grad_up = grad_blocks(normed, grad_before, up_w)
    grad_normed = apply_t(grad_before, up_w)
    grad_residual, grad_gain = norm_backward(residual, gain_vec, grad_normed)
    return grad_out + grad_residual, grad_up, grad_down, grad_gain


def exchange_rows(rows, split):
    if split == 1:
        return [rows]
    heads = lax.axis_size("heads")
    out = [rows]
    for shift in range(1, split):
        pairs = []
        for h in range(heads):
            base, pos = (h // split) * split, h % split
            pairs.append((h, base + (pos - shift) % split))
        out.append(lax.ppermute(rows, "heads", pairs))
    return out


def return_rows(parts, split):
    total = parts[0]
    heads = lax.axis_size("heads")
    for shift in range(1, split):
        pairs = []
        for h in range(heads):
            base, pos = (h // split) * split, h % split
            pairs.append((h, base + (pos + shift) % split))
        total = total + lax.ppermute(parts[shift], "heads", pairs)
    return total


def attention_block(residual, gain_vec, weight_set, split):
    query_w, key_w, value_w, out_w = weight_set
    rows = residual.shape[0]
    normed = rounded(norm_rows(residual, gain_vec))
    query_rows = rounded(apply(normed, query_w))
    key_rows = rounded(apply(normed, key_w))
    value_rows = rounded(apply(normed, value_w))
    heads_n = query_rows.shape[1] // HEAD
    key_all = jnp.concatenate(exchange_rows(key_rows, split), axis=0)
    value_all = jnp.concatenate(exchange_rows(value_rows, split), axis=0)
    keys = key_all.shape[0]
    q4 = query_rows.reshape(rows, heads_n, HEAD)
    k4 = key_all.reshape(keys, heads_n, HEAD)
    v4 = value_all.reshape(keys, heads_n, HEAD)
    scores = jnp.einsum("qhd,khd->hqk", q4, k4, preferred_element_type=jnp.float32) * (
        1.0 / math.sqrt(HEAD)
    )
    row_top = jnp.max(scores, axis=-1, keepdims=True)
    raw_weights = jnp.exp(scores - row_top)
    row_total = jnp.sum(raw_weights, axis=-1, keepdims=True)
    weights_low = rounded(raw_weights / row_total)
    mixed_full = jnp.einsum("hqk,khd->qhd", weights_low, v4, preferred_element_type=jnp.float32)
    mixed = rounded(mixed_full.reshape(rows, heads_n * HEAD))
    saved = (normed, q4, k4, v4, weights_low, mixed_full, mixed)
    return residual + apply(mixed, out_w), saved


def attention_block_back(residual, gain_vec, weight_set, split, saved, grad_out):
    query_w, key_w, value_w, out_w = weight_set
    normed, q4, k4, v4, weights_low, mixed_full, mixed = saved
    rows = residual.shape[0]
    keys = k4.shape[0]
    scale = 1.0 / math.sqrt(HEAD)
    grad_round = rounded(grad_out)
    grad_out_w = grad_blocks(mixed, grad_round, out_w)
    grad_mixed = rounded(apply_t(grad_round, out_w)).reshape(q4.shape)
    grad_value = jnp.einsum(
        "hqk,qhd->khd", weights_low, grad_mixed, preferred_element_type=jnp.float32
    ).reshape(keys, -1)
    row_dot = jnp.sum(widened(grad_mixed) * mixed_full, axis=-1).T[:, :, None]
    grad_weights = jnp.einsum("qhd,khd->hqk", grad_mixed, v4, preferred_element_type=jnp.float32)
    grad_scores = rounded(widened(weights_low) * (grad_weights - row_dot))
    grad_query = jnp.einsum("hqk,khd->qhd", grad_scores, k4, preferred_element_type=jnp.float32)
    grad_query = rounded((grad_query * scale).reshape(rows, -1))
    grad_key = jnp.einsum("hqk,qhd->khd", grad_scores, q4, preferred_element_type=jnp.float32)
    grad_key = (grad_key * scale).reshape(keys, -1)
    if split > 1:
        grad_key = return_rows(jnp.split(grad_key, split, axis=0), split)
        grad_value = return_rows(jnp.split(grad_value, split, axis=0), split)
    grad_key = rounded(grad_key)
    grad_value = rounded(grad_value)
    grad_query_w = grad_blocks(normed, grad_query, query_w)
    grad_key_w = grad_blocks(normed, grad_key, key_w)
    grad_value_w = grad_blocks(normed, grad_value, value_w)
    grad_normed = (
        apply_t(grad_query, query_w) + apply_t(grad_key, key_w) + apply_t(grad_value, value_w)
    )
    grad_residual, grad_gain = norm_backward(residual, gain_vec, grad_normed)
    return (grad_out + grad_residual, grad_query_w, grad_key_w, grad_value_w, grad_out_w, grad_gain)


def pixel_window(pixels, item_ids, item):
    count = pixels.shape[1]
    width = min(count, -(-PIX_MOST // LANE) * LANE + LANE)
    start = jnp.sum((item_ids < item).astype(jnp.int32))
    first = jnp.clip((start // LANE) * LANE, 0, count - width)
    window = lax.dynamic_slice_in_dim(pixels, first, width, axis=1)
    ids = lax.dynamic_slice_in_dim(item_ids, first, width, axis=0)
    return window, ids == item


SOFTMAX_ROWS = 128


def softmax_mix_kernel(keyed_ref, pixel_ref, mask_ref, weights_ref, mix_ref):
    scores = jnp.dot(keyed_ref[...], pixel_ref[...], preferred_element_type=jnp.float32)
    scores = jnp.where(mask_ref[...] > 0.0, scores, MASKED)
    row_top = jnp.max(scores, axis=-1, keepdims=True)
    raw = jnp.exp(scores - row_top)
    row_total = jnp.sum(raw, axis=-1, keepdims=True)
    weights = (raw / row_total).astype(jnp.bfloat16)
    weights_ref[...] = weights
    mix_ref[...] = lax.dot_general(
        weights, pixel_ref[...], (((1,), (1,)), ((), ())), preferred_element_type=jnp.float32
    )


def softmax_mix(keyed, pixel_pad, mask):
    rows, channels = keyed.shape
    width = pixel_pad.shape[1]
    block = min(SOFTMAX_ROWS, rows)
    cost = pl.CostEstimate(
        flops=4 * rows * channels * width,
        transcendentals=rows * width,
        bytes_accessed=2 * (rows * channels + channels * width + rows * width) + 4 * rows * channels,
    )
    return pl.pallas_call(
        softmax_mix_kernel,
        grid=(rows // block,),
        in_specs=[
            pl.BlockSpec((block, channels), lambda i: (i, 0)),
            pl.BlockSpec((channels, width), lambda i: (0, 0)),
            pl.BlockSpec((1, width), lambda i: (0, 0)),
        ],
        out_specs=[
            pl.BlockSpec((block, width), lambda i: (i, 0)),
            pl.BlockSpec((block, channels), lambda i: (i, 0)),
        ],
        out_shape=[
            jax.ShapeDtypeStruct((rows, width), jnp.bfloat16),
            jax.ShapeDtypeStruct((rows, channels), jnp.float32),
        ],
        compiler_params=pltpu.CompilerParams(vmem_limit_bytes=48 * 1024 * 1024),
        cost_estimate=cost,
    )(keyed, pixel_pad, mask)


def softmax_back_kernel(grad_ref, pixel_ref, weights_ref, dot_ref, mix_ref):
    grad_weights = jnp.dot(grad_ref[...], pixel_ref[...], preferred_element_type=jnp.float32)
    weights = weights_ref[...].astype(jnp.float32)
    grad_scores = (weights * (grad_weights - dot_ref[...])).astype(jnp.bfloat16)
    mix_ref[...] = lax.dot_general(
        grad_scores, pixel_ref[...], (((1,), (1,)), ((), ())), preferred_element_type=jnp.float32
    )


def softmax_back_mix(grad_keyed, pixel_pad, weights_low, row_dot):
    rows, channels = grad_keyed.shape
    width = pixel_pad.shape[1]
    block = min(SOFTMAX_ROWS, rows)
    cost = pl.CostEstimate(
        flops=4 * rows * channels * width,
        transcendentals=0,
        bytes_accessed=2 * (rows * channels + channels * width + rows * width) + 4 * rows * (channels + 1),
    )
    return pl.pallas_call(
        softmax_back_kernel,
        grid=(rows // block,),
        in_specs=[
            pl.BlockSpec((block, channels), lambda i: (i, 0)),
            pl.BlockSpec((channels, width), lambda i: (0, 0)),
            pl.BlockSpec((block, width), lambda i: (i, 0)),
            pl.BlockSpec((block, 1), lambda i: (i, 0)),
        ],
        out_specs=pl.BlockSpec((block, channels), lambda i: (i, 0)),
        out_shape=jax.ShapeDtypeStruct((rows, channels), jnp.float32),
        compiler_params=pltpu.CompilerParams(vmem_limit_bytes=48 * 1024 * 1024),
        cost_estimate=cost,
    )(grad_keyed, pixel_pad, weights_low, row_dot)


def cross_block(residual, gain_vec, query_w, key_w, value_w, out_w, pixel_norm, allowed):
    scale = 1.0 / math.sqrt(residual.shape[1])
    normed = rounded(norm_rows(residual, gain_vec))
    query_rows = rounded(apply(normed, query_w))
    query_keyed = rounded(apply(query_rows, key_w) * scale)
    pixel_pad, mask = allowed
    channels = pixel_norm.shape[0]
    keyed_pad = jnp.pad(query_keyed, ((0, 0), (0, pixel_pad.shape[0] - channels)))
    weights_low, pixel_mix = softmax_mix(keyed_pad, pixel_pad, mask)
    pixel_mix = pixel_mix[:, :channels]
    mixed = rounded(split_apply_t(pixel_mix, value_w))
    saved = (normed, query_rows, weights_low, pixel_mix, mixed)
    return residual + apply(mixed, out_w), saved


def cross_block_back(
    residual, gain_vec, query_w, key_w, value_w, out_w, pixel_norm, allowed, saved, grad_out
):
    normed, query_rows, weights_low, pixel_mix, mixed = saved
    scale = 1.0 / math.sqrt(residual.shape[1])
    grad_round = rounded(grad_out)
    grad_out_w = grad_blocks(mixed, grad_round, out_w)
    grad_mixed = rounded(apply_t(grad_round, out_w))
    grad_keyed = rounded(apply(grad_mixed, value_w))
    row_dot = jnp.sum(widened(grad_keyed) * pixel_mix, axis=-1, keepdims=True)
    pixel_pad = allowed[0]
    channels = pixel_norm.shape[0]
    grad_pad = jnp.pad(grad_keyed, ((0, 0), (0, pixel_pad.shape[0] - channels)))
    score_mix = softmax_back_mix(grad_pad, pixel_pad, weights_low, row_dot)[:, :channels]
    grad_query = rounded(split_apply_t(score_mix, key_w) * scale)
    grad_query_w = grad_blocks(normed, grad_query, query_w)
    grad_key_w = split_grad_blocks(query_rows, score_mix, key_w) * scale
    grad_value_w = split_grad_blocks(grad_mixed, pixel_mix, value_w)
    grad_normed = apply_t(grad_query, query_w)
    grad_residual, grad_gain = norm_backward(residual, gain_vec, grad_normed)
    return (grad_out + grad_residual, grad_query_w, grad_key_w, grad_value_w, grad_out_w, grad_gain)


def local(latents, pixels, pixel_item, cotangent, *params):
    weights, gains = params[:12], params[12:]
    items = lax.axis_size("items")
    heads = lax.axis_size("heads")
    rows = latents.shape[0]
    split = max(1, NLAT // rows)
    (
        query_cross,
        key_cross,
        value_cross,
        out_cross,
        up_cross,
        down_cross,
        query_self,
        key_self,
        value_self,
        out_self,
        up_self,
        down_self,
    ), gain_list = gather_weights(weights, gains, items, heads)
    attention_set = (query_self, key_self, value_self, out_self)

    item = (lax.axis_index("heads") * rows) // NLAT
    window, allowed = pixel_window(pixels, pixel_item[0], item)
    pixel_norm = rounded(norm_pixels(widened(window)))
    channels = pixel_norm.shape[0]
    pixel_pad = jnp.pad(pixel_norm, ((0, -channels % LANE), (0, 0)))
    mask = allowed.astype(jnp.float32)[None, :]
    pixel_norm, pixel_pad, mask = lax.optimization_barrier((pixel_norm, pixel_pad, mask))
    allowed = (pixel_pad, mask)

    start_rows = widened(latents)
    after_cross, saved_cross = cross_block(
        start_rows, gain_list[0], query_cross, key_cross, value_cross, out_cross, pixel_norm, allowed
    )
    after_mlp_one, saved_mlp_one = mlp_block(after_cross, gain_list[1], up_cross, down_cross)
    after_self, saved_self = attention_block(after_mlp_one, gain_list[2], attention_set, split)
    final_rows, saved_mlp_two = mlp_block(after_self, gain_list[3], up_self, down_self)

    grad_final = widened(cotangent)
    grad_after_self, grad_self_up, grad_self_down, grad_gain_four = mlp_block_back(
        after_self, gain_list[3], up_self, down_self, saved_mlp_two, grad_final
    )
    (
        grad_after_mlp,
        grad_self_query,
        grad_self_key,
        grad_self_value,
        grad_self_out,
        grad_gain_three,
    ) = attention_block_back(
        after_mlp_one, gain_list[2], attention_set, split, saved_self, grad_after_self
    )
    grad_after_cross, grad_cross_up, grad_cross_down, grad_gain_two = mlp_block_back(
        after_cross, gain_list[1], up_cross, down_cross, saved_mlp_one, grad_after_mlp
    )
    (
        latents_grad,
        grad_cross_query,
        grad_cross_key,
        grad_cross_value,
        grad_cross_out,
        grad_gain_one,
    ) = cross_block_back(
        start_rows,
        gain_list[0],
        query_cross,
        key_cross,
        value_cross,
        out_cross,
        pixel_norm,
        allowed,
        saved_cross,
        grad_after_cross,
    )
    weight_grads = (
        grad_cross_query,
        grad_cross_key,
        grad_cross_value,
        grad_cross_out,
        grad_cross_up,
        grad_cross_down,
        grad_self_query,
        grad_self_key,
        grad_self_value,
        grad_self_out,
        grad_self_up,
        grad_self_down,
    )
    gain_grads = (grad_gain_one, grad_gain_two, grad_gain_three, grad_gain_four)
    reduced = reduce_grads(weight_grads, gain_grads, weights, items, heads)
    shaped = [r.reshape(w.shape) for r, w in zip(reduced[:12], weights)]
    shaped += [r.reshape(g.shape) for r, g in zip(reduced[12:], gains)]
    return (rounded(final_rows), latents_grad, *shaped)


def solution(mesh):
    weight_specs = (
        P(ALL, None),
        P(None, ALL),
        P(None, ALL),
        P(ALL, None),
        P("items", "heads"),
        P("heads", "items"),
        P("items", "heads"),
        P("items", "heads"),
        P("items", "heads"),
        P("heads", "items"),
        P("items", "heads"),
        P("heads", "items"),
    )
    gain_specs = (P(ALL),) * 4
    placed = (P(ALL, None), P(None, "items"), P("items", None), P(ALL, None)) + weight_specs + gain_specs
    return jax.shard_map(
        local,
        mesh=mesh,
        in_specs=placed,
        out_specs=(P(ALL, None), P(ALL, None)) + weight_specs + gain_specs,
        check_vma=False,
    )
```

```python
import math

import jax
import jax.numpy as jnp
from jax import lax
from jax.experimental import pallas as pl
from jax.experimental.pallas import tpu as pltpu
from jax.sharding import PartitionSpec as P

HEAD = 128
NLAT = 512
PIX_MOST = 6144
LANE = 128

EPSILON = 1e-05
MASKED = -1e30
ALL = ("items", "heads")


def rounded(values):
    return values.astype(jnp.bfloat16)


def widened(values):
    return values.astype(jnp.float32)


def product(left_side, right_side):
    return jnp.dot(left_side, right_side, preferred_element_type=jnp.float32)


def product_tn(left_side, right_side):
    return lax.dot_general(
        left_side, right_side, (((0,), (0,)), ((), ())), preferred_element_type=jnp.float32
    )


def product_nt(left_side, right_side):
    return lax.dot_general(
        left_side, right_side, (((1,), (1,)), ((), ())), preferred_element_type=jnp.float32
    )


def split_parts(values):
    high = rounded(values)
    return high, rounded(values - widened(high))


def split_apply_t(values_f32, weight):
    high, low = split_parts(values_f32)
    return apply_t(high, weight) + apply_t(low, weight)


def norm_rows(values, gain_vec):
    centre = values - jnp.mean(values, axis=-1, keepdims=True)
    spread = jnp.mean(centre * centre, axis=-1, keepdims=True)
    return centre * lax.rsqrt(spread + EPSILON) * gain_vec


def norm_pixels(values):
    centre = values - jnp.mean(values, axis=0, keepdims=True)
    spread = jnp.mean(centre * centre, axis=0, keepdims=True)
    return centre * lax.rsqrt(spread + EPSILON)


def norm_backward(residual, gain_vec, grad_normed):
    unused, norm_back = jax.vjp(norm_rows, residual, gain_vec)
    return norm_back(grad_normed)


WEIGHT_KINDS = (
    "rows",
    "cols",
    "cols",
    "rows",
    "ih",
    "hi",
    "ih",
    "ih",
    "ih",
    "hi",
    "ih",
    "hi",
)

PANEL = 128
ROW_TILE = 16
ROW_GROUP = 48


def contract(left, right, left_dims, right_dims):
    return lax.dot_general(
        left, right, ((left_dims, right_dims), ((), ())), preferred_element_type=jnp.float32
    )


def lane_pad(values, width):
    panels = -(-width // PANEL)
    if panels * PANEL != width:
        pad = [(0, 0)] * (values.ndim - 1) + [(0, panels * PANEL - width)]
        values = jnp.pad(values, pad)
    return values.reshape(values.shape[:-1] + (panels, PANEL))


def lane_cut(values, width):
    values = values.reshape(values.shape[:-2] + (-1,))
    return values if values.shape[-1] == width else values[..., :width]


def local_panels(block):
    rows, width = block.shape
    parts = lane_pad(block, width).transpose(1, 0, 2)
    return parts.reshape(-1, PANEL)


def padded_rows(rows):
    return -(-rows // ROW_TILE) * ROW_TILE


def local_shape(w, kind):
    return (w.shape[1], w.shape[0]) if kind == "cols" else w.shape


def make_weight(piece, kind, shape, items, heads):
    rows, width = shape
    panels = -(-width // PANEL)
    blocks = piece[:, : panels * rows, :].reshape(items * heads, panels, rows, PANEL)
    if kind in ("ih", "hi"):
        blocks = blocks.reshape(items, heads, panels, rows, PANEL)
    return kind, blocks, width


def apply(values, weight):
    kind, blocks, width = weight
    count = values.shape[0]
    if kind in ("rows", "cols"):
        devices, panels, rows, lanes = blocks.shape
        out = contract(values.reshape(count, devices, rows), blocks, (1, 2), (0, 2))
        return lane_cut(out, width)
    items, heads, panels, rows, lanes = blocks.shape
    if kind == "ih":
        out = contract(values.reshape(count, items, rows), blocks, (1, 2), (0, 3))
    else:
        out = contract(values.reshape(count, heads, rows), blocks, (1, 2), (1, 3))
    return lane_cut(out, width).reshape(count, -1)


def apply_t(values, weight):
    kind, blocks, width = weight
    count = values.shape[0]
    if kind in ("rows", "cols"):
        devices, panels, rows, lanes = blocks.shape
        out = contract(lane_pad(values, width), blocks, (1, 2), (1, 3))
        return out.reshape(count, devices * rows)
    items, heads, panels, rows, lanes = blocks.shape
    if kind == "ih":
        spread = lane_pad(values.reshape(count, heads, width), width)
        out = contract(spread, blocks, (1, 2, 3), (1, 2, 4))
        return out.reshape(count, items * rows)
    spread = lane_pad(values.reshape(count, items, width), width)
    out = contract(spread, blocks, (1, 2, 3), (0, 2, 4))
    return out.reshape(count, heads * rows)


def grad_blocks(values, grads, weight):
    kind, blocks, width = weight
    count = values.shape[0]
    if kind in ("rows", "cols"):
        devices, panels, rows, lanes = blocks.shape
        out = contract(values.reshape(count, devices, rows), lane_pad(grads, width), (0,), (0,))
        out = out.transpose(0, 2, 1, 3)
    else:
        items, heads, panels, rows, lanes = blocks.shape
        devices = items * heads
        if kind == "ih":
            spread = lane_pad(grads.reshape(count, heads, width), width)
            out = contract(values.reshape(count, items, rows), spread, (0,), (0,))
            out = out.transpose(0, 2, 3, 1, 4)
        else:
            spread = lane_pad(grads.reshape(count, items, width), width)
            out = contract(values.reshape(count, heads, rows), spread, (0,), (0,))
            out = out.transpose(2, 0, 3, 1, 4)
    return out.reshape(devices, -1, PANEL)


def split_grad_blocks(values, grads_f32, weight):
    high, low = split_parts(grads_f32)
    return grad_blocks(values, high, weight) + grad_blocks(values, low, weight)


def pad_rows(block, rows):
    extra = rows - block.shape[-2]
    if extra == 0:
        return block
    pad = [(0, 0)] * (block.ndim - 2) + [(0, extra), (0, 0)]
    return jnp.pad(block, pad)


def gather_weights(weights, gains, items, heads):
    count = items * heads
    pieces, places, row = [], [], 0
    for w, kind in zip(weights, WEIGHT_KINDS):
        block = local_panels(rounded(w.T if kind == "cols" else w))
        rows = padded_rows(block.shape[0])
        pieces.append(pad_rows(block, rows))
        places.append((row, rows))
        row += rows
    gain_row = rounded(jnp.concatenate(gains)).reshape(1, -1)
    gain_block = local_panels(gain_row)
    total = -(-(row + gain_block.shape[0]) // ROW_GROUP) * ROW_GROUP
    pieces.append(pad_rows(gain_block, total - row))
    places.append((row, gain_block.shape[0]))
    packed = jnp.concatenate(pieces, axis=0)
    gathered = lax.all_gather(packed, ALL, axis=0, tiled=True).reshape(count, total, PANEL)
    out = []
    for w, kind, (first, rows) in zip(weights, WEIGHT_KINDS, places):
        piece = gathered[:, first : first + rows, :]
        out.append(make_weight(piece, kind, local_shape(w, kind), items, heads))
    first, rows = places[-1]
    gain_all = gathered[:, first : first + rows, :].reshape(count, -1)[:, : gain_row.shape[1]]
    gain_all = gain_all.reshape(count, len(gains), -1)
    whole_gains = [widened(gain_all[:, k, :].reshape(-1)) for k in range(len(gains))]
    return out, whole_gains


def reduce_grads(grad_parts, gain_grads, weights, items, heads):
    count = items * heads
    pieces, places, row = [], [], 0
    for part in grad_parts:
        rows = padded_rows(part.shape[1])
        pieces.append(pad_rows(rounded(part), rows))
        places.append((row, part.shape[1]))
        row += rows
    gain_stack = jnp.stack([g.reshape(count, -1) for g in gain_grads], axis=1).reshape(count, 1, -1)
    gain_block = lane_pad(gain_stack, gain_stack.shape[-1]).reshape(count, -1, PANEL)
    total = -(-(row + gain_block.shape[1]) // ROW_GROUP) * ROW_GROUP
    pieces.append(pad_rows(rounded(gain_block), total - row))
    places.append((row, gain_block.shape[1]))
    packed = jnp.concatenate(pieces, axis=1)
    mine = lax.psum_scatter(
        packed.reshape(count * total, PANEL), "items", scatter_dimension=0, tiled=True
    )
    mine = lax.psum_scatter(mine, "heads", scatter_dimension=0, tiled=True)
    out = []
    for w, kind, (first, rows) in zip(weights, WEIGHT_KINDS, places):
        r, width = local_shape(w, kind)
        panels = -(-width // PANEL)
        block = mine[first : first + rows].reshape(panels, r, PANEL).transpose(1, 0, 2)
        block = widened(lane_cut(block, width))
        out.append(block.T if kind == "cols" else block)
    first, rows = places[-1]
    gain_part = widened(mine[first : first + rows].reshape(-1)[: gain_stack.shape[-1]])
    gain_part = gain_part.reshape(len(gain_grads), -1)
    out += [gain_part[k] for k in range(len(gain_grads))]
    return out


def mlp_block(residual, gain_vec, up_w, down_w):
    normed = rounded(norm_rows(residual, gain_vec))
    before = apply(normed, up_w)
    hidden = rounded(jax.nn.gelu(before))
    return residual + apply(hidden, down_w), (normed, before, hidden)


def mlp_block_back(residual, gain_vec, up_w, down_w, saved, grad_out):
    normed, before, hidden = saved
    grad_round = rounded(grad_out)
    grad_down = grad_blocks(hidden, grad_round, down_w)
    grad_hidden = apply_t(grad_round, down_w)
    unused, gelu_back = jax.vjp(jax.nn.gelu, before)
    grad_before = rounded(gelu_back(grad_hidden)[0])
    grad_up = grad_blocks(normed, grad_before, up_w)
    grad_normed = apply_t(grad_before, up_w)
    grad_residual, grad_gain = norm_backward(residual, gain_vec, grad_normed)
    return grad_out + grad_residual, grad_up, grad_down, grad_gain


def exchange_rows(rows, split):
    if split == 1:
        return [rows]
    heads = lax.axis_size("heads")
    out = [rows]
    for shift in range(1, split):
        pairs = []
        for h in range(heads):
            base, pos = (h // split) * split, h % split
            pairs.append((h, base + (pos - shift) % split))
        out.append(lax.ppermute(rows, "heads", pairs))
    return out


def return_rows(parts, split):
    total = parts[0]
    heads = lax.axis_size("heads")
    for shift in range(1, split):
        pairs = []
        for h in range(heads):
            base, pos = (h // split) * split, h % split
            pairs.append((h, base + (pos + shift) % split))
        total = total + lax.ppermute(parts[shift], "heads", pairs)
    return total


def attention_block(residual, gain_vec, weight_set, split):
    query_w, key_w, value_w, out_w = weight_set
    rows = residual.shape[0]
    normed = rounded(norm_rows(residual, gain_vec))
    query_rows = rounded(apply(normed, query_w))
    key_rows = rounded(apply(normed, key_w))
    value_rows = rounded(apply(normed, value_w))
    heads_n = query_rows.shape[1] // HEAD
    key_all = jnp.concatenate(exchange_rows(key_rows, split), axis=0)
    value_all = jnp.concatenate(exchange_rows(value_rows, split), axis=0)
    keys = key_all.shape[0]
    q4 = query_rows.reshape(rows, heads_n, HEAD)
    k4 = key_all.reshape(keys, heads_n, HEAD)
    v4 = value_all.reshape(keys, heads_n, HEAD)
    scores = jnp.einsum("qhd,khd->hqk", q4, k4, preferred_element_type=jnp.float32) * (
        1.0 / math.sqrt(HEAD)
    )
    row_top = jnp.max(scores, axis=-1, keepdims=True)
    raw_weights = jnp.exp(scores - row_top)
    row_total = jnp.sum(raw_weights, axis=-1, keepdims=True)
    weights_low = rounded(raw_weights / row_total)
    mixed_full = jnp.einsum("hqk,khd->qhd", weights_low, v4, preferred_element_type=jnp.float32)
    mixed = rounded(mixed_full.reshape(rows, heads_n * HEAD))
    saved = (normed, q4, k4, v4, weights_low, mixed_full, mixed)
    return residual + apply(mixed, out_w), saved


def attention_block_back(residual, gain_vec, weight_set, split, saved, grad_out):
    query_w, key_w, value_w, out_w = weight_set
    normed, q4, k4, v4, weights_low, mixed_full, mixed = saved
    rows = residual.shape[0]
    keys = k4.shape[0]
    scale = 1.0 / math.sqrt(HEAD)
    grad_round = rounded(grad_out)
    grad_out_w = grad_blocks(mixed, grad_round, out_w)
    grad_mixed = rounded(apply_t(grad_round, out_w)).reshape(q4.shape)
    grad_value = jnp.einsum(
        "hqk,qhd->khd", weights_low, grad_mixed, preferred_element_type=jnp.float32
    ).reshape(keys, -1)
    row_dot = jnp.sum(widened(grad_mixed) * mixed_full, axis=-1).T[:, :, None]
    grad_weights = jnp.einsum("qhd,khd->hqk", grad_mixed, v4, preferred_element_type=jnp.float32)
    grad_scores = rounded(widened(weights_low) * (grad_weights - row_dot))
    grad_query = jnp.einsum("hqk,khd->qhd", grad_scores, k4, preferred_element_type=jnp.float32)
    grad_query = rounded((grad_query * scale).reshape(rows, -1))
    grad_key = jnp.einsum("hqk,qhd->khd", grad_scores, q4, preferred_element_type=jnp.float32)
    grad_key = (grad_key * scale).reshape(keys, -1)
    if split > 1:
        grad_key = return_rows(jnp.split(grad_key, split, axis=0), split)
        grad_value = return_rows(jnp.split(grad_value, split, axis=0), split)
    grad_key = rounded(grad_key)
    grad_value = rounded(grad_value)
    grad_query_w = grad_blocks(normed, grad_query, query_w)
    grad_key_w = grad_blocks(normed, grad_key, key_w)
    grad_value_w = grad_blocks(normed, grad_value, value_w)
    grad_normed = (
        apply_t(grad_query, query_w) + apply_t(grad_key, key_w) + apply_t(grad_value, value_w)
    )
    grad_residual, grad_gain = norm_backward(residual, gain_vec, grad_normed)
    return (grad_out + grad_residual, grad_query_w, grad_key_w, grad_value_w, grad_out_w, grad_gain)


def pixel_window(pixels, item_ids, item):
    count = pixels.shape[1]
    width = min(count, -(-PIX_MOST // LANE) * LANE + LANE)
    start = jnp.sum((item_ids < item).astype(jnp.int32))
    first = jnp.clip((start // LANE) * LANE, 0, count - width)
    window = lax.dynamic_slice_in_dim(pixels, first, width, axis=1)
    ids = lax.dynamic_slice_in_dim(item_ids, first, width, axis=0)
    return window, ids == item


SOFTMAX_ROWS = 256


def softmax_mix_kernel(keyed_ref, pixel_ref, mask_ref, weights_ref, mix_ref):
    scores = jnp.dot(keyed_ref[...], pixel_ref[...], preferred_element_type=jnp.float32)
    scores = jnp.where(mask_ref[...] > 0.0, scores, MASKED)
    row_top = jnp.max(scores, axis=-1, keepdims=True)
    raw = jnp.exp(scores - row_top)
    row_total = jnp.sum(raw, axis=-1, keepdims=True)
    weights = (raw / row_total).astype(jnp.bfloat16)
    weights_ref[...] = weights
    mix_ref[...] = lax.dot_general(
        weights, pixel_ref[...], (((1,), (1,)), ((), ())), preferred_element_type=jnp.float32
    )


def softmax_mix(keyed, pixel_pad, mask):
    rows, channels = keyed.shape
    width = pixel_pad.shape[1]
    block = min(SOFTMAX_ROWS, rows)
    cost = pl.CostEstimate(
        flops=4 * rows * channels * width,
        transcendentals=rows * width,
        bytes_accessed=2 * (rows * channels + channels * width + rows * width) + 4 * rows * channels,
    )
    return pl.pallas_call(
        softmax_mix_kernel,
        grid=(rows // block,),
        in_specs=[
            pl.BlockSpec((block, channels), lambda i: (i, 0)),
            pl.BlockSpec((channels, width), lambda i: (0, 0)),
            pl.BlockSpec((1, width), lambda i: (0, 0)),
        ],
        out_specs=[
            pl.BlockSpec((block, width), lambda i: (i, 0)),
            pl.BlockSpec((block, channels), lambda i: (i, 0)),
        ],
        out_shape=[
            jax.ShapeDtypeStruct((rows, width), jnp.bfloat16),
            jax.ShapeDtypeStruct((rows, channels), jnp.float32),
        ],
        compiler_params=pltpu.CompilerParams(vmem_limit_bytes=48 * 1024 * 1024),
        cost_estimate=cost,
    )(keyed, pixel_pad, mask)


def softmax_back_kernel(grad_ref, pixel_ref, weights_ref, dot_ref, mix_ref):
    grad_weights = jnp.dot(grad_ref[...], pixel_ref[...], preferred_element_type=jnp.float32)
    weights = weights_ref[...].astype(jnp.float32)
    grad_scores = (weights * (grad_weights - dot_ref[...])).astype(jnp.bfloat16)
    mix_ref[...] = lax.dot_general(
        grad_scores, pixel_ref[...], (((1,), (1,)), ((), ())), preferred_element_type=jnp.float32
    )


def softmax_back_mix(grad_keyed, pixel_pad, weights_low, row_dot):
    rows, channels = grad_keyed.shape
    width = pixel_pad.shape[1]
    block = min(SOFTMAX_ROWS, rows)
    cost = pl.CostEstimate(
        flops=4 * rows * channels * width,
        transcendentals=0,
        bytes_accessed=2 * (rows * channels + channels * width + rows * width) + 4 * rows * (channels + 1),
    )
    return pl.pallas_call(
        softmax_back_kernel,
        grid=(rows // block,),
        in_specs=[
            pl.BlockSpec((block, channels), lambda i: (i, 0)),
            pl.BlockSpec((channels, width), lambda i: (0, 0)),
            pl.BlockSpec((block, width), lambda i: (i, 0)),
            pl.BlockSpec((block, 1), lambda i: (i, 0)),
        ],
        out_specs=pl.BlockSpec((block, channels), lambda i: (i, 0)),
        out_shape=jax.ShapeDtypeStruct((rows, channels), jnp.float32),
        compiler_params=pltpu.CompilerParams(vmem_limit_bytes=48 * 1024 * 1024),
        cost_estimate=cost,
    )(grad_keyed, pixel_pad, weights_low, row_dot)


def cross_block(residual, gain_vec, query_w, key_w, value_w, out_w, pixel_norm, allowed):
    scale = 1.0 / math.sqrt(residual.shape[1])
    normed = rounded(norm_rows(residual, gain_vec))
    query_rows = rounded(apply(normed, query_w))
    query_keyed = rounded(apply(query_rows, key_w) * scale)
    pixel_pad, mask = allowed
    channels = pixel_norm.shape[0]
    keyed_pad = jnp.pad(query_keyed, ((0, 0), (0, pixel_pad.shape[0] - channels)))
    weights_low, pixel_mix = softmax_mix(keyed_pad, pixel_pad, mask)
    pixel_mix = pixel_mix[:, :channels]
    mixed = rounded(split_apply_t(pixel_mix, value_w))
    saved = (normed, query_rows, weights_low, pixel_mix, mixed)
    return residual + apply(mixed, out_w), saved


def cross_block_back(
    residual, gain_vec, query_w, key_w, value_w, out_w, pixel_norm, allowed, saved, grad_out
):
    normed, query_rows, weights_low, pixel_mix, mixed = saved
    scale = 1.0 / math.sqrt(residual.shape[1])
    grad_round = rounded(grad_out)
    grad_out_w = grad_blocks(mixed, grad_round, out_w)
    grad_mixed = rounded(apply_t(grad_round, out_w))
    grad_keyed = rounded(apply(grad_mixed, value_w))
    row_dot = jnp.sum(widened(grad_keyed) * pixel_mix, axis=-1, keepdims=True)
    pixel_pad = allowed[0]
    channels = pixel_norm.shape[0]
    grad_pad = jnp.pad(grad_keyed, ((0, 0), (0, pixel_pad.shape[0] - channels)))
    score_mix = softmax_back_mix(grad_pad, pixel_pad, weights_low, row_dot)[:, :channels]
    grad_query = rounded(split_apply_t(score_mix, key_w) * scale)
    grad_query_w = grad_blocks(normed, grad_query, query_w)
    grad_key_w = split_grad_blocks(query_rows, score_mix, key_w) * scale
    grad_value_w = split_grad_blocks(grad_mixed, pixel_mix, value_w)
    grad_normed = apply_t(grad_query, query_w)
    grad_residual, grad_gain = norm_backward(residual, gain_vec, grad_normed)
    return (grad_out + grad_residual, grad_query_w, grad_key_w, grad_value_w, grad_out_w, grad_gain)


def local(latents, pixels, pixel_item, cotangent, *params):
    weights, gains = params[:12], params[12:]
    items = lax.axis_size("items")
    heads = lax.axis_size("heads")
    rows = latents.shape[0]
    split = max(1, NLAT // rows)
    (
        query_cross,
        key_cross,
        value_cross,
        out_cross,
        up_cross,
        down_cross,
        query_self,
        key_self,
        value_self,
        out_self,
        up_self,
        down_self,
    ), gain_list = gather_weights(weights, gains, items, heads)
    attention_set = (query_self, key_self, value_self, out_self)

    item = (lax.axis_index("heads") * rows) // NLAT
    window, allowed = pixel_window(pixels, pixel_item[0], item)
    pixel_norm = rounded(norm_pixels(widened(window)))
    channels = pixel_norm.shape[0]
    pixel_pad = jnp.pad(pixel_norm, ((0, -channels % LANE), (0, 0)))
    mask = allowed.astype(jnp.float32)[None, :]
    pixel_norm, pixel_pad, mask = lax.optimization_barrier((pixel_norm, pixel_pad, mask))
    allowed = (pixel_pad, mask)

    start_rows = widened(latents)
    after_cross, saved_cross = cross_block(
        start_rows, gain_list[0], query_cross, key_cross, value_cross, out_cross, pixel_norm, allowed
    )
    after_mlp_one, saved_mlp_one = mlp_block(after_cross, gain_list[1], up_cross, down_cross)
    after_self, saved_self = attention_block(after_mlp_one, gain_list[2], attention_set, split)
    final_rows, saved_mlp_two = mlp_block(after_self, gain_list[3], up_self, down_self)

    grad_final = widened(cotangent)
    grad_after_self, grad_self_up, grad_self_down, grad_gain_four = mlp_block_back(
        after_self, gain_list[3], up_self, down_self, saved_mlp_two, grad_final
    )
    (
        grad_after_mlp,
        grad_self_query,
        grad_self_key,
        grad_self_value,
        grad_self_out,
        grad_gain_three,
    ) = attention_block_back(
        after_mlp_one, gain_list[2], attention_set, split, saved_self, grad_after_self
    )
    grad_after_cross, grad_cross_up, grad_cross_down, grad_gain_two = mlp_block_back(
        after_cross, gain_list[1], up_cross, down_cross, saved_mlp_one, grad_after_mlp
    )
    (
        latents_grad,
        grad_cross_query,
        grad_cross_key,
        grad_cross_value,
        grad_cross_out,
        grad_gain_one,
    ) = cross_block_back(
        start_rows,
        gain_list[0],
        query_cross,
        key_cross,
        value_cross,
        out_cross,
        pixel_norm,
        allowed,
        saved_cross,
        grad_after_cross,
    )
    weight_grads = (
        grad_cross_query,
        grad_cross_key,
        grad_cross_value,
        grad_cross_out,
        grad_cross_up,
        grad_cross_down,
        grad_self_query,
        grad_self_key,
        grad_self_value,
        grad_self_out,
        grad_self_up,
        grad_self_down,
    )
    gain_grads = (grad_gain_one, grad_gain_two, grad_gain_three, grad_gain_four)
    reduced = reduce_grads(weight_grads, gain_grads, weights, items, heads)
    shaped = [r.reshape(w.shape) for r, w in zip(reduced[:12], weights)]
    shaped += [r.reshape(g.shape) for r, g in zip(reduced[12:], gains)]
    return (rounded(final_rows), latents_grad, *shaped)


def solution(mesh):
    weight_specs = (
        P(ALL, None),
        P(None, ALL),
        P(None, ALL),
        P(ALL, None),
        P("items", "heads"),
        P("heads", "items"),
        P("items", "heads"),
        P("items", "heads"),
        P("items", "heads"),
        P("heads", "items"),
        P("items", "heads"),
        P("heads", "items"),
    )
    gain_specs = (P(ALL),) * 4
    placed = (P(ALL, None), P(None, "items"), P("items", None), P(ALL, None)) + weight_specs + gain_specs
    return jax.shard_map(
        local,
        mesh=mesh,
        in_specs=placed,
        out_specs=(P(ALL, None), P(ALL, None)) + weight_specs + gain_specs,
        check_vma=False,
    )
```

```python
import math

import jax
import jax.numpy as jnp
from jax import lax
from jax.experimental import pallas as pl
from jax.experimental.pallas import tpu as pltpu
from jax.sharding import PartitionSpec as P

HEAD = 128
NLAT = 512
PIX_MOST = 6144
LANE = 128

EPSILON = 1e-05
MASKED = -1e30
ALL = ("items", "heads")


def rounded(values):
    return values.astype(jnp.bfloat16)


def widened(values):
    return values.astype(jnp.float32)


def product(left_side, right_side):
    return jnp.dot(left_side, right_side, preferred_element_type=jnp.float32)


def product_tn(left_side, right_side):
    return lax.dot_general(
        left_side, right_side, (((0,), (0,)), ((), ())), preferred_element_type=jnp.float32
    )


def product_nt(left_side, right_side):
    return lax.dot_general(
        left_side, right_side, (((1,), (1,)), ((), ())), preferred_element_type=jnp.float32
    )


def split_parts(values):
    high = rounded(values)
    return high, rounded(values - widened(high))


def split_apply_t(values_f32, weight):
    high, low = split_parts(values_f32)
    return apply_t(high, weight) + apply_t(low, weight)


def norm_rows(values, gain_vec):
    centre = values - jnp.mean(values, axis=-1, keepdims=True)
    spread = jnp.mean(centre * centre, axis=-1, keepdims=True)
    return centre * lax.rsqrt(spread + EPSILON) * gain_vec


def norm_pixels(values):
    centre = values - jnp.mean(values, axis=0, keepdims=True)
    spread = jnp.mean(centre * centre, axis=0, keepdims=True)
    return centre * lax.rsqrt(spread + EPSILON)


def norm_backward(residual, gain_vec, grad_normed):
    unused, norm_back = jax.vjp(norm_rows, residual, gain_vec)
    return norm_back(grad_normed)


WEIGHT_KINDS = (
    "rows",
    "cols",
    "cols",
    "rows",
    "ih",
    "hi",
    "ih",
    "ih",
    "ih",
    "hi",
    "ih",
    "hi",
)

PANEL = 128
ROW_TILE = 16
ROW_GROUP = 48


def contract(left, right, left_dims, right_dims):
    return lax.dot_general(
        left, right, ((left_dims, right_dims), ((), ())), preferred_element_type=jnp.float32
    )


def lane_pad(values, width):
    panels = -(-width // PANEL)
    if panels * PANEL != width:
        pad = [(0, 0)] * (values.ndim - 1) + [(0, panels * PANEL - width)]
        values = jnp.pad(values, pad)
    return values.reshape(values.shape[:-1] + (panels, PANEL))


def lane_cut(values, width):
    values = values.reshape(values.shape[:-2] + (-1,))
    return values if values.shape[-1] == width else values[..., :width]


def local_panels(block):
    rows, width = block.shape
    parts = lane_pad(block, width).transpose(1, 0, 2)
    return parts.reshape(-1, PANEL)


def padded_rows(rows):
    return -(-rows // ROW_TILE) * ROW_TILE


def local_shape(w, kind):
    return (w.shape[1], w.shape[0]) if kind == "cols" else w.shape


def make_weight(piece, kind, shape, items, heads):
    rows, width = shape
    panels = -(-width // PANEL)
    blocks = piece[:, : panels * rows, :].reshape(items * heads, panels, rows, PANEL)
    if kind in ("ih", "hi"):
        blocks = blocks.reshape(items, heads, panels, rows, PANEL)
    return kind, blocks, width


def apply(values, weight):
    kind, blocks, width = weight
    count = values.shape[0]
    if kind in ("rows", "cols"):
        devices, panels, rows, lanes = blocks.shape
        out = contract(values.reshape(count, devices, rows), blocks, (1, 2), (0, 2))
        return lane_cut(out, width)
    items, heads, panels, rows, lanes = blocks.shape
    if kind == "ih":
        out = contract(values.reshape(count, items, rows), blocks, (1, 2), (0, 3))
    else:
        out = contract(values.reshape(count, heads, rows), blocks, (1, 2), (1, 3))
    return lane_cut(out, width).reshape(count, -1)


def apply_t(values, weight):
    kind, blocks, width = weight
    count = values.shape[0]
    if kind in ("rows", "cols"):
        devices, panels, rows, lanes = blocks.shape
        out = contract(lane_pad(values, width), blocks, (1, 2), (1, 3))
        return out.reshape(count, devices * rows)
    items, heads, panels, rows, lanes = blocks.shape
    if kind == "ih":
        spread = lane_pad(values.reshape(count, heads, width), width)
        out = contract(spread, blocks, (1, 2, 3), (1, 2, 4))
        return out.reshape(count, items * rows)
    spread = lane_pad(values.reshape(count, items, width), width)
    out = contract(spread, blocks, (1, 2, 3), (0, 2, 4))
    return out.reshape(count, heads * rows)


def grad_blocks(values, grads, weight):
    kind, blocks, width = weight
    count = values.shape[0]
    if kind in ("rows", "cols"):
        devices, panels, rows, lanes = blocks.shape
        out = contract(values.reshape(count, devices, rows), lane_pad(grads, width), (0,), (0,))
        out = out.transpose(0, 2, 1, 3)
    else:
        items, heads, panels, rows, lanes = blocks.shape
        devices = items * heads
        if kind == "ih":
            spread = lane_pad(grads.reshape(count, heads, width), width)
            out = contract(values.reshape(count, items, rows), spread, (0,), (0,))
            out = out.transpose(0, 2, 3, 1, 4)
        else:
            spread = lane_pad(grads.reshape(count, items, width), width)
            out = contract(values.reshape(count, heads, rows), spread, (0,), (0,))
            out = out.transpose(2, 0, 3, 1, 4)
    return out.reshape(devices, -1, PANEL)


def split_grad_blocks(values, grads_f32, weight):
    high, low = split_parts(grads_f32)
    return grad_blocks(values, high, weight) + grad_blocks(values, low, weight)


def pad_rows(block, rows):
    extra = rows - block.shape[-2]
    if extra == 0:
        return block
    pad = [(0, 0)] * (block.ndim - 2) + [(0, extra), (0, 0)]
    return jnp.pad(block, pad)


def gather_weights(weights, gains, items, heads):
    count = items * heads
    pieces, places, row = [], [], 0
    for w, kind in zip(weights, WEIGHT_KINDS):
        block = local_panels(rounded(w.T if kind == "cols" else w))
        rows = padded_rows(block.shape[0])
        pieces.append(pad_rows(block, rows))
        places.append((row, rows))
        row += rows
    gain_row = rounded(jnp.concatenate(gains)).reshape(1, -1)
    gain_block = local_panels(gain_row)
    total = -(-(row + gain_block.shape[0]) // ROW_GROUP) * ROW_GROUP
    pieces.append(pad_rows(gain_block, total - row))
    places.append((row, gain_block.shape[0]))
    packed = jnp.concatenate(pieces, axis=0)
    gathered = lax.all_gather(packed, ALL, axis=0, tiled=True).reshape(count, total, PANEL)
    out = []
    for w, kind, (first, rows) in zip(weights, WEIGHT_KINDS, places):
        piece = gathered[:, first : first + rows, :]
        out.append(make_weight(piece, kind, local_shape(w, kind), items, heads))
    first, rows = places[-1]
    gain_all = gathered[:, first : first + rows, :].reshape(count, -1)[:, : gain_row.shape[1]]
    gain_all = gain_all.reshape(count, len(gains), -1)
    whole_gains = [widened(gain_all[:, k, :].reshape(-1)) for k in range(len(gains))]
    return out, whole_gains


def reduce_grads(grad_parts, gain_grads, weights, items, heads):
    count = items * heads
    pieces, places, row = [], [], 0
    for part in grad_parts:
        rows = padded_rows(part.shape[1])
        pieces.append(pad_rows(rounded(part), rows))
        places.append((row, part.shape[1]))
        row += rows
    gain_stack = jnp.stack([g.reshape(count, -1) for g in gain_grads], axis=1).reshape(count, 1, -1)
    gain_block = lane_pad(gain_stack, gain_stack.shape[-1]).reshape(count, -1, PANEL)
    total = -(-(row + gain_block.shape[1]) // ROW_GROUP) * ROW_GROUP
    pieces.append(pad_rows(rounded(gain_block), total - row))
    places.append((row, gain_block.shape[1]))
    packed = jnp.concatenate(pieces, axis=1)
    mine = lax.psum_scatter(
        packed.reshape(count * total, PANEL), "items", scatter_dimension=0, tiled=True
    )
    mine = lax.psum_scatter(mine, "heads", scatter_dimension=0, tiled=True)
    out = []
    for w, kind, (first, rows) in zip(weights, WEIGHT_KINDS, places):
        r, width = local_shape(w, kind)
        panels = -(-width // PANEL)
        block = mine[first : first + rows].reshape(panels, r, PANEL).transpose(1, 0, 2)
        block = widened(lane_cut(block, width))
        out.append(block.T if kind == "cols" else block)
    first, rows = places[-1]
    gain_part = widened(mine[first : first + rows].reshape(-1)[: gain_stack.shape[-1]])
    gain_part = gain_part.reshape(len(gain_grads), -1)
    out += [gain_part[k] for k in range(len(gain_grads))]
    return out


def mlp_block(residual, gain_vec, up_w, down_w):
    normed = rounded(norm_rows(residual, gain_vec))
    before = apply(normed, up_w)
    hidden = rounded(jax.nn.gelu(before))
    return residual + apply(hidden, down_w), (normed, before, hidden)


def mlp_block_back(residual, gain_vec, up_w, down_w, saved, grad_out):
    normed, before, hidden = saved
    grad_round = rounded(grad_out)
    grad_down = grad_blocks(hidden, grad_round, down_w)
    grad_hidden = apply_t(grad_round, down_w)
    unused, gelu_back = jax.vjp(jax.nn.gelu, before)
    grad_before = rounded(gelu_back(grad_hidden)[0])
    grad_up = grad_blocks(normed, grad_before, up_w)
    grad_normed = apply_t(grad_before, up_w)
    grad_residual, grad_gain = norm_backward(residual, gain_vec, grad_normed)
    return grad_out + grad_residual, grad_up, grad_down, grad_gain


def exchange_rows(rows, split):
    if split == 1:
        return [rows]
    heads = lax.axis_size("heads")
    out = [rows]
    for shift in range(1, split):
        pairs = []
        for h in range(heads):
            base, pos = (h // split) * split, h % split
            pairs.append((h, base + (pos - shift) % split))
        out.append(lax.ppermute(rows, "heads", pairs))
    return out


def return_rows(parts, split):
    total = parts[0]
    heads = lax.axis_size("heads")
    for shift in range(1, split):
        pairs = []
        for h in range(heads):
            base, pos = (h // split) * split, h % split
            pairs.append((h, base + (pos + shift) % split))
        total = total + lax.ppermute(parts[shift], "heads", pairs)
    return total


def attention_block(residual, gain_vec, weight_set, split):
    query_w, key_w, value_w, out_w = weight_set
    rows = residual.shape[0]
    normed = rounded(norm_rows(residual, gain_vec))
    query_rows = rounded(apply(normed, query_w))
    key_rows = rounded(apply(normed, key_w))
    value_rows = rounded(apply(normed, value_w))
    heads_n = query_rows.shape[1] // HEAD
    key_all = jnp.concatenate(exchange_rows(key_rows, split), axis=0)
    value_all = jnp.concatenate(exchange_rows(value_rows, split), axis=0)
    keys = key_all.shape[0]
    q4 = query_rows.reshape(rows, heads_n, HEAD)
    k4 = key_all.reshape(keys, heads_n, HEAD)
    v4 = value_all.reshape(keys, heads_n, HEAD)
    scores = jnp.einsum("qhd,khd->hqk", q4, k4, preferred_element_type=jnp.float32) * (
        1.0 / math.sqrt(HEAD)
    )
    row_top = jnp.max(scores, axis=-1, keepdims=True)
    raw_weights = jnp.exp(scores - row_top)
    row_total = jnp.sum(raw_weights, axis=-1, keepdims=True)
    weights_low = rounded(raw_weights / row_total)
    mixed_full = jnp.einsum("hqk,khd->qhd", weights_low, v4, preferred_element_type=jnp.float32)
    mixed = rounded(mixed_full.reshape(rows, heads_n * HEAD))
    saved = (normed, q4, k4, v4, weights_low, mixed_full, mixed)
    return residual + apply(mixed, out_w), saved


def attention_block_back(residual, gain_vec, weight_set, split, saved, grad_out):
    query_w, key_w, value_w, out_w = weight_set
    normed, q4, k4, v4, weights_low, mixed_full, mixed = saved
    rows = residual.shape[0]
    keys = k4.shape[0]
    scale = 1.0 / math.sqrt(HEAD)
    grad_round = rounded(grad_out)
    grad_out_w = grad_blocks(mixed, grad_round, out_w)
    grad_mixed = rounded(apply_t(grad_round, out_w)).reshape(q4.shape)
    grad_value = jnp.einsum(
        "hqk,qhd->khd", weights_low, grad_mixed, preferred_element_type=jnp.float32
    ).reshape(keys, -1)
    row_dot = jnp.sum(widened(grad_mixed) * mixed_full, axis=-1).T[:, :, None]
    grad_weights = jnp.einsum("qhd,khd->hqk", grad_mixed, v4, preferred_element_type=jnp.float32)
    grad_scores = rounded(widened(weights_low) * (grad_weights - row_dot))
    grad_query = jnp.einsum("hqk,khd->qhd", grad_scores, k4, preferred_element_type=jnp.float32)
    grad_query = rounded((grad_query * scale).reshape(rows, -1))
    grad_key = jnp.einsum("hqk,qhd->khd", grad_scores, q4, preferred_element_type=jnp.float32)
    grad_key = (grad_key * scale).reshape(keys, -1)
    if split > 1:
        grad_key = return_rows(jnp.split(grad_key, split, axis=0), split)
        grad_value = return_rows(jnp.split(grad_value, split, axis=0), split)
    grad_key = rounded(grad_key)
    grad_value = rounded(grad_value)
    grad_query_w = grad_blocks(normed, grad_query, query_w)
    grad_key_w = grad_blocks(normed, grad_key, key_w)
    grad_value_w = grad_blocks(normed, grad_value, value_w)
    grad_normed = (
        apply_t(grad_query, query_w) + apply_t(grad_key, key_w) + apply_t(grad_value, value_w)
    )
    grad_residual, grad_gain = norm_backward(residual, gain_vec, grad_normed)
    return (grad_out + grad_residual, grad_query_w, grad_key_w, grad_value_w, grad_out_w, grad_gain)


def pixel_window(pixels, item_ids, item):
    count = pixels.shape[1]
    width = min(count, -(-PIX_MOST // LANE) * LANE + LANE)
    start = jnp.sum((item_ids < item).astype(jnp.int32))
    first = jnp.clip((start // LANE) * LANE, 0, count - width)
    window = lax.dynamic_slice_in_dim(pixels, first, width, axis=1)
    ids = lax.dynamic_slice_in_dim(item_ids, first, width, axis=0)
    return window, ids == item


SOFTMAX_ROWS = 512


def softmax_mix_kernel(keyed_ref, pixel_ref, mask_ref, weights_ref, mix_ref):
    scores = jnp.dot(keyed_ref[...], pixel_ref[...], preferred_element_type=jnp.float32)
    scores = jnp.where(mask_ref[...] > 0.0, scores, MASKED)
    row_top = jnp.max(scores, axis=-1, keepdims=True)
    raw = jnp.exp(scores - row_top)
    row_total = jnp.sum(raw, axis=-1, keepdims=True)
    weights = (raw / row_total).astype(jnp.bfloat16)
    weights_ref[...] = weights
    mix_ref[...] = lax.dot_general(
        weights, pixel_ref[...], (((1,), (1,)), ((), ())), preferred_element_type=jnp.float32
    )


def softmax_mix(keyed, pixel_pad, mask):
    rows, channels = keyed.shape
    width = pixel_pad.shape[1]
    block = min(SOFTMAX_ROWS, rows)
    cost = pl.CostEstimate(
        flops=4 * rows * channels * width,
        transcendentals=rows * width,
        bytes_accessed=2 * (rows * channels + channels * width + rows * width) + 4 * rows * channels,
    )
    return pl.pallas_call(
        softmax_mix_kernel,
        grid=(rows // block,),
        in_specs=[
            pl.BlockSpec((block, channels), lambda i: (i, 0)),
            pl.BlockSpec((channels, width), lambda i: (0, 0)),
            pl.BlockSpec((1, width), lambda i: (0, 0)),
        ],
        out_specs=[
            pl.BlockSpec((block, width), lambda i: (i, 0)),
            pl.BlockSpec((block, channels), lambda i: (i, 0)),
        ],
        out_shape=[
            jax.ShapeDtypeStruct((rows, width), jnp.bfloat16),
            jax.ShapeDtypeStruct((rows, channels), jnp.float32),
        ],
        compiler_params=pltpu.CompilerParams(vmem_limit_bytes=48 * 1024 * 1024),
        cost_estimate=cost,
    )(keyed, pixel_pad, mask)


def softmax_back_kernel(grad_ref, pixel_ref, weights_ref, dot_ref, mix_ref):
    grad_weights = jnp.dot(grad_ref[...], pixel_ref[...], preferred_element_type=jnp.float32)
    weights = weights_ref[...].astype(jnp.float32)
    grad_scores = (weights * (grad_weights - dot_ref[...])).astype(jnp.bfloat16)
    mix_ref[...] = lax.dot_general(
        grad_scores, pixel_ref[...], (((1,), (1,)), ((), ())), preferred_element_type=jnp.float32
    )


def softmax_back_mix(grad_keyed, pixel_pad, weights_low, row_dot):
    rows, channels = grad_keyed.shape
    width = pixel_pad.shape[1]
    block = min(SOFTMAX_ROWS, rows)
    cost = pl.CostEstimate(
        flops=4 * rows * channels * width,
        transcendentals=0,
        bytes_accessed=2 * (rows * channels + channels * width + rows * width) + 4 * rows * (channels + 1),
    )
    return pl.pallas_call(
        softmax_back_kernel,
        grid=(rows // block,),
        in_specs=[
            pl.BlockSpec((block, channels), lambda i: (i, 0)),
            pl.BlockSpec((channels, width), lambda i: (0, 0)),
            pl.BlockSpec((block, width), lambda i: (i, 0)),
            pl.BlockSpec((block, 1), lambda i: (i, 0)),
        ],
        out_specs=pl.BlockSpec((block, channels), lambda i: (i, 0)),
        out_shape=jax.ShapeDtypeStruct((rows, channels), jnp.float32),
        compiler_params=pltpu.CompilerParams(vmem_limit_bytes=48 * 1024 * 1024),
        cost_estimate=cost,
    )(grad_keyed, pixel_pad, weights_low, row_dot)


def cross_block(residual, gain_vec, query_w, key_w, value_w, out_w, pixel_norm, allowed):
    scale = 1.0 / math.sqrt(residual.shape[1])
    normed = rounded(norm_rows(residual, gain_vec))
    query_rows = rounded(apply(normed, query_w))
    query_keyed = rounded(apply(query_rows, key_w) * scale)
    pixel_pad, mask = allowed
    channels = pixel_norm.shape[0]
    keyed_pad = jnp.pad(query_keyed, ((0, 0), (0, pixel_pad.shape[0] - channels)))
    weights_low, pixel_mix = softmax_mix(keyed_pad, pixel_pad, mask)
    pixel_mix = pixel_mix[:, :channels]
    mixed = rounded(split_apply_t(pixel_mix, value_w))
    saved = (normed, query_rows, weights_low, pixel_mix, mixed)
    return residual + apply(mixed, out_w), saved


def cross_block_back(
    residual, gain_vec, query_w, key_w, value_w, out_w, pixel_norm, allowed, saved, grad_out
):
    normed, query_rows, weights_low, pixel_mix, mixed = saved
    scale = 1.0 / math.sqrt(residual.shape[1])
    grad_round = rounded(grad_out)
    grad_out_w = grad_blocks(mixed, grad_round, out_w)
    grad_mixed = rounded(apply_t(grad_round, out_w))
    grad_keyed = rounded(apply(grad_mixed, value_w))
    row_dot = jnp.sum(widened(grad_keyed) * pixel_mix, axis=-1, keepdims=True)
    pixel_pad = allowed[0]
    channels = pixel_norm.shape[0]
    grad_pad = jnp.pad(grad_keyed, ((0, 0), (0, pixel_pad.shape[0] - channels)))
    score_mix = softmax_back_mix(grad_pad, pixel_pad, weights_low, row_dot)[:, :channels]
    grad_query = rounded(split_apply_t(score_mix, key_w) * scale)
    grad_query_w = grad_blocks(normed, grad_query, query_w)
    grad_key_w = split_grad_blocks(query_rows, score_mix, key_w) * scale
    grad_value_w = split_grad_blocks(grad_mixed, pixel_mix, value_w)
    grad_normed = apply_t(grad_query, query_w)
    grad_residual, grad_gain = norm_backward(residual, gain_vec, grad_normed)
    return (grad_out + grad_residual, grad_query_w, grad_key_w, grad_value_w, grad_out_w, grad_gain)


def local(latents, pixels, pixel_item, cotangent, *params):
    weights, gains = params[:12], params[12:]
    items = lax.axis_size("items")
    heads = lax.axis_size("heads")
    rows = latents.shape[0]
    split = max(1, NLAT // rows)
    (
        query_cross,
        key_cross,
        value_cross,
        out_cross,
        up_cross,
        down_cross,
        query_self,
        key_self,
        value_self,
        out_self,
        up_self,
        down_self,
    ), gain_list = gather_weights(weights, gains, items, heads)
    attention_set = (query_self, key_self, value_self, out_self)

    item = (lax.axis_index("heads") * rows) // NLAT
    window, allowed = pixel_window(pixels, pixel_item[0], item)
    pixel_norm = rounded(norm_pixels(widened(window)))
    channels = pixel_norm.shape[0]
    pixel_pad = jnp.pad(pixel_norm, ((0, -channels % LANE), (0, 0)))
    mask = allowed.astype(jnp.float32)[None, :]
    pixel_norm, pixel_pad, mask = lax.optimization_barrier((pixel_norm, pixel_pad, mask))
    allowed = (pixel_pad, mask)

    start_rows = widened(latents)
    after_cross, saved_cross = cross_block(
        start_rows, gain_list[0], query_cross, key_cross, value_cross, out_cross, pixel_norm, allowed
    )
    after_mlp_one, saved_mlp_one = mlp_block(after_cross, gain_list[1], up_cross, down_cross)
    after_self, saved_self = attention_block(after_mlp_one, gain_list[2], attention_set, split)
    final_rows, saved_mlp_two = mlp_block(after_self, gain_list[3], up_self, down_self)

    grad_final = widened(cotangent)
    grad_after_self, grad_self_up, grad_self_down, grad_gain_four = mlp_block_back(
        after_self, gain_list[3], up_self, down_self, saved_mlp_two, grad_final
    )
    (
        grad_after_mlp,
        grad_self_query,
        grad_self_key,
        grad_self_value,
        grad_self_out,
        grad_gain_three,
    ) = attention_block_back(
        after_mlp_one, gain_list[2], attention_set, split, saved_self, grad_after_self
    )
    grad_after_cross, grad_cross_up, grad_cross_down, grad_gain_two = mlp_block_back(
        after_cross, gain_list[1], up_cross, down_cross, saved_mlp_one, grad_after_mlp
    )
    (
        latents_grad,
        grad_cross_query,
        grad_cross_key,
        grad_cross_value,
        grad_cross_out,
        grad_gain_one,
    ) = cross_block_back(
        start_rows,
        gain_list[0],
        query_cross,
        key_cross,
        value_cross,
        out_cross,
        pixel_norm,
        allowed,
        saved_cross,
        grad_after_cross,
    )
    weight_grads = (
        grad_cross_query,
        grad_cross_key,
        grad_cross_value,
        grad_cross_out,
        grad_cross_up,
        grad_cross_down,
        grad_self_query,
        grad_self_key,
        grad_self_value,
        grad_self_out,
        grad_self_up,
        grad_self_down,
    )
    gain_grads = (grad_gain_one, grad_gain_two, grad_gain_three, grad_gain_four)
    reduced = reduce_grads(weight_grads, gain_grads, weights, items, heads)
    shaped = [r.reshape(w.shape) for r, w in zip(reduced[:12], weights)]
    shaped += [r.reshape(g.shape) for r, g in zip(reduced[12:], gains)]
    return (rounded(final_rows), latents_grad, *shaped)


def solution(mesh):
    weight_specs = (
        P(ALL, None),
        P(None, ALL),
        P(None, ALL),
        P(ALL, None),
        P("items", "heads"),
        P("heads", "items"),
        P("items", "heads"),
        P("items", "heads"),
        P("items", "heads"),
        P("heads", "items"),
        P("items", "heads"),
        P("heads", "items"),
    )
    gain_specs = (P(ALL),) * 4
    placed = (P(ALL, None), P(None, "items"), P("items", None), P(ALL, None)) + weight_specs + gain_specs
    return jax.shard_map(
        local,
        mesh=mesh,
        in_specs=placed,
        out_specs=(P(ALL, None), P(ALL, None)) + weight_specs + gain_specs,
        check_vma=False,
    )
```

```python
import math

import jax
import jax.numpy as jnp
from jax import lax
from jax.experimental import pallas as pl
from jax.experimental.pallas import tpu as pltpu
from jax.sharding import PartitionSpec as P

HEAD = 128
NLAT = 512
PIX_MOST = 6144
LANE = 128

EPSILON = 1e-05
MASKED = -1e30
ALL = ("items", "heads")


def rounded(values):
    return values.astype(jnp.bfloat16)


def widened(values):
    return values.astype(jnp.float32)


def product(left_side, right_side):
    return jnp.dot(left_side, right_side, preferred_element_type=jnp.float32)


def product_tn(left_side, right_side):
    return lax.dot_general(
        left_side, right_side, (((0,), (0,)), ((), ())), preferred_element_type=jnp.float32
    )


def product_nt(left_side, right_side):
    return lax.dot_general(
        left_side, right_side, (((1,), (1,)), ((), ())), preferred_element_type=jnp.float32
    )


def split_parts(values):
    high = rounded(values)
    return high, rounded(values - widened(high))


def split_apply_t(values_f32, weight):
    high, low = split_parts(values_f32)
    return apply_t(high, weight) + apply_t(low, weight)


def norm_rows(values, gain_vec):
    centre = values - jnp.mean(values, axis=-1, keepdims=True)
    spread = jnp.mean(centre * centre, axis=-1, keepdims=True)
    return centre * lax.rsqrt(spread + EPSILON) * gain_vec


def norm_pixels(values):
    centre = values - jnp.mean(values, axis=0, keepdims=True)
    spread = jnp.mean(centre * centre, axis=0, keepdims=True)
    return centre * lax.rsqrt(spread + EPSILON)


def norm_backward(residual, gain_vec, grad_normed):
    unused, norm_back = jax.vjp(norm_rows, residual, gain_vec)
    return norm_back(grad_normed)


WEIGHT_KINDS = (
    "rows",
    "cols",
    "cols",
    "rows",
    "ih",
    "hi",
    "ih",
    "ih",
    "ih",
    "hi",
    "ih",
    "hi",
)

PANEL = 128
ROW_TILE = 16
ROW_GROUP = 48


def contract(left, right, left_dims, right_dims):
    return lax.dot_general(
        left, right, ((left_dims, right_dims), ((), ())), preferred_element_type=jnp.float32
    )


def lane_pad(values, width):
    panels = -(-width // PANEL)
    if panels * PANEL != width:
        pad = [(0, 0)] * (values.ndim - 1) + [(0, panels * PANEL - width)]
        values = jnp.pad(values, pad)
    return values.reshape(values.shape[:-1] + (panels, PANEL))


def lane_cut(values, width):
    values = values.reshape(values.shape[:-2] + (-1,))
    return values if values.shape[-1] == width else values[..., :width]


def local_panels(block):
    rows, width = block.shape
    parts = lane_pad(block, width).transpose(1, 0, 2)
    return parts.reshape(-1, PANEL)


def padded_rows(rows):
    return -(-rows // ROW_TILE) * ROW_TILE


def local_shape(w, kind):
    return (w.shape[1], w.shape[0]) if kind == "cols" else w.shape


def make_weight(piece, kind, shape, items, heads):
    rows, width = shape
    panels = -(-width // PANEL)
    blocks = piece[:, : panels * rows, :].reshape(items * heads, panels, rows, PANEL)
    if kind in ("ih", "hi"):
        blocks = blocks.reshape(items, heads, panels, rows, PANEL)
    return kind, blocks, width


def apply(values, weight):
    kind, blocks, width = weight
    count = values.shape[0]
    if kind in ("rows", "cols"):
        devices, panels, rows, lanes = blocks.shape
        out = contract(values.reshape(count, devices, rows), blocks, (1, 2), (0, 2))
        return lane_cut(out, width)
    items, heads, panels, rows, lanes = blocks.shape
    if kind == "ih":
        out = contract(values.reshape(count, items, rows), blocks, (1, 2), (0, 3))
    else:
        out = contract(values.reshape(count, heads, rows), blocks, (1, 2), (1, 3))
    return lane_cut(out, width).reshape(count, -1)


def apply_t(values, weight):
    kind, blocks, width = weight
    count = values.shape[0]
    if kind in ("rows", "cols"):
        devices, panels, rows, lanes = blocks.shape
        out = contract(lane_pad(values, width), blocks, (1, 2), (1, 3))
        return out.reshape(count, devices * rows)
    items, heads, panels, rows, lanes = blocks.shape
    if kind == "ih":
        spread = lane_pad(values.reshape(count, heads, width), width)
        out = contract(spread, blocks, (1, 2, 3), (1, 2, 4))
        return out.reshape(count, items * rows)
    spread = lane_pad(values.reshape(count, items, width), width)
    out = contract(spread, blocks, (1, 2, 3), (0, 2, 4))
    return out.reshape(count, heads * rows)


def grad_blocks(values, grads, weight):
    kind, blocks, width = weight
    count = values.shape[0]
    if kind in ("rows", "cols"):
        devices, panels, rows, lanes = blocks.shape
        out = contract(values.reshape(count, devices, rows), lane_pad(grads, width), (0,), (0,))
        out = out.transpose(0, 2, 1, 3)
    else:
        items, heads, panels, rows, lanes = blocks.shape
        devices = items * heads
        if kind == "ih":
            spread = lane_pad(grads.reshape(count, heads, width), width)
            out = contract(values.reshape(count, items, rows), spread, (0,), (0,))
            out = out.transpose(0, 2, 3, 1, 4)
        else:
            spread = lane_pad(grads.reshape(count, items, width), width)
            out = contract(values.reshape(count, heads, rows), spread, (0,), (0,))
            out = out.transpose(2, 0, 3, 1, 4)
    return out.reshape(devices, -1, PANEL)


def split_grad_blocks(values, grads_f32, weight):
    high, low = split_parts(grads_f32)
    return grad_blocks(values, high, weight) + grad_blocks(values, low, weight)


def pad_rows(block, rows):
    extra = rows - block.shape[-2]
    if extra == 0:
        return block
    pad = [(0, 0)] * (block.ndim - 2) + [(0, extra), (0, 0)]
    return jnp.pad(block, pad)


def gather_weights(weights, gains, items, heads):
    count = items * heads
    pieces, places, row = [], [], 0
    for w, kind in zip(weights, WEIGHT_KINDS):
        block = local_panels(rounded(w.T if kind == "cols" else w))
        rows = padded_rows(block.shape[0])
        pieces.append(pad_rows(block, rows))
        places.append((row, rows))
        row += rows
    gain_row = rounded(jnp.concatenate(gains)).reshape(1, -1)
    gain_block = local_panels(gain_row)
    total = -(-(row + gain_block.shape[0]) // ROW_GROUP) * ROW_GROUP
    pieces.append(pad_rows(gain_block, total - row))
    places.append((row, gain_block.shape[0]))
    packed = jnp.concatenate(pieces, axis=0)
    gathered = lax.all_gather(packed, ALL, axis=0, tiled=True).reshape(count, total, PANEL)
    out = []
    for w, kind, (first, rows) in zip(weights, WEIGHT_KINDS, places):
        piece = gathered[:, first : first + rows, :]
        out.append(make_weight(piece, kind, local_shape(w, kind), items, heads))
    first, rows = places[-1]
    gain_all = gathered[:, first : first + rows, :].reshape(count, -1)[:, : gain_row.shape[1]]
    gain_all = gain_all.reshape(count, len(gains), -1)
    whole_gains = [widened(gain_all[:, k, :].reshape(-1)) for k in range(len(gains))]
    return out, whole_gains


def reduce_grads(grad_parts, gain_grads, weights, items, heads):
    count = items * heads
    pieces, places, row = [], [], 0
    for part in grad_parts:
        rows = padded_rows(part.shape[1])
        pieces.append(pad_rows(rounded(part), rows))
        places.append((row, part.shape[1]))
        row += rows
    gain_stack = jnp.stack([g.reshape(count, -1) for g in gain_grads], axis=1).reshape(count, 1, -1)
    gain_block = lane_pad(gain_stack, gain_stack.shape[-1]).reshape(count, -1, PANEL)
    total = -(-(row + gain_block.shape[1]) // ROW_GROUP) * ROW_GROUP
    pieces.append(pad_rows(rounded(gain_block), total - row))
    places.append((row, gain_block.shape[1]))
    packed = jnp.concatenate(pieces, axis=1)
    mine = lax.psum_scatter(
        packed.reshape(count * total, PANEL), "items", scatter_dimension=0, tiled=True
    )
    mine = lax.psum_scatter(mine, "heads", scatter_dimension=0, tiled=True)
    out = []
    for w, kind, (first, rows) in zip(weights, WEIGHT_KINDS, places):
        r, width = local_shape(w, kind)
        panels = -(-width // PANEL)
        block = mine[first : first + rows].reshape(panels, r, PANEL).transpose(1, 0, 2)
        block = widened(lane_cut(block, width))
        out.append(block.T if kind == "cols" else block)
    first, rows = places[-1]
    gain_part = widened(mine[first : first + rows].reshape(-1)[: gain_stack.shape[-1]])
    gain_part = gain_part.reshape(len(gain_grads), -1)
    out += [gain_part[k] for k in range(len(gain_grads))]
    return out


def mlp_block(residual, gain_vec, up_w, down_w):
    normed = rounded(norm_rows(residual, gain_vec))
    before = apply(normed, up_w)
    hidden = rounded(jax.nn.gelu(before))
    return residual + apply(hidden, down_w), (normed, before, hidden)


def mlp_block_back(residual, gain_vec, up_w, down_w, saved, grad_out):
    normed, before, hidden = saved
    grad_round = rounded(grad_out)
    grad_down = grad_blocks(hidden, grad_round, down_w)
    grad_hidden = apply_t(grad_round, down_w)
    unused, gelu_back = jax.vjp(jax.nn.gelu, before)
    grad_before = rounded(gelu_back(grad_hidden)[0])
    grad_up = grad_blocks(normed, grad_before, up_w)
    grad_normed = apply_t(grad_before, up_w)
    grad_residual, grad_gain = norm_backward(residual, gain_vec, grad_normed)
    return grad_out + grad_residual, grad_up, grad_down, grad_gain


def exchange_rows(rows, split):
    if split == 1:
        return [rows]
    heads = lax.axis_size("heads")
    out = [rows]
    for shift in range(1, split):
        pairs = []
        for h in range(heads):
            base, pos = (h // split) * split, h % split
            pairs.append((h, base + (pos - shift) % split))
        out.append(lax.ppermute(rows, "heads", pairs))
    return out


def return_rows(parts, split):
    total = parts[0]
    heads = lax.axis_size("heads")
    for shift in range(1, split):
        pairs = []
        for h in range(heads):
            base, pos = (h // split) * split, h % split
            pairs.append((h, base + (pos + shift) % split))
        total = total + lax.ppermute(parts[shift], "heads", pairs)
    return total


def attention_block(residual, gain_vec, weight_set, split):
    query_w, key_w, value_w, out_w = weight_set
    rows = residual.shape[0]
    normed = rounded(norm_rows(residual, gain_vec))
    query_rows = rounded(apply(normed, query_w))
    key_rows = rounded(apply(normed, key_w))
    value_rows = rounded(apply(normed, value_w))
    heads_n = query_rows.shape[1] // HEAD
    key_all = jnp.concatenate(exchange_rows(key_rows, split), axis=0)
    value_all = jnp.concatenate(exchange_rows(value_rows, split), axis=0)
    keys = key_all.shape[0]
    q4 = query_rows.reshape(rows, heads_n, HEAD)
    k4 = key_all.reshape(keys, heads_n, HEAD)
    v4 = value_all.reshape(keys, heads_n, HEAD)
    scores = jnp.einsum("qhd,khd->hqk", q4, k4, preferred_element_type=jnp.float32) * (
        1.0 / math.sqrt(HEAD)
    )
    row_top = jnp.max(scores, axis=-1, keepdims=True)
    raw_weights = jnp.exp(scores - row_top)
    row_total = jnp.sum(raw_weights, axis=-1, keepdims=True)
    weights_low = rounded(raw_weights * (1.0 / row_total))
    mixed_full = jnp.einsum("hqk,khd->qhd", weights_low, v4, preferred_element_type=jnp.float32)
    mixed = rounded(mixed_full.reshape(rows, heads_n * HEAD))
    saved = (normed, q4, k4, v4, weights_low, mixed_full, mixed)
    return residual + apply(mixed, out_w), saved


def attention_block_back(residual, gain_vec, weight_set, split, saved, grad_out):
    query_w, key_w, value_w, out_w = weight_set
    normed, q4, k4, v4, weights_low, mixed_full, mixed = saved
    rows = residual.shape[0]
    keys = k4.shape[0]
    scale = 1.0 / math.sqrt(HEAD)
    grad_round = rounded(grad_out)
    grad_out_w = grad_blocks(mixed, grad_round, out_w)
    grad_mixed = rounded(apply_t(grad_round, out_w)).reshape(q4.shape)
    grad_value = jnp.einsum(
        "hqk,qhd->khd", weights_low, grad_mixed, preferred_element_type=jnp.float32
    ).reshape(keys, -1)
    row_dot = jnp.sum(widened(grad_mixed) * mixed_full, axis=-1).T[:, :, None]
    grad_weights = jnp.einsum("qhd,khd->hqk", grad_mixed, v4, preferred_element_type=jnp.float32)
    grad_scores = rounded(widened(weights_low) * (grad_weights - row_dot))
    grad_query = jnp.einsum("hqk,khd->qhd", grad_scores, k4, preferred_element_type=jnp.float32)
    grad_query = rounded((grad_query * scale).reshape(rows, -1))
    grad_key = jnp.einsum("hqk,qhd->khd", grad_scores, q4, preferred_element_type=jnp.float32)
    grad_key = (grad_key * scale).reshape(keys, -1)
    if split > 1:
        grad_key = return_rows(jnp.split(grad_key, split, axis=0), split)
        grad_value = return_rows(jnp.split(grad_value, split, axis=0), split)
    grad_key = rounded(grad_key)
    grad_value = rounded(grad_value)
    grad_query_w = grad_blocks(normed, grad_query, query_w)
    grad_key_w = grad_blocks(normed, grad_key, key_w)
    grad_value_w = grad_blocks(normed, grad_value, value_w)
    grad_normed = (
        apply_t(grad_query, query_w) + apply_t(grad_key, key_w) + apply_t(grad_value, value_w)
    )
    grad_residual, grad_gain = norm_backward(residual, gain_vec, grad_normed)
    return (grad_out + grad_residual, grad_query_w, grad_key_w, grad_value_w, grad_out_w, grad_gain)


def pixel_window(pixels, item_ids, item):
    count = pixels.shape[1]
    width = min(count, -(-PIX_MOST // LANE) * LANE + LANE)
    start = jnp.sum((item_ids < item).astype(jnp.int32))
    first = jnp.clip((start // LANE) * LANE, 0, count - width)
    window = lax.dynamic_slice_in_dim(pixels, first, width, axis=1)
    ids = lax.dynamic_slice_in_dim(item_ids, first, width, axis=0)
    return window, ids == item


SOFTMAX_ROWS = 256


def softmax_mix_kernel(keyed_ref, pixel_ref, mask_ref, weights_ref, mix_ref):
    scores = jnp.dot(keyed_ref[...], pixel_ref[...], preferred_element_type=jnp.float32)
    scores = jnp.where(mask_ref[...] > 0.0, scores, MASKED)
    row_top = jnp.max(scores, axis=-1, keepdims=True)
    raw = jnp.exp(scores - row_top)
    row_total = jnp.sum(raw, axis=-1, keepdims=True)
    weights = (raw * (1.0 / row_total)).astype(jnp.bfloat16)
    weights_ref[...] = weights
    mix_ref[...] = lax.dot_general(
        weights, pixel_ref[...], (((1,), (1,)), ((), ())), preferred_element_type=jnp.float32
    )


def softmax_mix(keyed, pixel_pad, mask):
    rows, channels = keyed.shape
    width = pixel_pad.shape[1]
    block = min(SOFTMAX_ROWS, rows)
    cost = pl.CostEstimate(
        flops=4 * rows * channels * width,
        transcendentals=rows * width,
        bytes_accessed=2 * (rows * channels + channels * width + rows * width) + 4 * rows * channels,
    )
    return pl.pallas_call(
        softmax_mix_kernel,
        grid=(rows // block,),
        in_specs=[
            pl.BlockSpec((block, channels), lambda i: (i, 0)),
            pl.BlockSpec((channels, width), lambda i: (0, 0)),
            pl.BlockSpec((1, width), lambda i: (0, 0)),
        ],
        out_specs=[
            pl.BlockSpec((block, width), lambda i: (i, 0)),
            pl.BlockSpec((block, channels), lambda i: (i, 0)),
        ],
        out_shape=[
            jax.ShapeDtypeStruct((rows, width), jnp.bfloat16),
            jax.ShapeDtypeStruct((rows, channels), jnp.float32),
        ],
        compiler_params=pltpu.CompilerParams(vmem_limit_bytes=48 * 1024 * 1024),
        cost_estimate=cost,
    )(keyed, pixel_pad, mask)


def softmax_back_kernel(grad_ref, pixel_ref, weights_ref, dot_ref, mix_ref):
    grad_weights = jnp.dot(grad_ref[...], pixel_ref[...], preferred_element_type=jnp.float32)
    weights = weights_ref[...].astype(jnp.float32)
    grad_scores = (weights * (grad_weights - dot_ref[...])).astype(jnp.bfloat16)
    mix_ref[...] = lax.dot_general(
        grad_scores, pixel_ref[...], (((1,), (1,)), ((), ())), preferred_element_type=jnp.float32
    )


def softmax_back_mix(grad_keyed, pixel_pad, weights_low, row_dot):
    rows, channels = grad_keyed.shape
    width = pixel_pad.shape[1]
    block = min(SOFTMAX_ROWS, rows)
    cost = pl.CostEstimate(
        flops=4 * rows * channels * width,
        transcendentals=0,
        bytes_accessed=2 * (rows * channels + channels * width + rows * width) + 4 * rows * (channels + 1),
    )
    return pl.pallas_call(
        softmax_back_kernel,
        grid=(rows // block,),
        in_specs=[
            pl.BlockSpec((block, channels), lambda i: (i, 0)),
            pl.BlockSpec((channels, width), lambda i: (0, 0)),
            pl.BlockSpec((block, width), lambda i: (i, 0)),
            pl.BlockSpec((block, 1), lambda i: (i, 0)),
        ],
        out_specs=pl.BlockSpec((block, channels), lambda i: (i, 0)),
        out_shape=jax.ShapeDtypeStruct((rows, channels), jnp.float32),
        compiler_params=pltpu.CompilerParams(vmem_limit_bytes=48 * 1024 * 1024),
        cost_estimate=cost,
    )(grad_keyed, pixel_pad, weights_low, row_dot)


def cross_block(residual, gain_vec, query_w, key_w, value_w, out_w, pixel_norm, allowed):
    scale = 1.0 / math.sqrt(residual.shape[1])
    normed = rounded(norm_rows(residual, gain_vec))
    query_rows = rounded(apply(normed, query_w))
    query_keyed = rounded(apply(query_rows, key_w) * scale)
    pixel_pad, mask = allowed
    channels = pixel_norm.shape[0]
    keyed_pad = jnp.pad(query_keyed, ((0, 0), (0, pixel_pad.shape[0] - channels)))
    weights_low, pixel_mix = softmax_mix(keyed_pad, pixel_pad, mask)
    pixel_mix = pixel_mix[:, :channels]
    mixed = rounded(split_apply_t(pixel_mix, value_w))
    saved = (normed, query_rows, weights_low, pixel_mix, mixed)
    return residual + apply(mixed, out_w), saved


def cross_block_back(
    residual, gain_vec, query_w, key_w, value_w, out_w, pixel_norm, allowed, saved, grad_out
):
    normed, query_rows, weights_low, pixel_mix, mixed = saved
    scale = 1.0 / math.sqrt(residual.shape[1])
    grad_round = rounded(grad_out)
    grad_out_w = grad_blocks(mixed, grad_round, out_w)
    grad_mixed = rounded(apply_t(grad_round, out_w))
    grad_keyed = rounded(apply(grad_mixed, value_w))
    row_dot = jnp.sum(widened(grad_keyed) * pixel_mix, axis=-1, keepdims=True)
    pixel_pad = allowed[0]
    channels = pixel_norm.shape[0]
    grad_pad = jnp.pad(grad_keyed, ((0, 0), (0, pixel_pad.shape[0] - channels)))
    score_mix = softmax_back_mix(grad_pad, pixel_pad, weights_low, row_dot)[:, :channels]
    grad_query = rounded(split_apply_t(score_mix, key_w) * scale)
    grad_query_w = grad_blocks(normed, grad_query, query_w)
    grad_key_w = split_grad_blocks(query_rows, score_mix, key_w) * scale
    grad_value_w = split_grad_blocks(grad_mixed, pixel_mix, value_w)
    grad_normed = apply_t(grad_query, query_w)
    grad_residual, grad_gain = norm_backward(residual, gain_vec, grad_normed)
    return (grad_out + grad_residual, grad_query_w, grad_key_w, grad_value_w, grad_out_w, grad_gain)


def local(latents, pixels, pixel_item, cotangent, *params):
    weights, gains = params[:12], params[12:]
    items = lax.axis_size("items")
    heads = lax.axis_size("heads")
    rows = latents.shape[0]
    split = max(1, NLAT // rows)
    (
        query_cross,
        key_cross,
        value_cross,
        out_cross,
        up_cross,
        down_cross,
        query_self,
        key_self,
        value_self,
        out_self,
        up_self,
        down_self,
    ), gain_list = gather_weights(weights, gains, items, heads)
    attention_set = (query_self, key_self, value_self, out_self)

    item = (lax.axis_index("heads") * rows) // NLAT
    window, allowed = pixel_window(pixels, pixel_item[0], item)
    pixel_norm = rounded(norm_pixels(widened(window)))
    channels = pixel_norm.shape[0]
    pixel_pad = jnp.pad(pixel_norm, ((0, -channels % LANE), (0, 0)))
    mask = allowed.astype(jnp.float32)[None, :]
    pixel_norm, pixel_pad, mask = lax.optimization_barrier((pixel_norm, pixel_pad, mask))
    allowed = (pixel_pad, mask)

    start_rows = widened(latents)
    after_cross, saved_cross = cross_block(
        start_rows, gain_list[0], query_cross, key_cross, value_cross, out_cross, pixel_norm, allowed
    )
    after_mlp_one, saved_mlp_one = mlp_block(after_cross, gain_list[1], up_cross, down_cross)
    after_self, saved_self = attention_block(after_mlp_one, gain_list[2], attention_set, split)
    final_rows, saved_mlp_two = mlp_block(after_self, gain_list[3], up_self, down_self)

    grad_final = widened(cotangent)
    grad_after_self, grad_self_up, grad_self_down, grad_gain_four = mlp_block_back(
        after_self, gain_list[3], up_self, down_self, saved_mlp_two, grad_final
    )
    (
        grad_after_mlp,
        grad_self_query,
        grad_self_key,
        grad_self_value,
        grad_self_out,
        grad_gain_three,
    ) = attention_block_back(
        after_mlp_one, gain_list[2], attention_set, split, saved_self, grad_after_self
    )
    grad_after_cross, grad_cross_up, grad_cross_down, grad_gain_two = mlp_block_back(
        after_cross, gain_list[1], up_cross, down_cross, saved_mlp_one, grad_after_mlp
    )
    (
        latents_grad,
        grad_cross_query,
        grad_cross_key,
        grad_cross_value,
        grad_cross_out,
        grad_gain_one,
    ) = cross_block_back(
        start_rows,
        gain_list[0],
        query_cross,
        key_cross,
        value_cross,
        out_cross,
        pixel_norm,
        allowed,
        saved_cross,
        grad_after_cross,
    )
    weight_grads = (
        grad_cross_query,
        grad_cross_key,
        grad_cross_value,
        grad_cross_out,
        grad_cross_up,
        grad_cross_down,
        grad_self_query,
        grad_self_key,
        grad_self_value,
        grad_self_out,
        grad_self_up,
        grad_self_down,
    )
    gain_grads = (grad_gain_one, grad_gain_two, grad_gain_three, grad_gain_four)
    reduced = reduce_grads(weight_grads, gain_grads, weights, items, heads)
    shaped = [r.reshape(w.shape) for r, w in zip(reduced[:12], weights)]
    shaped += [r.reshape(g.shape) for r, g in zip(reduced[12:], gains)]
    return (rounded(final_rows), latents_grad, *shaped)


def solution(mesh):
    weight_specs = (
        P(ALL, None),
        P(None, ALL),
        P(None, ALL),
        P(ALL, None),
        P("items", "heads"),
        P("heads", "items"),
        P("items", "heads"),
        P("items", "heads"),
        P("items", "heads"),
        P("heads", "items"),
        P("items", "heads"),
        P("heads", "items"),
    )
    gain_specs = (P(ALL),) * 4
    placed = (P(ALL, None), P(None, "items"), P("items", None), P(ALL, None)) + weight_specs + gain_specs
    return jax.shard_map(
        local,
        mesh=mesh,
        in_specs=placed,
        out_specs=(P(ALL, None), P(ALL, None)) + weight_specs + gain_specs,
        check_vma=False,
    )
```
